128 devices in a mesh: data: 128 (over z, y, x, core).
Axes of the slice: x: 4, y: 4, z: 4, core: 2. Of those that a mesh axis runs over, the one named last changes fastest.
Arguments:
- act_in: bfloat16 [131072, 768], P('data')
- grad_out: bfloat16 [131072, 768], P('data')
- w_up1: bfloat16 [768, 3072], replicated
- w_down1: bfloat16 [3072, 768], replicated
- w_up2: bfloat16 [768, 3072], replicated
- w_down2: bfloat16 [3072, 768], replicated
- master_up1: float32 [768, 3072], P('data')
- master_down1: float32 [3072, 768], P('data')
- master_up2: float32 [768, 3072], P('data')
- master_down2: float32 [3072, 768], P('data')
- mom_up1: float32 [768, 3072], P('data')
- mom_down1: float32 [3072, 768], P('data')
- mom_up2: float32 [768, 3072], P('data')
- mom_down2: float32 [3072, 768], P('data')
- vel_up1: float32 [768, 3072], P('data')
- vel_down1: float32 [3072, 768], P('data')
- vel_up2: float32 [768, 3072], P('data')
- vel_down2: float32 [3072, 768], P('data')
- learn_rate: float32 [], replicated
- clip_norm: float32 [], replicated
Outputs:
- output 1: bfloat16 [768, 3072], replicated
- output 2: bfloat16 [3072, 768], replicated
- output 3: bfloat16 [768, 3072], replicated
- output 4: bfloat16 [3072, 768], replicated
- output 5: float32 [768, 3072], P('data')
- output 6: float32 [3072, 768], P('data')
- output 7: float32 [768, 3072], P('data')
- output 8: float32 [3072, 768], P('data')
- output 9: float32 [768, 3072], P('data')
- output 10: float32 [3072, 768], P('data')
- output 11: float32 [768, 3072], P('data')
- output 12: float32 [3072, 768], P('data')
- output 13: float32 [768, 3072], P('data')
- output 14: float32 [3072, 768], P('data')
- output 15: float32 [768, 3072], P('data')
- output 16: float32 [3072, 768], P('data')
- output 17: float32 [], replicated
All inputs are finite; a program needn't handle non-finite values.
Results may differ from the reference program's by a relative error of at most 0.0109451.
Values are sent between devices in bfloat16 or wider.
A program may use at most 1 GiB of HBM per device.

```python
import math
import jax
import jax.numpy as jnp
from jax import lax

D = 768
FF = 3072
ROWS = 131072
GROUP = 128
STEP = 20
SAMPLE = 256

BETA_ONE = 0.9
BETA_TWO = 0.95
EPSILON = 1e-8
NORM_EPS = 1e-6
CORR_ONE = 1.0 - BETA_ONE ** STEP
CORR_TWO = 1.0 - BETA_TWO ** STEP
ROOT_HALF = math.sqrt(0.5)
INV_ROOT_TAU = 1.0 / math.sqrt(2.0 * math.pi)
LAYER_GAINS = (1.0, 1.5, 1.0, 2.0)
LAYER_NAMES = ("up1", "down1", "up2", "down2")


def gelu_pair(pre):
    normal_cdf = 0.5 * (1.0 + lax.erf(pre * ROOT_HALF))
    density = jnp.exp(-0.5 * pre * pre) * INV_ROOT_TAU
    return pre * normal_cdf, normal_cdf + pre * density


def fwd_bwd(rows_in, rows_grad, w_up1, w_down1, w_up2, w_down2):
    pre_up1 = jnp.dot(rows_in, w_up1, preferred_element_type=jnp.float32)
    gel_up1, der_up1 = gelu_pair(pre_up1)
    act_up1 = gel_up1.astype(jnp.bfloat16)
    mid_act = jnp.dot(act_up1, w_down1, preferred_element_type=jnp.float32).astype(jnp.bfloat16)
    pre_up2 = jnp.dot(mid_act, w_up2, preferred_element_type=jnp.float32)
    gel_up2, der_up2 = gelu_pair(pre_up2)
    act_up2 = gel_up2.astype(jnp.bfloat16)
    grad_act2 = jnp.dot(rows_grad, w_down2.T, preferred_element_type=jnp.float32).astype(jnp.bfloat16)
    grad_pre2 = (grad_act2.astype(jnp.float32) * der_up2).astype(jnp.bfloat16)
    grad_mid = jnp.dot(grad_pre2, w_up2.T, preferred_element_type=jnp.float32).astype(jnp.bfloat16)
    grad_act1 = jnp.dot(grad_mid, w_down1.T, preferred_element_type=jnp.float32).astype(jnp.bfloat16)
    grad_pre1 = (grad_act1.astype(jnp.float32) * der_up1).astype(jnp.bfloat16)
    return ((act_up2, rows_grad), (mid_act, grad_pre2), (act_up1, grad_mid), (rows_in, grad_pre1))


def adam_step(grad_rows, master_old, mom_old, vel_old, clip_scale, learn_rate):
    scaled = clip_scale * grad_rows
    mom_new = BETA_ONE * mom_old + (1.0 - BETA_ONE) * scaled
    vel_new = BETA_TWO * vel_old + (1.0 - BETA_TWO) * scaled * scaled
    master_new = master_old - learn_rate * (mom_new / CORR_ONE) / (jnp.sqrt(vel_new / CORR_TWO) + EPSILON)
    return master_new.astype(jnp.bfloat16), master_new, mom_new, vel_new


def norm_estimate(act_in, grad_out, weights):
    stride = ROWS // SAMPLE
    grad_pairs = fwd_bwd(act_in[::stride], grad_out[::stride], weights[0], weights[1], weights[2], weights[3])
    row_total = 0.0
    for layer_in, layer_delta in grad_pairs:
        in_sq = jnp.sum(jnp.square(layer_in.astype(jnp.float32)), axis=1)
        delta_sq = jnp.sum(jnp.square(layer_delta.astype(jnp.float32)), axis=1)
        row_total = row_total + jnp.sum(in_sq * delta_sq)
    return jnp.sqrt(row_total * stride) / GROUP


def setup_inputs(seed: int = 0) -> dict:
    key_list = jax.random.split(jax.random.key(seed), 20)
    act_in = jax.random.normal(key_list[0], (ROWS, D), jnp.float32).astype(jnp.bfloat16)
    grad_scale = 2.0 * GROUP / math.sqrt(ROWS * D * FF)
    grad_out = (grad_scale * jax.random.normal(key_list[1], (ROWS, D), jnp.float32)).astype(jnp.bfloat16)
    shapes = ((D, FF), (FF, D), (D, FF), (FF, D))
    weights = []
    masters = []
    for layer_idx in range(4):
        init_scale = LAYER_GAINS[layer_idx] / math.sqrt(shapes[layer_idx][0])
        weight = init_scale * jax.random.normal(key_list[2 + layer_idx], shapes[layer_idx], jnp.float32)
        weights.append(weight.astype(jnp.bfloat16))
        masters.append(weight + 0.01 * init_scale * jax.random.normal(key_list[6 + layer_idx], shapes[layer_idx], jnp.float32))
    clip_norm = norm_estimate(act_in, grad_out, weights) * jax.random.uniform(key_list[10], (), jnp.float32, 0.3, 0.6)
    unit_size = clip_norm / math.sqrt(4 * D * FF)
    inputs = {"act_in": act_in, "grad_out": grad_out}
    for layer_idx in range(4):
        inputs["w_" + LAYER_NAMES[layer_idx]] = weights[layer_idx]
    for layer_idx in range(4):
        inputs["master_" + LAYER_NAMES[layer_idx]] = masters[layer_idx]
    for layer_idx in range(4):
        inputs["mom_" + LAYER_NAMES[layer_idx]] = 0.1 * unit_size * jax.random.normal(key_list[11 + layer_idx], shapes[layer_idx], jnp.float32)
    for layer_idx in range(4):
        inputs["vel_" + LAYER_NAMES[layer_idx]] = 0.05 * unit_size * unit_size * jax.random.uniform(key_list[15 + layer_idx], shapes[layer_idx], jnp.float32, 0.5, 1.5)
    inputs["learn_rate"] = 0.5 / math.sqrt(D) * jax.random.uniform(key_list[19], (), jnp.float32, 0.2, 1.0)
    inputs["clip_norm"] = clip_norm
    return inputs


def reference(act_in, grad_out, w_up1, w_down1, w_up2, w_down2, master_up1, master_down1, master_up2, master_down2, mom_up1, mom_down1, mom_up2, mom_down2, vel_up1, vel_down1, vel_up2, vel_down2, learn_rate, clip_norm):
    rows_dev = ROWS // GROUP
    dev_in = act_in.reshape(GROUP, rows_dev, D)
    dev_grad = grad_out.reshape(GROUP, rows_dev, D)

    def accumulate(carry, block):
        grad_pairs = fwd_bwd(block[0], block[1], w_up1, w_down1, w_up2, w_down2)
        summed = tuple(carry[layer_idx] + jnp.dot(grad_pairs[layer_idx][0].T, grad_pairs[layer_idx][1], preferred_element_type=jnp.float32) for layer_idx in range(4))
        return summed, None

    start_sums = (jnp.zeros((FF, D), jnp.float32), jnp.zeros((D, FF), jnp.float32), jnp.zeros((FF, D), jnp.float32), jnp.zeros((D, FF), jnp.float32))
    totals = lax.scan(accumulate, start_sums, (dev_in, dev_grad))[0]
    grad_list = [totals[3] / GROUP, totals[2] / GROUP, totals[1] / GROUP, totals[0] / GROUP]
    grad_norm = jnp.sqrt(sum(jnp.sum(grad_rows * grad_rows) for grad_rows in grad_list))
    clip_scale = jnp.minimum(1.0, clip_norm / (grad_norm + NORM_EPS))
    state_up1 = adam_step(grad_list[0], master_up1, mom_up1, vel_up1, clip_scale, learn_rate)
    state_down1 = adam_step(grad_list[1], master_down1, mom_down1, vel_down1, clip_scale, learn_rate)
    state_up2 = adam_step(grad_list[2], master_up2, mom_up2, vel_up2, clip_scale, learn_rate)
    state_down2 = adam_step(grad_list[3], master_down2, mom_down2, vel_down2, clip_scale, learn_rate)
    return (state_up1[0], state_down1[0], state_up2[0], state_down2[0], state_up1[1], state_down1[1], state_up2[1], state_down2[1], state_up1[2], state_down1[2], state_up2[2], state_down2[2], state_up1[3], state_down1[3], state_up2[3], state_down2[3], grad_norm)
```

```python
import functools
import math
import jax
import jax.numpy as jnp
from jax import lax
from jax.experimental import pallas as pl
from jax.experimental.pallas import tpu as pltpu
from jax.sharding import PartitionSpec as P

STEP = 20
BETA_ONE = 0.9
BETA_TWO = 0.95
EPSILON = 1e-8
NORM_EPS = 1e-6
CORR_ONE = 1.0 - BETA_ONE ** STEP
CORR_TWO = 1.0 - BETA_TWO ** STEP
ROOT_HALF = math.sqrt(0.5)
INV_ROOT_TAU = 1.0 / math.sqrt(2.0 * math.pi)

MESH = pl.DeviceIdType.MESH
STRIDES = (32, 8, 2)
ORDERS = ((2, 1, 0), (1, 0, 2), (0, 2, 1))
ROWS = 24
SUB = 6
CHUNK = 8


def adam_step(scaled, master_old, mom_old, vel_old, learn_rate):
    mom_new = BETA_ONE * mom_old + (1.0 - BETA_ONE) * scaled
    vel_new = BETA_TWO * vel_old + (1.0 - BETA_TWO) * scaled * scaled
    master_new = master_old - learn_rate * (mom_new / CORR_ONE) / (jnp.sqrt(vel_new / CORR_TWO) + EPSILON)
    return master_new, mom_new, vel_new


def comm_kernel(lanes, *refs):
    (g_up1, g_down1, g_up2, g_down2), refs = refs[:4], refs[4:]
    masters, moms, vels, refs = refs[:4], refs[4:8], refs[8:12], refs[12:]
    (lr_ref, clip_ref), refs = refs[:2], refs[2:]
    w_out, refs = refs[0], refs[1:]
    new_masters, new_moms, new_vels, refs = refs[:4], refs[4:8], refs[8:12], refs[12:]
    norm_out, refs = refs[0], refs[1:]
    (total, peer_in, rs1, rs2, rs3, norm_core, norm_axis, send_g, recv_g, send_w, recv_w, block_tmp, w_own), refs = refs[:13], refs[13:]
    (load_sem, pair_s, pair_r, rs1_s, rs1_r, rs2_s, rs2_r, rs3_s, rs3_r, nc_s, nc_r, na_s, na_r, xg_s, xg_r, xw_s, xw_r, own_sem, ag_s, ag_r, out_s, out_r) = refs
    half = lanes // 2
    me = lax.axis_index("data")
    core = lax.rem(me, 2)
    member = lax.rem(me, 4)
    pos = (me // 32, lax.rem(me // 8, 4), lax.rem(me // 2, 4))
    partner = me + 1 - 2 * core

    def device(axis, coord):
        return me + (coord - pos[axis]) * STRIDES[axis]

    def step(axis, hops):
        return lax.rem(pos[axis] + hops, 4)

    def remote(src, dst, send_sem, recv_sem, target):
        return pltpu.make_async_remote_copy(src_ref=src, dst_ref=dst, send_sem=send_sem, recv_sem=recv_sem, device_id=(target,), device_id_type=MESH)

    peers = [partner] + [device(axis, step(axis, hops)) for axis in range(3) for hops in (1, 2, 3)]
    peers.append(me - member + lax.rem(member + 2, 4) + 1 - 2 * core)
    barrier = pltpu.get_barrier_semaphore()
    for peer in peers:
        pl.semaphore_signal(barrier, inc=1, device_id=(peer,), device_id_type=MESH)

    grads = (g_up1, g_down1, g_up2, g_down2)
    mat_order = (3, 2, 1, 0)

    def pieces(mat, owner):
        if mat % 2:
            return [(grads[mat].at[:, :, :, owner], (mat,))]
        out = []
        for x in range(4):
            col = pl.multiple_of(((x % 2) * 2 + owner) * lanes, lanes)
            out.append((grads[mat].at[:, :, x // 2, :, pl.ds(col, lanes)], (mat, slice(None), slice(None), x)))
        return out

    loads, pairs = {}, {}
    for mat in mat_order:
        loads[mat] = [pltpu.make_async_copy(src, total.at[dst], load_sem.at[mat, i]) for i, (src, dst) in enumerate(pieces(mat, core))]
        for copy in loads[mat]:
            copy.start()
    pl.semaphore_wait(barrier, len(peers))
    for mat in mat_order:
        pairs[mat] = [remote(src, peer_in.at[dst], pair_s.at[mat, i], pair_r.at[mat, i], partner) for i, (src, dst) in enumerate(pieces(mat, 1 - core))]
        for copy in pairs[mat]:
            copy.start()

    def part(mats, coords, colour, side):
        index = [mats, slice(None), slice(None), slice(None), pl.ds(CHUNK * colour, CHUNK), pl.ds(half * side, half)]
        for axis, coord in coords.items():
            index[1 + axis] = coord
        return tuple(index)

    class Phase:
        def __init__(self, level, mats, buf, send_sem, recv_sem):
            self.level, self.mats, self.buf, self.send_sem, self.recv_sem = level, mats, buf, send_sem, recv_sem
            self.copies = {}

        def where(self, colour, coord):
            order = ORDERS[colour]
            coords = {axis: pos[axis] for axis in order[:self.level]}
            coords[order[self.level]] = coord
            return coords

        def send(self, colour, side, kind, src, target):
            copy = remote(src, self.buf.at[colour, side, kind], self.send_sem.at[colour, side, kind], self.recv_sem.at[colour, side, kind], target)
            copy.start()
            self.copies[colour, side, kind] = copy

        def near(self, colour, side):
            axis = ORDERS[colour][self.level]
            coord = step(axis, 1 if side == 0 else 3)
            return coord, device(axis, coord)

        def start(self):
            for kind in range(2):
                for colour in range(3):
                    for side in range(2):
                        coord, target = self.near(colour, side)
                        aim = step(ORDERS[colour][self.level], 2) if kind == 0 else coord
                        src = total.at[part(self.mats, self.where(colour, aim), colour, side if kind == 0 else 1 - side)]
                        self.send(colour, side, kind, src, target)

        def forward(self):
            for colour in range(3):
                for side in range(2):
                    coord, target = self.near(colour, side)
                    self.copies[colour, side, 0].wait_recv()
                    self.buf[colour, side, 0] = self.buf[colour, side, 0] + total[part(self.mats, self.where(colour, coord), colour, side)]
                    self.send(colour, side, 2, self.buf.at[colour, side, 0], target)

        def finish(self):
            for colour in range(3):
                for side in range(2):
                    own = part(self.mats, self.where(colour, pos[ORDERS[colour][self.level]]), colour, side)
                    self.copies[colour, 1 - side, 1].wait_recv()
                    self.copies[colour, side, 2].wait_recv()
                    total[own] = total[own] + (self.buf[colour, 1 - side, 1] + self.buf[colour, side, 2])

        def drain(self):
            for copy in self.copies.values():
                copy.wait_send()

    everything = slice(None)
    first = {}
    previous = None
    for mat in mat_order:
        for copy in loads[mat]:
            copy.wait()
        for copy in pairs[mat]:
            copy.wait_recv()

        def add_pair(i, carry, mat=mat):
            total[mat, i // 4, lax.rem(i, 4)] = total[mat, i // 4, lax.rem(i, 4)] + peer_in[mat, i // 4, lax.rem(i, 4)]
            return carry

        lax.fori_loop(0, 16, add_pair, 0)
        first[mat] = Phase(0, mat, rs1.at[mat], rs1_s.at[mat], rs1_r.at[mat])
        first[mat].start()
        if previous is not None:
            first[previous].forward()
        previous = mat
    first[previous].forward()
    for mat in mat_order:
        first[mat].finish()
    second = Phase(1, everything, rs2, rs2_s, rs2_r)
    second.start()
    second.forward()
    second.finish()
    third = Phase(2, everything, rs3, rs3_s, rs3_r)
    third.start()
    third.forward()
    third.finish()

    group_scale = 1.0 / 128.0
    grad_own = [total[mat, pos[0], pos[1], pos[2]] * group_scale for mat in range(4)]
    partial = None
    for block in grad_own:
        square = block * block
        for row in range(ROWS // 8):
            for col in range(max(1, lanes // 128)):
                tile = square[8 * row:8 * row + 8, 128 * col:128 * col + 128]
                partial = tile if partial is None else partial + tile
    norm_core[core] = partial
    swap = remote(norm_core.at[core], norm_core.at[core], nc_s.at[0], nc_r.at[0], partner)
    swap.start()
    for target in range(4):
        for i, mat in enumerate((0, 2)):
            send_g[target, i] = grad_own[mat][SUB * target:SUB * target + SUB]
    moves = []
    for hops in range(1, 4):
        other = lax.rem(member + hops, 4)
        copy = remote(send_g.at[other], recv_g.at[member], xg_s.at[hops - 1], xg_r.at[hops - 1], me - member + other)
        copy.start()
        moves.append(copy)
    recv_g[member] = send_g[member]
    swap.wait_recv()
    running = norm_core[0] + norm_core[1]
    sends = [swap] + moves
    for axis in (2, 1, 0):
        norm_axis[axis, pos[axis]] = running
        copies = []
        for hops in (1, 2, 3):
            coord = step(axis, hops)
            copy = remote(norm_axis.at[axis, pos[axis]], norm_axis.at[axis, pos[axis]], na_s.at[axis, hops - 1], na_r.at[axis, hops - 1], device(axis, coord))
            copy.start()
            copies.append(copy)
        for copy in copies:
            copy.wait_recv()
        sends = sends + copies
        running = (norm_axis[axis, 0] + norm_axis[axis, 1]) + (norm_axis[axis, 2] + norm_axis[axis, 3])
    norm = jnp.sqrt(jnp.sum(jnp.sum(running, axis=1, keepdims=True), axis=0, keepdims=True))
    norm_out[...] = jnp.broadcast_to(norm, norm_out.shape)
    clip_scale = jnp.minimum(1.0, clip_ref[0] / (norm + NORM_EPS))
    learn_rate = lr_ref[0]

    for copy in moves:
        copy.wait_recv()
    for i, mat in enumerate((0, 2)):
        for col in range(4):
            cols = slice(col * lanes, (col + 1) * lanes)
            scaled = recv_g[col, i] * clip_scale
            master_new, mom_new, vel_new = adam_step(scaled, masters[mat][:, cols], moms[mat][:, cols], vels[mat][:, cols], learn_rate)
            new_masters[mat][:, cols] = master_new
            new_moms[mat][:, cols] = mom_new
            new_vels[mat][:, cols] = vel_new
            send_w[col, i] = master_new
    moves = []
    for hops in range(1, 4):
        other = lax.rem(member + hops, 4)
        copy = remote(send_w.at[other], recv_w.at[member], xw_s.at[hops - 1], xw_r.at[hops - 1], me - member + other)
        copy.start()
        moves.append(copy)
    recv_w[member] = send_w[member]
    for mat in (1, 3):
        master_new, mom_new, vel_new = adam_step(grad_own[mat] * clip_scale, masters[mat][...], moms[mat][...], vels[mat][...], learn_rate)
        new_masters[mat][...] = master_new
        new_moms[mat][...] = mom_new
        new_vels[mat][...] = vel_new
        w_own[mat] = master_new.astype(jnp.bfloat16)
    for copy in moves:
        copy.wait_recv()
    sends = sends + moves
    for i, mat in enumerate((0, 2)):
        for source in range(4):
            block_tmp[SUB * source:SUB * source + SUB] = recv_w[source, i]
        w_own[mat] = block_tmp[...].astype(jnp.bfloat16)

    keep = pltpu.make_async_copy(w_own, w_out.at[:, pos[0], pos[1], pos[2], core], own_sem)
    keep.start()

    def spot(coords, colour, side):
        lane = slice(None) if side is None else pl.ds(half * side, half)
        index = [slice(None), slice(None), slice(None), slice(None), core, pl.ds(CHUNK * colour, CHUNK), lane]
        for axis, coord in coords.items():
            index[1 + axis] = coord
        return w_out.at[tuple(index)]

    handed = []

    def hand(ref, slot):
        copy = remote(ref, ref, out_s.at[slot], out_r.at[slot], partner)
        copy.start()
        handed.append(copy)

    for level in (2, 1, 0):
        if level == 1:
            keep.wait()

        def where(colour, coord):
            order = ORDERS[colour]
            coords = {axis: pos[axis] for axis in order[:level]}
            coords[order[level]] = coord
            return coords

        def near(colour, side):
            axis = ORDERS[colour][level]
            coord = step(axis, 1 if side == 0 else 3)
            return coord, device(axis, coord)

        copies = {}
        for kind in range(2):
            for colour in range(3):
                for side in range(2):
                    lane_side = side if kind == 0 else 1 - side
                    dst = spot(where(colour, pos[ORDERS[colour][level]]), colour, lane_side)
                    src = w_own.at[:, pl.ds(CHUNK * colour, CHUNK), pl.ds(half * lane_side, half)] if level == 2 else dst
                    copy = remote(src, dst, ag_s.at[level, colour, side, kind], ag_r.at[level, colour, side, kind], near(colour, side)[1])
                    copy.start()
                    copies[colour, side, kind] = copy
        if level == 0:
            for colour in range(3):
                hand(spot(where(colour, pos[ORDERS[colour][0]]), colour, None), 5 * colour)
        for colour in range(3):
            for side in range(2):
                back = near(colour, 1 - side)[0]
                copies[colour, side, 0].wait_recv()
                ref = spot(where(colour, back), colour, side)
                copy = remote(ref, ref, ag_s.at[level, colour, side, 2], ag_r.at[level, colour, side, 2], near(colour, side)[1])
                copy.start()
                copies[colour, side, 2] = copy
        for colour in range(3):
            for side in range(2):
                copies[colour, side, 1].wait_recv()
                if level == 0:
                    hand(spot(where(colour, near(colour, 1 - side)[0]), colour, None), 5 * colour + 1 + side)
        for colour in range(3):
            for side in range(2):
                copies[colour, side, 2].wait_recv()
                if level == 0:
                    hand(spot(where(colour, step(ORDERS[colour][0], 2)), colour, side), 5 * colour + 3 + side)
        sends = sends + list(copies.values())
    for phase in list(first.values()) + [second, third]:
        phase.drain()
    for mat in mat_order:
        for copy in pairs[mat]:
            copy.wait_send()
    for copy in sends:
        copy.wait_send()
    for copy in handed:
        copy.wait()


def comm_call(lanes, grads, masters, moms, vels, learn_rate, clip_norm):
    up = (4, 4, 2, ROWS, 4 * lanes)
    down = (4, 4, 4, 2, ROWS, lanes)
    grads = [grads[0].reshape(up), grads[1].reshape(down), grads[2].reshape(up), grads[3].reshape(down)]
    half = lanes // 2
    f32 = jnp.float32
    dma = pltpu.SemaphoreType.DMA
    state_shapes = [jax.ShapeDtypeStruct(m.shape, f32) for m in masters] * 3
    vmem = pl.BlockSpec(memory_space=pltpu.VMEM)
    smem = pl.BlockSpec(memory_space=pltpu.SMEM)
    hbm = pl.BlockSpec(memory_space=pl.ANY)
    scratch = [
        pltpu.VMEM((4, 4, 4, 4, ROWS, lanes), f32),
        pltpu.VMEM((4, 4, 4, 4, ROWS, lanes), f32),
        pltpu.VMEM((4, 3, 2, 3, 4, 4, CHUNK, half), f32),
        pltpu.VMEM((3, 2, 3, 4, 4, CHUNK, half), f32),
        pltpu.VMEM((3, 2, 3, 4, CHUNK, half), f32),
        pltpu.VMEM((2, 8, min(lanes, 128)), f32),
        pltpu.VMEM((3, 4, 8, min(lanes, 128)), f32),
        pltpu.VMEM((4, 2, SUB, lanes), f32),
        pltpu.VMEM((4, 2, SUB, lanes), f32),
        pltpu.VMEM((4, 2, SUB, lanes), f32),
        pltpu.VMEM((4, 2, SUB, lanes), f32),
        pltpu.VMEM((ROWS, lanes), f32),
        pltpu.VMEM((4, ROWS, lanes), jnp.bfloat16),
        dma((4, 4)), dma((4, 4)), dma((4, 4)),
        dma((4, 3, 2, 3)), dma((4, 3, 2, 3)), dma((3, 2, 3)), dma((3, 2, 3)), dma((3, 2, 3)), dma((3, 2, 3)),
        dma((1,)), dma((1,)), dma((3, 3)), dma((3, 3)), dma((3,)), dma((3,)), dma((3,)), dma((3,)),
        dma, dma((3, 3, 2, 3)), dma((3, 3, 2, 3)), dma((15,)), dma((15,)),
    ]
    outs = pl.pallas_call(
        functools.partial(comm_kernel, lanes),
        name="reduce_update_gather",
        out_shape=[jax.ShapeDtypeStruct((4, 4, 4, 4, 2, ROWS, lanes), jnp.bfloat16)] + state_shapes + [jax.ShapeDtypeStruct((8, 128), f32)],
        in_specs=[hbm] * 4 + [vmem] * 12 + [smem] * 2,
        out_specs=[hbm] + [vmem] * 12 + [vmem],
        scratch_shapes=scratch,
        compiler_params=pltpu.CompilerParams(collective_id=0, has_side_effects=True, vmem_limit_bytes=67043328),
    )(*grads, *masters, *moms, *vels, learn_rate.reshape(1), clip_norm.reshape(1))
    blocks = outs[0]
    weights = []
    for mat in range(4):
        if mat % 2:
            weights.append(blocks[mat].reshape(3072, lanes))
        else:
            split = blocks[mat].reshape(4, 4, 2, 2, 2, ROWS, lanes)
            weights.append(split.transpose(0, 1, 2, 5, 3, 4, 6).reshape(768, 4 * lanes))
    return tuple(weights) + tuple(outs[1:13]) + (outs[13][0, 0],)


def mat_nt(left, right):
    return lax.dot_general(left, right, (((1,), (1,)), ((), ())), preferred_element_type=jnp.float32)


def mat_tn(left, right):
    return lax.dot_general(left, right, (((0,), (0,)), ((), ())), preferred_element_type=jnp.float32)


def gelu_pair(pre):
    normal_cdf = 0.5 * (1.0 + lax.erf(pre * ROOT_HALF))
    density = jnp.exp(-0.5 * pre * pre) * INV_ROOT_TAU
    return pre * normal_cdf, normal_cdf + pre * density


def fwd_bwd(rows_in, rows_grad, w_up1, w_down1, w_up2, w_down2):
    pre_up1 = jnp.dot(rows_in, w_up1, preferred_element_type=jnp.float32)
    gel_up1, der_up1 = gelu_pair(pre_up1)
    act_up1 = gel_up1.astype(jnp.bfloat16)
    mid_act = jnp.dot(act_up1, w_down1, preferred_element_type=jnp.float32).astype(jnp.bfloat16)
    pre_up2 = jnp.dot(mid_act, w_up2, preferred_element_type=jnp.float32)
    gel_up2, der_up2 = gelu_pair(pre_up2)
    act_up2 = gel_up2.astype(jnp.bfloat16)
    grad_act2 = mat_nt(rows_grad, w_down2).astype(jnp.bfloat16)
    grad_pre2 = (grad_act2.astype(jnp.float32) * der_up2).astype(jnp.bfloat16)
    grad_mid = mat_nt(grad_pre2, w_up2).astype(jnp.bfloat16)
    grad_act1 = mat_nt(grad_mid, w_down1).astype(jnp.bfloat16)
    grad_pre1 = (grad_act1.astype(jnp.float32) * der_up1).astype(jnp.bfloat16)
    return ((rows_in, grad_pre1), (act_up1, grad_mid), (mid_act, grad_pre2), (act_up2, rows_grad))


def solution(mesh):
    rows_spec = P("data", None)
    full_spec = P(None, None)
    scalar_spec = P()

    def shard_body(act_in, grad_out, w_up1, w_down1, w_up2, w_down2, *rest):
        pairs = fwd_bwd(act_in, grad_out, w_up1, w_down1, w_up2, w_down2)
        grads = [mat_tn(left, right) for left, right in pairs]
        return comm_call(768, grads, rest[0:4], rest[4:8], rest[8:12], rest[12], rest[13])

    in_specs = (rows_spec, rows_spec) + (full_spec,) * 4 + (rows_spec,) * 12 + (scalar_spec, scalar_spec)
    out_specs = (full_spec,) * 4 + (rows_spec,) * 12 + (scalar_spec,)
    return jax.shard_map(shard_body, mesh=mesh, in_specs=in_specs, out_specs=out_specs, check_vma=False)
```

```python
import functools
import math
import jax
import jax.numpy as jnp
from jax import lax
from jax.experimental import pallas as pl
from jax.experimental.pallas import tpu as pltpu
from jax.sharding import PartitionSpec as P

STEP = 20
BETA_ONE = 0.9
BETA_TWO = 0.95
EPSILON = 1e-8
NORM_EPS = 1e-6
CORR_ONE = 1.0 - BETA_ONE ** STEP
CORR_TWO = 1.0 - BETA_TWO ** STEP
ROOT_HALF = math.sqrt(0.5)
INV_ROOT_TAU = 1.0 / math.sqrt(2.0 * math.pi)

MESH = pl.DeviceIdType.MESH
STRIDES = (32, 8, 2)
ORDERS = ((2, 1, 0), (1, 0, 2), (0, 2, 1))
ROWS = 24
SUB = 6
CHUNK = 8


def adam_step(scaled, master_old, mom_old, vel_old, learn_rate):
    mom_new = BETA_ONE * mom_old + (1.0 - BETA_ONE) * scaled
    vel_new = BETA_TWO * vel_old + (1.0 - BETA_TWO) * scaled * scaled
    master_new = master_old - learn_rate * (mom_new / CORR_ONE) / (jnp.sqrt(vel_new / CORR_TWO) + EPSILON)
    return master_new, mom_new, vel_new


def comm_kernel(lanes, *refs):
    (g_up1, g_down1, g_up2, g_down2), refs = refs[:4], refs[4:]
    states, refs = refs[:12], refs[12:]
    (lr_ref, clip_ref), refs = refs[:2], refs[2:]
    (w_out, up_out, down_out, norm_out), refs = refs[:4], refs[4:]
    (total, peer_in, rs1, rs2, rs3, norm_core, norm_axis, send_g, recv_g, send_w, recv_w, block_tmp, w_own, up_state, down_state), refs = refs[:15], refs[15:]
    (load_sem, state_sem, pair_s, pair_r, rs1_s, rs1_r, rs2_s, rs2_r, rs3_s, rs3_r, nc_s, nc_r, na_s, na_r, xg_s, xg_r, xw_s, xw_r, own_sem, ag_s, ag_r, out_s, out_r) = refs
    half = lanes // 2
    me = lax.axis_index("data")
    core = lax.rem(me, 2)
    member = lax.rem(me, 4)
    pos = (me // 32, lax.rem(me // 8, 4), lax.rem(me // 2, 4))
    partner = me + 1 - 2 * core

    def device(axis, coord):
        return me + (coord - pos[axis]) * STRIDES[axis]

    def step(axis, hops):
        return lax.rem(pos[axis] + hops, 4)

    def remote(src, dst, send_sem, recv_sem, target):
        return pltpu.make_async_remote_copy(src_ref=src, dst_ref=dst, send_sem=send_sem, recv_sem=recv_sem, device_id=(target,), device_id_type=MESH)

    peers = [partner] + [device(axis, step(axis, hops)) for axis in range(3) for hops in (1, 2, 3)]
    peers.append(me - member + lax.rem(member + 2, 4) + 1 - 2 * core)
    barrier = pltpu.get_barrier_semaphore()
    for peer in peers:
        pl.semaphore_signal(barrier, inc=1, device_id=(peer,), device_id_type=MESH)

    grads = (g_up1, g_down1, g_up2, g_down2)
    mat_order = (3, 2, 1, 0)

    def pieces(mat, owner):
        if mat % 2:
            return [(grads[mat].at[:, :, :, owner], (mat,))]
        out = []
        for x in range(4):
            col = pl.multiple_of(((x % 2) * 2 + owner) * lanes, lanes)
            out.append((grads[mat].at[:, :, x // 2, :, pl.ds(col, lanes)], (mat, slice(None), slice(None), x)))
        return out

    loads, pairs = {}, {}
    for mat in mat_order:
        loads[mat] = [pltpu.make_async_copy(src, total.at[dst], load_sem.at[mat, i]) for i, (src, dst) in enumerate(pieces(mat, core))]
        for copy in loads[mat]:
            copy.start()
    state_loads = []
    for field in range(3):
        for mat in range(4):
            dst = (down_state if mat % 2 else up_state).at[field, mat // 2]
            copy = pltpu.make_async_copy(states[4 * field + mat], dst, state_sem.at[field, mat])
            copy.start()
            state_loads.append(copy)
    pl.semaphore_wait(barrier, len(peers))
    for mat in mat_order:
        pairs[mat] = [remote(src, peer_in.at[dst], pair_s.at[mat, i], pair_r.at[mat, i], partner) for i, (src, dst) in enumerate(pieces(mat, 1 - core))]
        for copy in pairs[mat]:
            copy.start()

    def part(mats, coords, colour, side):
        index = [mats, slice(None), slice(None), slice(None), pl.ds(CHUNK * colour, CHUNK), pl.ds(half * side, half)]
        for axis, coord in coords.items():
            index[1 + axis] = coord
        return tuple(index)

    class Phase:
        def __init__(self, level, mats, buf, send_sem, recv_sem):
            self.level, self.mats, self.buf, self.send_sem, self.recv_sem = level, mats, buf, send_sem, recv_sem
            self.copies = {}

        def where(self, colour, coord):
            order = ORDERS[colour]
            coords = {axis: pos[axis] for axis in order[:self.level]}
            coords[order[self.level]] = coord
            return coords

        def row(self, colour, coord, side, i):
            coords = self.where(colour, coord)
            if self.level:
                return part(i, coords, colour, side)
            coords[min(axis for axis in range(3) if axis not in coords)] = i
            return part(self.mats, coords, colour, side)

        def send(self, colour, side, kind, src, target):
            copy = remote(src, self.buf.at[colour, side, kind], self.send_sem.at[colour, side, kind], self.recv_sem.at[colour, side, kind], target)
            copy.start()
            self.copies[colour, side, kind] = copy

        def near(self, colour, side):
            axis = ORDERS[colour][self.level]
            coord = step(axis, 1 if side == 0 else 3)
            return coord, device(axis, coord)

        def start(self):
            for kind in range(2):
                for colour in range(3):
                    for side in range(2):
                        coord, target = self.near(colour, side)
                        aim = step(ORDERS[colour][self.level], 2) if kind == 0 else coord
                        src = total.at[part(self.mats, self.where(colour, aim), colour, side if kind == 0 else 1 - side)]
                        self.send(colour, side, kind, src, target)

        def forward(self):
            for colour in range(3):
                for side in range(2):
                    coord, target = self.near(colour, side)
                    self.copies[colour, side, 0].wait_recv()

                    def add_own(i, carry, colour=colour, side=side, coord=coord):
                        self.buf[colour, side, 0, i] = self.buf[colour, side, 0, i] + total[self.row(colour, coord, side, i)]
                        return carry

                    lax.fori_loop(0, 4, add_own, 0)
                    self.send(colour, side, 2, self.buf.at[colour, side, 0], target)

        def finish(self):
            for colour in range(3):
                for side in range(2):
                    self.copies[colour, 1 - side, 1].wait_recv()
                    self.copies[colour, side, 2].wait_recv()

                    def add_both(i, carry, colour=colour, side=side):
                        own = self.row(colour, pos[ORDERS[colour][self.level]], side, i)
                        total[own] = total[own] + (self.buf[colour, 1 - side, 1, i] + self.buf[colour, side, 2, i])
                        return carry

                    lax.fori_loop(0, 4, add_both, 0)

        def drain(self):
            for copy in self.copies.values():
                copy.wait_send()

    everything = slice(None)
    first = {}
    previous = None
    for mat in mat_order:
        for copy in loads[mat]:
            copy.wait()
        for copy in pairs[mat]:
            copy.wait_recv()

        def add_pair(i, carry, mat=mat):
            total[mat, i // 4, lax.rem(i, 4)] = total[mat, i // 4, lax.rem(i, 4)] + peer_in[mat, i // 4, lax.rem(i, 4)]
            return carry

        lax.fori_loop(0, 16, add_pair, 0)
        first[mat] = Phase(0, mat, rs1.at[mat], rs1_s.at[mat], rs1_r.at[mat])
        first[mat].start()
        if previous is not None:
            first[previous].forward()
        previous = mat
    first[previous].forward()
    for mat in mat_order:
        first[mat].finish()
    second = Phase(1, everything, rs2, rs2_s, rs2_r)
    second.start()
    second.forward()
    second.finish()
    third = Phase(2, everything, rs3, rs3_s, rs3_r)
    third.start()
    third.forward()
    third.finish()

    group_scale = 1.0 / 128.0
    grad_own = [total[mat, pos[0], pos[1], pos[2]] * group_scale for mat in range(4)]
    partial = None
    for block in grad_own:
        square = block * block
        for row in range(ROWS // 8):
            for col in range(max(1, lanes // 128)):
                tile = square[8 * row:8 * row + 8, 128 * col:128 * col + 128]
                partial = tile if partial is None else partial + tile
    norm_core[core] = partial
    swap = remote(norm_core.at[core], norm_core.at[core], nc_s.at[0], nc_r.at[0], partner)
    swap.start()
    for target in range(4):
        for i, mat in enumerate((0, 2)):
            send_g[target, i] = grad_own[mat][SUB * target:SUB * target + SUB]
    moves = []
    for hops in range(1, 4):
        other = lax.rem(member + hops, 4)
        copy = remote(send_g.at[other], recv_g.at[member], xg_s.at[hops - 1], xg_r.at[hops - 1], me - member + other)
        copy.start()
        moves.append(copy)
    recv_g[member] = send_g[member]
    swap.wait_recv()
    running = norm_core[0] + norm_core[1]
    sends = [swap] + moves
    for axis in (2, 1, 0):
        norm_axis[axis, pos[axis]] = running
        copies = []
        for hops in (1, 2, 3):
            coord = step(axis, hops)
            copy = remote(norm_axis.at[axis, pos[axis]], norm_axis.at[axis, pos[axis]], na_s.at[axis, hops - 1], na_r.at[axis, hops - 1], device(axis, coord))
            copy.start()
            copies.append(copy)
        for copy in copies:
            copy.wait_recv()
        sends = sends + copies
        running = (norm_axis[axis, 0] + norm_axis[axis, 1]) + (norm_axis[axis, 2] + norm_axis[axis, 3])
    norm = jnp.sqrt(jnp.sum(jnp.sum(running, axis=1, keepdims=True), axis=0, keepdims=True))
    norm_out[...] = jnp.broadcast_to(norm, norm_out.shape)
    clip_scale = jnp.minimum(1.0, clip_ref[0] / (norm + NORM_EPS))
    learn_rate = lr_ref[0]

    for copy in moves:
        copy.wait_recv()
    for copy in state_loads:
        copy.wait()
    for i in range(2):
        for col in range(4):
            cols = slice(col * lanes, (col + 1) * lanes)
            scaled = recv_g[col, i] * clip_scale
            fresh = adam_step(scaled, up_state[0, i, :, cols], up_state[1, i, :, cols], up_state[2, i, :, cols], learn_rate)
            for field in range(3):
                up_state[field, i, :, cols] = fresh[field]
            send_w[col, i] = fresh[0]
    moves = []
    for hops in range(1, 4):
        other = lax.rem(member + hops, 4)
        copy = remote(send_w.at[other], recv_w.at[member], xw_s.at[hops - 1], xw_r.at[hops - 1], me - member + other)
        copy.start()
        moves.append(copy)
    recv_w[member] = send_w[member]
    for mat in (1, 3):
        i = mat // 2
        fresh = adam_step(grad_own[mat] * clip_scale, down_state[0, i], down_state[1, i], down_state[2, i], learn_rate)
        for field in range(3):
            down_state[field, i] = fresh[field]
        w_own[mat] = fresh[0].astype(jnp.bfloat16)
    for copy in moves:
        copy.wait_recv()
    sends = sends + moves
    for i, mat in enumerate((0, 2)):
        for source in range(4):
            block_tmp[SUB * source:SUB * source + SUB] = recv_w[source, i]
        w_own[mat] = block_tmp[...].astype(jnp.bfloat16)

    keep = pltpu.make_async_copy(w_own, w_out.at[:, pos[0], pos[1], pos[2], core], own_sem)
    keep.start()
    state_stores = [pltpu.make_async_copy(up_state, up_out, state_sem.at[0, 0]), pltpu.make_async_copy(down_state, down_out, state_sem.at[0, 1])]
    for copy in state_stores:
        copy.start()

    def spot(coords, colour, side):
        lane = slice(None) if side is None else pl.ds(half * side, half)
        index = [slice(None), slice(None), slice(None), slice(None), core, pl.ds(CHUNK * colour, CHUNK), lane]
        for axis, coord in coords.items():
            index[1 + axis] = coord
        return w_out.at[tuple(index)]

    handed = []

    def hand(ref, slot):
        copy = remote(ref, ref, out_s.at[slot], out_r.at[slot], partner)
        copy.start()
        handed.append(copy)

    for level in (2, 1, 0):
        if level == 1:
            keep.wait()

        def where(colour, coord):
            order = ORDERS[colour]
            coords = {axis: pos[axis] for axis in order[:level]}
            coords[order[level]] = coord
            return coords

        def near(colour, side):
            axis = ORDERS[colour][level]
            coord = step(axis, 1 if side == 0 else 3)
            return coord, device(axis, coord)

        copies = {}
        for kind in range(2):
            for colour in range(3):
                for side in range(2):
                    lane_side = side if kind == 0 else 1 - side
                    dst = spot(where(colour, pos[ORDERS[colour][level]]), colour, lane_side)
                    src = w_own.at[:, pl.ds(CHUNK * colour, CHUNK), pl.ds(half * lane_side, half)] if level == 2 else dst
                    copy = remote(src, dst, ag_s.at[level, colour, side, kind], ag_r.at[level, colour, side, kind], near(colour, side)[1])
                    copy.start()
                    copies[colour, side, kind] = copy
        if level == 0:
            for colour in range(3):
                hand(spot(where(colour, pos[ORDERS[colour][0]]), colour, None), 5 * colour)
        for colour in range(3):
            for side in range(2):
                back = near(colour, 1 - side)[0]
                copies[colour, side, 0].wait_recv()
                ref = spot(where(colour, back), colour, side)
                copy = remote(ref, ref, ag_s.at[level, colour, side, 2], ag_r.at[level, colour, side, 2], near(colour, side)[1])
                copy.start()
                copies[colour, side, 2] = copy
        for colour in range(3):
            for side in range(2):
                copies[colour, side, 1].wait_recv()
                if level == 0:
                    hand(spot(where(colour, near(colour, 1 - side)[0]), colour, None), 5 * colour + 1 + side)
        for colour in range(3):
            for side in range(2):
                copies[colour, side, 2].wait_recv()
                if level == 0:
                    hand(spot(where(colour, step(ORDERS[colour][0], 2)), colour, side), 5 * colour + 3 + side)
        sends = sends + list(copies.values())
    for phase in list(first.values()) + [second, third]:
        phase.drain()
    for mat in mat_order:
        for copy in pairs[mat]:
            copy.wait_send()
    for copy in sends:
        copy.wait_send()
    for copy in handed + state_stores:
        copy.wait()


def place_kernel(lanes, w_ref, up_ref, down_ref, norm_ref, *refs):
    weights, states, norm_out, (w_tmp, up_tmp, down_tmp, in_sem, state_in, out_sem, state_out) = refs[:4], refs[4:16], refs[16], refs[17:]
    norm_out[0] = jnp.max(norm_ref[...])
    loads = [[pltpu.make_async_copy(w_ref.at[mat, z], w_tmp.at[mat, z], in_sem.at[mat, z]) for z in range(4)] for mat in range(4)]
    for row in loads:
        for copy in row:
            copy.start()
    state_loads = [pltpu.make_async_copy(up_ref, up_tmp, state_in.at[0]), pltpu.make_async_copy(down_ref, down_tmp, state_in.at[1])]
    for copy in state_loads:
        copy.start()
    stores = []
    for mat in range(4):
        for z in range(4):
            loads[mat][z].wait()
            if mat % 2:
                copies = [pltpu.make_async_copy(w_tmp.at[mat, z], weights[mat].at[z], out_sem.at[mat, z, 0])]
            else:
                copies = []
                for member in range(4):
                    src = w_tmp.at[mat, z, :, :, member // 2, member % 2]
                    copies.append(pltpu.make_async_copy(src, weights[mat].at[z, :, :, :, pl.ds(member * lanes, lanes)], out_sem.at[mat, z, member]))
            for copy in copies:
                copy.start()
            stores = stores + copies
    for copy in state_loads:
        copy.wait()
    for field in range(3):
        for mat in range(4):
            src = (down_tmp if mat % 2 else up_tmp).at[field, mat // 2]
            copy = pltpu.make_async_copy(src, states[4 * field + mat], state_out.at[field, mat])
            copy.start()
            stores.append(copy)
    for copy in stores:
        copy.wait()


def comm_call(lanes, grads, masters, moms, vels, learn_rate, clip_norm):
    up = (4, 4, 2, ROWS, 4 * lanes)
    down = (4, 4, 4, 2, ROWS, lanes)
    grads = [grads[0].reshape(up), grads[1].reshape(down), grads[2].reshape(up), grads[3].reshape(down)]
    half = lanes // 2
    f32 = jnp.float32
    bf16 = jnp.bfloat16
    up_shape = (3, 2, SUB, 4 * lanes)
    down_shape = (3, 2, ROWS, lanes)
    dma = pltpu.SemaphoreType.DMA
    vmem = pl.BlockSpec(memory_space=pltpu.VMEM)
    smem = pl.BlockSpec(memory_space=pltpu.SMEM)
    hbm = pl.BlockSpec(memory_space=pl.ANY)
    scratch = [
        pltpu.VMEM((4, 4, 4, 4, ROWS, lanes), f32),
        pltpu.VMEM((4, 4, 4, 4, ROWS, lanes), f32),
        pltpu.VMEM((4, 3, 2, 3, 4, 4, CHUNK, half), f32),
        pltpu.VMEM((3, 2, 3, 4, 4, CHUNK, half), f32),
        pltpu.VMEM((3, 2, 3, 4, CHUNK, half), f32),
        pltpu.VMEM((2, 8, min(lanes, 128)), f32),
        pltpu.VMEM((3, 4, 8, min(lanes, 128)), f32),
        pltpu.VMEM((4, 2, SUB, lanes), f32),
        pltpu.VMEM((4, 2, SUB, lanes), f32),
        pltpu.VMEM((4, 2, SUB, lanes), f32),
        pltpu.VMEM((4, 2, SUB, lanes), f32),
        pltpu.VMEM((ROWS, lanes), f32),
        pltpu.VMEM((4, ROWS, lanes), jnp.bfloat16),
        pltpu.VMEM(up_shape, f32),
        pltpu.VMEM(down_shape, f32),
        dma((4, 4)), dma((3, 4)), dma((4, 4)), dma((4, 4)),
        dma((4, 3, 2, 3)), dma((4, 3, 2, 3)), dma((3, 2, 3)), dma((3, 2, 3)), dma((3, 2, 3)), dma((3, 2, 3)),
        dma((1,)), dma((1,)), dma((3, 3)), dma((3, 3)), dma((3,)), dma((3,)), dma((3,)), dma((3,)),
        dma, dma((3, 3, 2, 3)), dma((3, 3, 2, 3)), dma((15,)), dma((15,)),
    ]
    outs = pl.pallas_call(
        functools.partial(comm_kernel, lanes),
        name="reduce_update_gather",
        out_shape=[jax.ShapeDtypeStruct((4, 4, 4, 4, 2, ROWS, lanes), bf16), jax.ShapeDtypeStruct(up_shape, f32), jax.ShapeDtypeStruct(down_shape, f32), jax.ShapeDtypeStruct((8, 128), f32)],
        in_specs=[hbm] * 16 + [smem] * 2,
        out_specs=[hbm] * 3 + [vmem],
        scratch_shapes=scratch,
        compiler_params=pltpu.CompilerParams(collective_id=0, has_side_effects=True, vmem_limit_bytes=67043328),
    )(*grads, *masters, *moms, *vels, learn_rate.reshape(1), clip_norm.reshape(1))
    split = (4, 4, 2, 2, 2, ROWS, lanes)
    placed = pl.pallas_call(
        functools.partial(place_kernel, lanes),
        name="place_outputs",
        out_shape=[jax.ShapeDtypeStruct(split if mat % 2 else up, bf16) for mat in range(4)] + [jax.ShapeDtypeStruct(m.shape, f32) for m in masters] * 3 + [jax.ShapeDtypeStruct((1,), f32)],
        in_specs=[hbm] * 3 + [vmem],
        out_specs=[hbm] * 16 + [smem],
        scratch_shapes=[
            pltpu.VMEM((4,) + split, bf16), pltpu.VMEM(up_shape, f32), pltpu.VMEM(down_shape, f32),
            dma((4, 4)), dma((2,)), dma((4, 4, 4)), dma((3, 4)),
        ],
        compiler_params=pltpu.CompilerParams(vmem_limit_bytes=50 * 1024 * 1024),
    )(outs[0].reshape((4,) + split), *outs[1:])
    weights = [placed[mat].reshape(masters[mat].shape[0] * 128, -1) for mat in range(4)]
    return tuple(weights) + tuple(placed[4:16]) + (placed[16][0],)


def mat_nt(left, right):
    return lax.dot_general(left, right, (((1,), (1,)), ((), ())), preferred_element_type=jnp.float32)


def mat_tn(left, right):
    return lax.dot_general(left, right, (((0,), (0,)), ((), ())), preferred_element_type=jnp.float32)


def gelu_pair(pre):
    normal_cdf = 0.5 * (1.0 + lax.erf(pre * ROOT_HALF))
    density = jnp.exp(-0.5 * pre * pre) * INV_ROOT_TAU
    return pre * normal_cdf, normal_cdf + pre * density


def fwd_bwd(rows_in, rows_grad, w_up1, w_down1, w_up2, w_down2):
    pre_up1 = jnp.dot(rows_in, w_up1, preferred_element_type=jnp.float32)
    gel_up1, der_up1 = gelu_pair(pre_up1)
    act_up1 = gel_up1.astype(jnp.bfloat16)
    mid_act = jnp.dot(act_up1, w_down1, preferred_element_type=jnp.float32).astype(jnp.bfloat16)
    pre_up2 = jnp.dot(mid_act, w_up2, preferred_element_type=jnp.float32)
    gel_up2, der_up2 = gelu_pair(pre_up2)
    act_up2 = gel_up2.astype(jnp.bfloat16)
    grad_act2 = mat_nt(rows_grad, w_down2).astype(jnp.bfloat16)
    grad_pre2 = (grad_act2.astype(jnp.float32) * der_up2).astype(jnp.bfloat16)
    grad_mid = mat_nt(grad_pre2, w_up2).astype(jnp.bfloat16)
    grad_act1 = mat_nt(grad_mid, w_down1).astype(jnp.bfloat16)
    grad_pre1 = (grad_act1.astype(jnp.float32) * der_up1).astype(jnp.bfloat16)
    return ((rows_in, grad_pre1), (act_up1, grad_mid), (mid_act, grad_pre2), (act_up2, rows_grad))


def solution(mesh):
    rows_spec = P("data", None)
    full_spec = P(None, None)
    scalar_spec = P()

    def shard_body(act_in, grad_out, w_up1, w_down1, w_up2, w_down2, *rest):
        pairs = fwd_bwd(act_in, grad_out, w_up1, w_down1, w_up2, w_down2)
        grads = [mat_tn(left, right) for left, right in pairs]
        return comm_call(768, grads, rest[0:4], rest[4:8], rest[8:12], rest[12], rest[13])

    in_specs = (rows_spec, rows_spec) + (full_spec,) * 4 + (rows_spec,) * 12 + (scalar_spec, scalar_spec)
    out_specs = (full_spec,) * 4 + (rows_spec,) * 12 + (scalar_spec,)
    return jax.shard_map(shard_body, mesh=mesh, in_specs=in_specs, out_specs=out_specs, check_vma=False)
```

```python
import functools
import math
import jax
import jax.numpy as jnp
from jax import lax
from jax.experimental import pallas as pl
from jax.experimental.pallas import tpu as pltpu
from jax.sharding import PartitionSpec as P

STEP = 20
BETA_ONE = 0.9
BETA_TWO = 0.95
EPSILON = 1e-8
NORM_EPS = 1e-6
CORR_ONE = 1.0 - BETA_ONE ** STEP
CORR_TWO = 1.0 - BETA_TWO ** STEP
ROOT_HALF = math.sqrt(0.5)
INV_ROOT_TAU = 1.0 / math.sqrt(2.0 * math.pi)

MESH = pl.DeviceIdType.MESH
STRIDES = (32, 8, 2)
ORDERS = ((2, 1, 0), (1, 0, 2), (0, 2, 1))
ROWS = 24
SUB = 6
CHUNK = 8
SIDE = 4
COLOURS = 3
SIDES = 2
ALL = slice(None)
TILE = 512


def adam_step(scaled, master_old, mom_old, vel_old, learn_rate):
    mom_new = BETA_ONE * mom_old + (1.0 - BETA_ONE) * scaled
    vel_new = BETA_TWO * vel_old + (1.0 - BETA_TWO) * scaled * scaled
    master_new = master_old - learn_rate * (mom_new / CORR_ONE) / (jnp.sqrt(vel_new / CORR_TWO) + EPSILON)
    return master_new, mom_new, vel_new


def comm_kernel(lanes, *refs):
    (g_down2, grad_rows, mid_rows, in_rows, w_down1, w_up2, w_down2, der1, der2, act1), refs = refs[:10], refs[10:]
    states, refs = refs[:12], refs[12:]
    (lr_ref, clip_ref), refs = refs[:2], refs[2:]
    (w_out, up_out, down_out, norm_out, g_up1, g_down1, g_up2), refs = refs[:7], refs[7:]
    (total, peer_in, rs1, rs2, rs3, norm_core, norm_axis, send_g, recv_g, send_w, recv_w, block_tmp, w_own, up_state, down_state), refs = refs[:15], refs[15:]
    (left, flipped, mid_acc, mid_grad, w_tile, act_tile, der_tile, out_tile), refs = refs[:8], refs[8:]
    (load_sem, state_sem, pair_s, pair_r, rs1_s, rs1_r, rs2_s, rs2_r, rs3_s, rs3_r, nc_s, nc_r, na_s, na_r, xg_s, xg_r, xw_s, xw_r, own_sem, ag_s, ag_r, out_s, out_r) = refs[:23]
    row_sem, tile_sem, store_sem, pair_credit, ring_credit = refs[23:]
    half = lanes // 2
    me = lax.axis_index("data")
    core = lax.rem(me, SIDES)
    member = lax.rem(me, 4)
    pos = (me // 32, lax.rem(me // 8, 4), lax.rem(me // 2, 4))
    partner = me + 1 - 2 * core

    def device(axis, coord):
        return me + (coord - pos[axis]) * STRIDES[axis]

    def step(axis, hops):
        return lax.rem(pos[axis] + hops, 4)

    def remote(src, dst, send_sem, recv_sem, target):
        return pltpu.make_async_remote_copy(src_ref=src, dst_ref=dst, send_sem=send_sem, recv_sem=recv_sem, device_id=(target,), device_id_type=MESH)

    peers = [partner] + [device(axis, step(axis, hops)) for axis in range(COLOURS) for hops in (1, 2, 3)]
    peers.append(me - member + lax.rem(member + 2, 4) + 1 - 2 * core)
    barrier = pltpu.get_barrier_semaphore()
    for peer in peers:
        pl.semaphore_signal(barrier, device_id=(peer,), device_id_type=MESH)

    grads = (g_up1, g_down1, g_up2, g_down2)
    mat_order = (3, 2, 1, 0)
    pair_slot = (1, 0, 1, 0)
    loads, pairs = {0: [], 2: []}, {0: [], 2: []}

    def issue_up(mat, x_low):
        for x in (x_low, x_low + 2):
            for owner in (1 - core, core):
                col = pl.multiple_of((x_low * 2 + owner) * lanes, lanes)
                src = grads[mat].at[:, :, x // SIDES, :, pl.ds(col, lanes)]
                if owner is core:
                    loads[mat].append(pltpu.make_async_copy(src, total.at[mat, :, :, x], load_sem.at[mat, x]))
                    loads[mat][-1].start()
                else:
                    pairs[mat].append(remote(src, peer_in.at[pair_slot[mat], :, :, x], pair_s.at[mat, x], pair_r.at[mat, x], partner))
                    pairs[mat][-1].start()

    def issue_rows(low, high):
        def move(i, carry):
            place = (i // 16, lax.rem(i // SIDE, 4), lax.rem(i, SIDE))
            there = g_down1.at[pl.ds(pl.multiple_of(i * 2 * ROWS + (1 - core) * ROWS, 8), ROWS)]
            here = g_down1.at[pl.ds(pl.multiple_of(i * 2 * ROWS + core * ROWS, 8), ROWS)]
            remote(there, peer_in.at[(pair_slot[1],) + place], pair_s.at[1, 0], pair_r.at[1, 0], partner).start()
            pltpu.make_async_copy(here, total.at[(1,) + place], load_sem.at[1, 0]).start()
            return carry

        lax.fori_loop(low, high, move, 0)

    loads[1] = [pltpu.make_async_copy(total.at[1], total.at[1], load_sem.at[1, 0])]
    pairs[1] = [remote(peer_in.at[pair_slot[1]], peer_in.at[pair_slot[1]], pair_s.at[1, 0], pair_r.at[1, 0], partner)]
    loads[3] = [pltpu.make_async_copy(g_down2.at[:, :, :, core], total.at[3], load_sem.at[3, 0])]
    loads[3][0].start()

    tiles = SIDE * lanes // TILE

    def span(t):
        return pl.ds(pl.multiple_of(t * TILE, TILE), TILE)

    def fetch_a(t, slot):
        return [
            pltpu.make_async_copy(w_down2.at[span(t)], w_tile.at[slot], tile_sem.at[slot, 0]),
            pltpu.make_async_copy(w_up2.at[:, span(t)], act_tile.at[slot, pl.ds(0, lanes)], tile_sem.at[slot, 1]),
            pltpu.make_async_copy(der2.at[:, span(t)], der_tile.at[slot], tile_sem.at[slot, 2]),
        ]

    def fetch_b(t, slot):
        return [
            pltpu.make_async_copy(w_down1.at[span(t)], w_tile.at[slot], tile_sem.at[slot, 0]),
            pltpu.make_async_copy(act1.at[:, span(t)], act_tile.at[slot], tile_sem.at[slot, 1]),
            pltpu.make_async_copy(der1.at[:, span(t)], der_tile.at[slot], tile_sem.at[slot, 2]),
        ]

    def begin(copies):
        for copy in copies:
            copy.start()

    def end(copies):
        for copy in copies:
            copy.wait()

    row_loads = [pltpu.make_async_copy(grad_rows, left, row_sem.at[0]), pltpu.make_async_copy(mid_rows, mid_grad, row_sem.at[1])]
    begin(row_loads)
    begin(fetch_a(0, 0))
    state_loads = []
    for field in range(COLOURS):
        for mat in range(SIDE):
            dst = (down_state if mat % SIDES else up_state).at[field, mat // SIDES]
            state_loads.append(pltpu.make_async_copy(states[4 * field + mat], dst, state_sem.at[field, mat]))
    begin(state_loads)
    def store_a(t, slot):
        return [pltpu.make_async_copy(out_tile.at[slot], g_up2.at[:, :, :, :, span(t)], store_sem.at[slot, 0])]

    def store_b(t, slot):
        return [
            pltpu.make_async_copy(out_tile.at[slot], g_up1.at[:, :, :, :, span(t)], store_sem.at[slot, 0]),
            pltpu.make_async_copy(mid_acc.at[slot], g_down1.at[span(t)], store_sem.at[slot, 1]),
        ]

    def run(first, last, fetch, store, work):
        def tile(t, carry):
            slot = lax.rem(t, SIDES)

            @pl.when(t + 1 < tiles)
            def _():
                begin(fetch(t + 1, 1 - slot))

            end(fetch(t, slot))

            @pl.when(t - first >= 2)
            def _():
                end(store(t - 2, slot))

            work(slot)
            begin(store(t, slot))
            return carry

        lax.fori_loop(first, last, tile, 0)
        for t in range(max(first, last - 2), last):
            end(store(t, t % 2))

    def dot(lhs, rhs, lhs_dim, rhs_dim):
        return lax.dot_general(lhs, rhs, (((lhs_dim,), (rhs_dim,)), ((), ())), preferred_element_type=jnp.float32)

    def work_a(slot):
        grad_act2 = dot(left[...], w_tile[slot], 1, 1).astype(jnp.bfloat16)
        grad_pre2 = (grad_act2.astype(jnp.float32) * der_tile[slot]).astype(jnp.bfloat16)
        out_tile[slot] = dot(flipped[...], grad_pre2, 1, 0).reshape(out_tile.shape[1:])
        mid_acc[...] += dot(grad_pre2, act_tile[slot, pl.ds(0, lanes)], 1, 1).reshape(mid_acc.shape)

    def work_b(slot):
        mid_acc[slot] = dot(act_tile[slot], mid_grad[...], 0, 0)
        grad_act1 = dot(mid_grad[...], w_tile[slot], 1, 1).astype(jnp.bfloat16)
        grad_pre1 = (grad_act1.astype(jnp.float32) * der_tile[slot]).astype(jnp.bfloat16)
        out_tile[slot] = dot(flipped[...], grad_pre1, 1, 0).reshape(out_tile.shape[1:])

    end(row_loads)
    flipped[...] = mid_grad[...].T
    mid_acc[...] = jnp.zeros_like(mid_acc)
    run(0, 1, fetch_a, store_a, work_a)
    pl.semaphore_wait(barrier, len(peers))
    pairs[3] = [remote(g_down2.at[:, :, :, 1 - core], peer_in.at[pair_slot[3]], pair_s.at[3, 0], pair_r.at[3, 0], partner)]
    pairs[3][0].start()

    def part(mats, coords, colour, side):
        index = [mats, ALL, ALL, ALL, pl.ds(CHUNK * colour, CHUNK), pl.ds(half * side, half)]
        for axis, coord in coords.items():
            index[1 + axis] = coord
        return tuple(index)

    class Phase:
        def __init__(self, level, base, buf, send_sem, recv_sem):
            self.level, self.base, self.buf, self.send_sem, self.recv_sem = level, base, buf, send_sem, recv_sem
            self.mats, self.count = (slice(base, base + 2), 2) if level else (base, 4)
            self.copies = {}

        def where(self, colour, coord):
            order = ORDERS[colour]
            coords = {axis: pos[axis] for axis in order[:self.level]}
            coords[order[self.level]] = coord
            return coords

        def row(self, colour, coord, side, i):
            coords = self.where(colour, coord)
            if self.level:
                return part(self.base + i, coords, colour, side)
            coords[min(axis for axis in range(COLOURS) if axis not in coords)] = i
            return part(self.mats, coords, colour, side)

        def send(self, colour, side, kind, src, target):
            copy = remote(src, self.buf.at[colour, side, kind], self.send_sem.at[colour, side, kind], self.recv_sem.at[colour, side, kind], target)
            copy.start()
            self.copies[colour, side, kind] = copy

        def near(self, colour, side):
            axis = ORDERS[colour][self.level]
            coord = step(axis, 1 if side == 0 else 3)
            return coord, device(axis, coord)

        def start(self):
            for kind in range(SIDES):
                for colour in range(COLOURS):
                    for side in range(SIDES):
                        coord, target = self.near(colour, side)
                        aim = step(ORDERS[colour][self.level], 2) if kind == 0 else coord
                        src = total.at[part(self.mats, self.where(colour, aim), colour, side if kind == 0 else 1 - side)]
                        self.send(colour, side, kind, src, target)

        def forward(self):
            for colour in range(COLOURS):
                for side in range(SIDES):
                    coord, target = self.near(colour, side)
                    self.copies[colour, side, 0].wait_recv()

                    def add_own(i, carry, colour=colour, side=side, coord=coord):
                        self.buf[colour, side, 0, i] = self.buf[colour, side, 0, i] + total[self.row(colour, coord, side, i)]
                        return carry

                    lax.fori_loop(0, self.count, add_own, 0)
                    self.send(colour, side, 2, self.buf.at[colour, side, 0], target)

        def finish(self):
            for colour in range(COLOURS):
                for side in range(SIDES):
                    self.copies[colour, 1 - side, 1].wait_recv()
                    self.copies[colour, side, 2].wait_recv()

                    def add_both(i, carry, colour=colour, side=side):
                        own = self.row(colour, pos[ORDERS[colour][self.level]], side, i)
                        total[own] = total[own] + (self.buf[colour, 1 - side, 1, i] + self.buf[colour, side, 2, i])
                        return carry

                    lax.fori_loop(0, self.count, add_both, 0)

        def drain(self):
            for copy in self.copies.values():
                copy.wait_send()

    ring_slot = (1, 0, 1, 0)
    first = {mat: Phase(0, mat, rs1.at[ring_slot[mat]], rs1_s.at[mat], rs1_r.at[mat]) for mat in mat_order}

    def add_pair(mat):
        end(loads[mat])
        for copy in pairs[mat]:
            copy.wait_recv()

        def add(i, carry):
            total[mat, i // SIDE, lax.rem(i, SIDE)] = total[mat, i // SIDE, lax.rem(i, SIDE)] + peer_in[pair_slot[mat], i // SIDE, lax.rem(i, SIDE)]
            return carry

        lax.fori_loop(0, 16, add, 0)
        if mat >= 2:
            pl.semaphore_signal(pair_credit, device_id=(partner,), device_id_type=MESH)

    ring = [device(axis, step(axis, hops)) for axis in range(COLOURS) for hops in (1, 3)]

    def close(mat):
        first[mat].finish()
        first[mat].drain()
        for peer in ring:
            pl.semaphore_signal(ring_credit.at[ring_slot[mat]], device_id=(peer,), device_id_type=MESH)

    second = {base: Phase(1, base, rs2.at[base // 2], rs2_s.at[base // 2], rs2_r.at[base // 2]) for base in (2, 0)}
    third = {base: Phase(2, base, rs3.at[base // 2], rs3_s.at[base // 2], rs3_r.at[base // 2]) for base in (2, 0)}
    run(1, 4, fetch_a, store_a, work_a)
    add_pair(3)
    first[3].start()
    issue_up(2, 0)
    run(4, tiles, fetch_a, store_a, work_a)
    issue_up(2, 1)
    begin(fetch_b(0, 0))
    in_load = pltpu.make_async_copy(in_rows, left, row_sem.at[0])
    in_load.start()
    first[3].forward()
    mid_grad[...] = mid_acc[...].reshape(mid_grad.shape).astype(jnp.bfloat16)
    in_load.wait()
    flipped[...] = left[...].T
    run(0, 2, fetch_b, store_b, work_b)
    add_pair(2)
    first[2].start()
    run(2, 4, fetch_b, store_b, work_b)
    first[2].forward()
    pl.semaphore_wait(pair_credit, 1)
    issue_rows(0, 32)
    pl.semaphore_wait(pair_credit, 1)
    issue_up(0, 0)
    close(3)
    run(4, tiles, fetch_b, store_b, work_b)
    issue_rows(32, 64)
    issue_up(0, 1)
    close(2)
    second[2].start()
    add_pair(1)
    pl.semaphore_wait(ring_credit.at[0], len(ring))
    first[1].start()
    second[2].forward()
    add_pair(0)
    pl.semaphore_wait(ring_credit.at[1], len(ring))
    first[0].start()
    second[2].finish()
    third[2].start()
    first[1].forward()
    third[2].forward()
    first[1].finish()
    third[2].finish()
    first[0].forward()
    first[0].finish()
    second[0].start()
    second[0].forward()
    second[0].finish()
    third[0].start()
    third[0].forward()
    third[0].finish()

    group_scale = 1.0 / 128.0
    grad_own = [total[mat, pos[0], pos[1], pos[2]] * group_scale for mat in range(SIDE)]
    partial = None
    for block in grad_own:
        square = block * block
        for row in range(ROWS // 8):
            for col in range(max(1, lanes // 128)):
                tile = square[8 * row:8 * row + 8, 128 * col:128 * col + 128]
                partial = tile if partial is None else partial + tile
    norm_core[core] = partial
    swap = remote(norm_core.at[core], norm_core.at[core], nc_s.at[0], nc_r.at[0], partner)
    swap.start()
    for target in range(SIDE):
        for i, mat in enumerate((0, 2)):
            send_g[target, i] = grad_own[mat][SUB * target:SUB * target + SUB]
    moves = []
    for hops in range(1, SIDE):
        other = lax.rem(member + hops, SIDE)
        copy = remote(send_g.at[other], recv_g.at[member], xg_s.at[hops - 1], xg_r.at[hops - 1], me - member + other)
        copy.start()
        moves.append(copy)
    recv_g[member] = send_g[member]
    swap.wait_recv()
    running = norm_core[0] + norm_core[1]
    sends = [swap] + moves
    for axis in (2, 1, 0):
        norm_axis[axis, pos[axis]] = running
        copies = []
        for hops in (1, 2, 3):
            coord = step(axis, hops)
            copy = remote(norm_axis.at[axis, pos[axis]], norm_axis.at[axis, pos[axis]], na_s.at[axis, hops - 1], na_r.at[axis, hops - 1], device(axis, coord))
            copy.start()
            copies.append(copy)
        for copy in copies:
            copy.wait_recv()
        sends = sends + copies
        running = (norm_axis[axis, 0] + norm_axis[axis, 1]) + (norm_axis[axis, 2] + norm_axis[axis, 3])
    norm = jnp.sqrt(jnp.sum(jnp.sum(running, axis=1, keepdims=True), axis=0, keepdims=True))
    norm_out[...] = jnp.broadcast_to(norm, norm_out.shape)
    clip_scale = jnp.minimum(1.0, clip_ref[0] / (norm + NORM_EPS))
    learn_rate = lr_ref[0]

    end(state_loads)
    for i in range(SIDES):
        fresh = adam_step(grad_own[2 * i + 1] * clip_scale, down_state[0, i], down_state[1, i], down_state[2, i], learn_rate)
        for field in range(COLOURS):
            down_state[field, i] = fresh[field]
        w_own[2 + i] = fresh[0].astype(jnp.bfloat16)

    def spot(group, coords, colour, side):
        lane = ALL if side is None else pl.ds(half * side, half)
        index = [pl.ds(2 * group, 2), ALL, ALL, ALL, core, pl.ds(CHUNK * colour, CHUNK), lane]
        for axis, coord in coords.items():
            index[1 + axis] = coord
        return w_out.at[tuple(index)]

    handed = []

    class Gather:
        def __init__(self, group, level):
            self.group, self.level = group, level
            self.copies = {}

        def spot(self, colour, coord, side):
            order = ORDERS[colour]
            coords = {axis: pos[axis] for axis in order[:self.level]}
            coords[order[self.level]] = coord
            return spot(self.group, coords, colour, side)

        def near(self, colour, side):
            axis = ORDERS[colour][self.level]
            coord = step(axis, 1 if side == 0 else 3)
            return coord, device(axis, coord)

        def send(self, colour, side, kind, src, dst):
            spots = (self.group, self.level, colour, side, kind)
            copy = remote(src, dst, ag_s.at[spots], ag_r.at[spots], self.near(colour, side)[1])
            copy.start()
            self.copies[colour, side, kind] = copy

        def hand(self, ref, slot):
            copy = remote(ref, ref, out_s.at[self.group, slot], out_r.at[self.group, slot], partner)
            copy.start()
            handed.append(copy)

        def start(self):
            for kind in range(SIDES):
                for colour in range(COLOURS):
                    for side in range(SIDES):
                        lane_side = side if kind == 0 else 1 - side
                        dst = self.spot(colour, pos[ORDERS[colour][self.level]], lane_side)
                        src = dst
                        if self.level == 2:
                            src = w_own.at[pl.ds(2 * self.group, 2), pl.ds(CHUNK * colour, CHUNK), pl.ds(half * lane_side, half)]
                        self.send(colour, side, kind, src, dst)
            if self.level == 0:
                for colour in range(COLOURS):
                    self.hand(self.spot(colour, pos[ORDERS[colour][0]], None), 5 * colour)

        def forward(self):
            for colour in range(COLOURS):
                for side in range(SIDES):
                    self.copies[colour, side, 0].wait_recv()
                    ref = self.spot(colour, self.near(colour, 1 - side)[0], side)
                    self.send(colour, side, 2, ref, ref)

        def finish(self):
            for colour in range(COLOURS):
                for side in range(SIDES):
                    self.copies[colour, side, 1].wait_recv()
                    if self.level == 0:
                        self.hand(self.spot(colour, self.near(colour, 1 - side)[0], None), 5 * colour + 1 + side)
            for colour in range(COLOURS):
                for side in range(SIDES):
                    self.copies[colour, side, 2].wait_recv()
                    if self.level == 0:
                        self.hand(self.spot(colour, step(ORDERS[colour][0], 2), side), 5 * colour + 3 + side)

    keeps = [pltpu.make_async_copy(w_own.at[pl.ds(2 * group, 2)], w_out.at[pl.ds(2 * group, 2), pos[0], pos[1], pos[2], core], own_sem.at[group]) for group in range(SIDES)]
    gathers = {(group, level): Gather(group, level) for group in range(SIDES) for level in range(COLOURS)}
    gathers[1, 2].start()
    keeps[1].start()

    for copy in moves:
        copy.wait_recv()
    for i in range(SIDES):
        for col in range(SIDE):
            cols = slice(col * lanes, (col + 1) * lanes)
            scaled = recv_g[col, i] * clip_scale
            fresh = adam_step(scaled, up_state[0, i, :, cols], up_state[1, i, :, cols], up_state[2, i, :, cols], learn_rate)
            for field in range(COLOURS):
                up_state[field, i, :, cols] = fresh[field]
            send_w[col, i] = fresh[0]
    moves = []
    for hops in range(1, SIDE):
        other = lax.rem(member + hops, SIDE)
        copy = remote(send_w.at[other], recv_w.at[member], xw_s.at[hops - 1], xw_r.at[hops - 1], me - member + other)
        copy.start()
        moves.append(copy)
    recv_w[member] = send_w[member]
    state_stores = [pltpu.make_async_copy(up_state, up_out, state_sem.at[0, 0]), pltpu.make_async_copy(down_state, down_out, state_sem.at[0, 1])]
    begin(state_stores)
    gathers[1, 2].forward()
    for copy in moves:
        copy.wait_recv()
    sends = sends + moves
    for i in range(SIDES):
        for source in range(SIDE):
            block_tmp[SUB * source:SUB * source + SUB] = recv_w[source, i]
        w_own[i] = block_tmp[...].astype(jnp.bfloat16)
    gathers[0, 2].start()
    keeps[0].start()
    gathers[1, 2].finish()
    keeps[1].wait()
    gathers[1, 1].start()
    gathers[0, 2].forward()
    gathers[1, 1].forward()
    gathers[0, 2].finish()
    keeps[0].wait()
    gathers[0, 1].start()
    gathers[1, 1].finish()
    gathers[1, 0].start()
    gathers[0, 1].forward()
    gathers[0, 1].finish()
    gathers[0, 0].start()
    gathers[1, 0].forward()
    gathers[0, 0].forward()
    gathers[1, 0].finish()
    gathers[0, 0].finish()
    for gather in gathers.values():
        sends = sends + list(gather.copies.values())
    for phase in [first[1], first[0]] + list(second.values()) + list(third.values()):
        phase.drain()
    for mat in mat_order:
        for copy in pairs[mat]:
            copy.wait_send()
    for copy in sends:
        copy.wait_send()
    for copy in handed + state_stores:
        copy.wait()


def place_kernel(lanes, w_ref, up_ref, down_ref, norm_ref, *refs):
    weights, states, norm_out, (w_tmp, up_tmp, down_tmp, in_sem, state_in, out_sem, state_out) = refs[:4], refs[4:16], refs[16], refs[17:]
    norm_out[0] = jnp.max(norm_ref[...])
    loads = [[pltpu.make_async_copy(w_ref.at[mat % SIDES * 2 + mat // SIDES, z], w_tmp.at[mat, z], in_sem.at[mat, z]) for z in range(SIDE)] for mat in range(SIDE)]
    for row in loads:
        for copy in row:
            copy.start()
    state_loads = [pltpu.make_async_copy(up_ref, up_tmp, state_in.at[0]), pltpu.make_async_copy(down_ref, down_tmp, state_in.at[1])]
    for copy in state_loads:
        copy.start()
    stores = []
    for mat in range(SIDE):
        for z in range(SIDE):
            loads[mat][z].wait()
            if mat % SIDES:
                copies = [pltpu.make_async_copy(w_tmp.at[mat, z], weights[mat].at[z], out_sem.at[mat, z, 0])]
            else:
                copies = []
                for member in range(SIDE):
                    src = w_tmp.at[mat, z, :, :, member // SIDES, member % SIDES]
                    copies.append(pltpu.make_async_copy(src, weights[mat].at[z, :, :, :, pl.ds(member * lanes, lanes)], out_sem.at[mat, z, member]))
            for copy in copies:
                copy.start()
            stores = stores + copies
    for copy in state_loads:
        copy.wait()
    for field in range(COLOURS):
        for mat in range(SIDE):
            src = (down_tmp if mat % SIDES else up_tmp).at[field, mat // SIDES]
            copy = pltpu.make_async_copy(src, states[4 * field + mat], state_out.at[field, mat])
            copy.start()
            stores.append(copy)
    for copy in stores:
        copy.wait()


def comm_call(lanes, grad_down2, rows, weights_in, hidden, masters, moms, vels, learn_rate, clip_norm):
    up = (SIDE, SIDE, SIDES, ROWS, SIDE * lanes)
    down = (SIDE, SIDE, SIDE, SIDES, ROWS, lanes)
    local_rows = rows[0].shape[0]
    half = lanes // 2
    f32 = jnp.float32
    bf16 = jnp.bfloat16
    up_shape = (COLOURS, SIDES, SUB, SIDE * lanes)
    down_shape = (COLOURS, SIDES, ROWS, lanes)
    dma = pltpu.SemaphoreType.DMA
    vmem = pl.BlockSpec(memory_space=pltpu.VMEM)
    smem = pl.BlockSpec(memory_space=pltpu.SMEM)
    hbm = pl.BlockSpec(memory_space=pl.ANY)
    scratch = [
        pltpu.VMEM((SIDE, SIDE, SIDE, SIDE, ROWS, lanes), f32),
        pltpu.VMEM((SIDES, SIDE, SIDE, SIDE, ROWS, lanes), f32),
        pltpu.VMEM((SIDES, COLOURS, SIDES, COLOURS, SIDE, SIDE, CHUNK, half), f32),
        pltpu.VMEM((SIDES, COLOURS, SIDES, COLOURS, SIDES, SIDE, CHUNK, half), f32),
        pltpu.VMEM((SIDES, COLOURS, SIDES, COLOURS, SIDES, CHUNK, half), f32),
        pltpu.VMEM((2, 8, min(lanes, 128)), f32),
        pltpu.VMEM((3, 4, 8, min(lanes, 128)), f32),
        pltpu.VMEM((SIDE, SIDES, SUB, lanes), f32),
        pltpu.VMEM((SIDE, SIDES, SUB, lanes), f32),
        pltpu.VMEM((SIDE, SIDES, SUB, lanes), f32),
        pltpu.VMEM((SIDE, SIDES, SUB, lanes), f32),
        pltpu.VMEM((ROWS, lanes), f32),
        pltpu.VMEM((SIDE, ROWS, lanes), jnp.bfloat16),
        pltpu.VMEM(up_shape, f32),
        pltpu.VMEM(down_shape, f32),
        pltpu.VMEM((local_rows, lanes), bf16),
        pltpu.VMEM((lanes, local_rows), bf16),
        pltpu.VMEM((SIDES, local_rows // SIDES, lanes), f32),
        pltpu.VMEM((local_rows, lanes), bf16),
        pltpu.VMEM((SIDES, TILE, lanes), bf16),
        pltpu.VMEM((SIDES, local_rows, TILE), bf16),
        pltpu.VMEM((SIDES, local_rows, TILE), f32),
        pltpu.VMEM((SIDES, SIDE, SIDE, SIDES, ROWS, TILE), f32),
        dma((SIDE, SIDE)), dma((COLOURS, SIDE)), dma((SIDE, SIDE)), dma((SIDE, SIDE)),
        dma((SIDE, COLOURS, SIDES, COLOURS)), dma((SIDE, COLOURS, SIDES, COLOURS)), dma((SIDES, COLOURS, SIDES, COLOURS)), dma((SIDES, COLOURS, SIDES, COLOURS)), dma((SIDES, COLOURS, SIDES, COLOURS)), dma((SIDES, COLOURS, SIDES, COLOURS)),
        dma((1,)), dma((1,)), dma((COLOURS, COLOURS)), dma((COLOURS, COLOURS)), dma((COLOURS,)), dma((COLOURS,)), dma((COLOURS,)), dma((COLOURS,)),
        dma((SIDES,)), dma((SIDES, COLOURS, COLOURS, SIDES, COLOURS)), dma((SIDES, COLOURS, COLOURS, SIDES, COLOURS)), dma((SIDES, 15)), dma((SIDES, 15)),
        dma((SIDES,)), dma((SIDES, COLOURS)), dma((SIDES, SIDES)), pltpu.SemaphoreType.REGULAR, pltpu.SemaphoreType.REGULAR((2,)),
    ]
    outs = pl.pallas_call(
        functools.partial(comm_kernel, lanes),
        name="reduce_update_gather",
        out_shape=[jax.ShapeDtypeStruct((SIDE, SIDE, SIDE, SIDE, SIDES, ROWS, lanes), bf16), jax.ShapeDtypeStruct(up_shape, f32), jax.ShapeDtypeStruct(down_shape, f32), jax.ShapeDtypeStruct((8, 128), f32), jax.ShapeDtypeStruct(up, f32), jax.ShapeDtypeStruct((3072, lanes), f32), jax.ShapeDtypeStruct(up, f32)],
        in_specs=[hbm] * 22 + [smem] * 2,
        out_specs=[hbm] * 3 + [vmem] + [hbm] * 3,
        scratch_shapes=scratch,
        compiler_params=pltpu.CompilerParams(collective_id=0, has_side_effects=True, vmem_limit_bytes=67043328),
    )(grad_down2.reshape(down), *rows, *weights_in, *hidden, *masters, *moms, *vels, learn_rate.reshape(1), clip_norm.reshape(1))
    split = (SIDE, SIDE, SIDES, SIDES, SIDES, ROWS, lanes)
    placed = pl.pallas_call(
        functools.partial(place_kernel, lanes),
        name="place_outputs",
        out_shape=[jax.ShapeDtypeStruct(split if mat % SIDES else up, bf16) for mat in range(SIDE)] + [jax.ShapeDtypeStruct(m.shape, f32) for m in masters] * 3 + [jax.ShapeDtypeStruct((1,), f32)],
        in_specs=[hbm] * 3 + [vmem],
        out_specs=[hbm] * 16 + [smem],
        scratch_shapes=[
            pltpu.VMEM((SIDE,) + split, bf16), pltpu.VMEM(up_shape, f32), pltpu.VMEM(down_shape, f32),
            dma((SIDE, SIDE)), dma((SIDES,)), dma((SIDE, SIDE, SIDE)), dma((COLOURS, SIDE)),
        ],
        compiler_params=pltpu.CompilerParams(vmem_limit_bytes=67043328),
    )(outs[0].reshape((4,) + split), *outs[1:4])
    weights = [placed[mat].reshape(masters[mat].shape[0] * 128, -1) for mat in range(SIDE)]
    return tuple(weights) + tuple(placed[4:16]) + (placed[16][0],)


def mat_tn(left, right):
    return lax.dot_general(left, right, (((0,), (0,)), ((), ())), preferred_element_type=jnp.float32)


def gelu_pair(pre):
    normal_cdf = 0.5 * (1.0 + lax.erf(pre * ROOT_HALF))
    density = jnp.exp(-0.5 * pre * pre) * INV_ROOT_TAU
    return pre * normal_cdf, normal_cdf + pre * density


def solution(mesh):
    rows_spec = P("data", None)
    full_spec = P(None, None)
    scalar_spec = P()

    def shard_body(act_in, grad_out, w_up1, w_down1, w_up2, w_down2, *rest):
        gel_up1, der_up1 = gelu_pair(jnp.dot(act_in, w_up1, preferred_element_type=jnp.float32))
        act_up1 = gel_up1.astype(jnp.bfloat16)
        mid_act = jnp.dot(act_up1, w_down1, preferred_element_type=jnp.float32).astype(jnp.bfloat16)
        gel_up2, der_up2 = gelu_pair(jnp.dot(mid_act, w_up2, preferred_element_type=jnp.float32))
        grad_down2 = mat_tn(gel_up2.astype(jnp.bfloat16), grad_out)
        return comm_call(768, grad_down2, (grad_out, mid_act, act_in), (w_down1, w_up2, w_down2), (der_up1, der_up2, act_up1), rest[0:4], rest[4:8], rest[8:12], rest[12], rest[13])

    in_specs = (rows_spec, rows_spec) + (full_spec,) * 4 + (rows_spec,) * 12 + (scalar_spec, scalar_spec)
    out_specs = (full_spec,) * 4 + (rows_spec,) * 12 + (scalar_spec,)
    return jax.shard_map(shard_body, mesh=mesh, in_specs=in_specs, out_specs=out_specs, check_vma=False)
```

```python
import functools
import math
import jax
import jax.numpy as jnp
from jax import lax
from jax.experimental import pallas as pl
from jax.experimental.pallas import tpu as pltpu
from jax.sharding import PartitionSpec as P

STEP = 20
BETA_ONE = 0.9
BETA_TWO = 0.95
EPSILON = 1e-8
NORM_EPS = 1e-6
CORR_ONE = 1.0 - BETA_ONE ** STEP
CORR_TWO = 1.0 - BETA_TWO ** STEP
ROOT_HALF = math.sqrt(0.5)
INV_ROOT_TAU = 1.0 / math.sqrt(2.0 * math.pi)

MESH = pl.DeviceIdType.MESH
UP1, DOWN1, UP2, DOWN2 = 0, 1, 2, 3
UP, DOWN = 0, 1
LAST, MIDDLE, EARLY = 0, 1, 2
FAR, NEAR, PASS = 0, 1, 2
STRIDES = (32, 8, 2)
ORDERS = ((2, 1, 0), (1, 0, 2), (0, 2, 1))
ROWS = 24
SUB = 6
CHUNK = 8
SIDE = 4
COLOURS = 3
SIDES = 2
ALL = slice(None)
TILE = 512


def adam_step(scaled, master_old, mom_old, vel_old, learn_rate):
    mom_new = BETA_ONE * mom_old + (1.0 - BETA_ONE) * scaled
    vel_new = BETA_TWO * vel_old + (1.0 - BETA_TWO) * scaled * scaled
    master_new = master_old - learn_rate * (mom_new / CORR_ONE) / (jnp.sqrt(vel_new / CORR_TWO) + EPSILON)
    return master_new, mom_new, vel_new


def comm_kernel(lanes, *refs):
    (g_down2, grad_rows, mid_rows, in_rows, w_down1, w_up2, w_down2, der1, der2, act1), refs = refs[:10], refs[10:]
    states, refs = refs[:12], refs[12:]
    (lr_ref, clip_ref), refs = refs[:2], refs[2:]
    (w_out, up_out, down_out, norm_out, g_up1, g_down1, g_up2), refs = refs[:7], refs[7:]
    (total, peer_in, rs1, rs2, rs3, norm_line, norm_plane, send_g, recv_g, send_w, recv_w, block_tmp, w_own, up_state, down_state), refs = refs[:15], refs[15:]
    (left, flipped, mid_acc, mid_grad, w_tile, act_tile, der_tile, out_tile), refs = refs[:8], refs[8:]
    (load_sem, state_sem, pair_s, pair_r, rs1_s, rs1_r, rs2_s, rs2_r, rs3_s, rs3_r, nc_s, nc_r, na_s, na_r, xg_s, xg_r, xw_s, xw_r, own_sem, ag_s, ag_r, out_s, out_r) = refs[:23]
    row_sem, tile_sem, store_sem, pair_credit, ring_credit = refs[23:]
    half = lanes // 2
    me = lax.axis_index("data")
    core = lax.rem(me, SIDES)
    member = lax.rem(me, 4)
    pos = (me // 32, lax.rem(me // 8, 4), lax.rem(me // 2, 4))
    partner = me + 1 - 2 * core

    def device(axis, coord):
        return me + (coord - pos[axis]) * STRIDES[axis]

    def step(axis, hops):
        return lax.rem(pos[axis] + hops, 4)

    def remote(src, dst, send_sem, recv_sem, target):
        return pltpu.make_async_remote_copy(src_ref=src, dst_ref=dst, send_sem=send_sem, recv_sem=recv_sem, device_id=(target,), device_id_type=MESH)

    line, plane = lax.rem(me, 8), me // 8
    line_peers = [me - line + lax.rem(line + hops, 8) for hops in range(1, 8)]
    plane_peers = [8 * lax.rem(plane + hops, 16) + line for hops in range(1, 16)]
    peers = line_peers + plane_peers
    barrier = pltpu.get_barrier_semaphore()
    for peer in peers:
        pl.semaphore_signal(barrier, device_id=(peer,), device_id_type=MESH)

    grads = (g_up1, g_down1, g_up2, g_down2)
    mat_order = (3, 2, 1, 0)
    pair_slot = (1, 0, 1, 0)
    loads, pairs = {0: [], 2: []}, {0: [], 2: []}

    def issue_up(mat, x_low):
        for x in (x_low, x_low + 2):
            for owner in (1 - core, core):
                col = pl.multiple_of((x_low * 2 + owner) * lanes, lanes)
                src = grads[mat].at[:, :, x // SIDES, :, pl.ds(col, lanes)]
                if owner is core:
                    loads[mat].append(pltpu.make_async_copy(src, total.at[mat, :, :, x], load_sem.at[mat, x]))
                    loads[mat][-1].start()
                else:
                    pairs[mat].append(remote(src, peer_in.at[pair_slot[mat], :, :, x], pair_s.at[mat, x], pair_r.at[mat, x], partner))
                    pairs[mat][-1].start()

    def issue_rows(low, high):
        def move(i, carry):
            place = (i // 16, lax.rem(i // SIDE, 4), lax.rem(i, SIDE))
            there = g_down1.at[pl.ds(pl.multiple_of(i * 2 * ROWS + (1 - core) * ROWS, 8), ROWS)]
            here = g_down1.at[pl.ds(pl.multiple_of(i * 2 * ROWS + core * ROWS, 8), ROWS)]
            remote(there, peer_in.at[(pair_slot[DOWN1],) + place], pair_s.at[DOWN1, 0], pair_r.at[DOWN1, 0], partner).start()
            pltpu.make_async_copy(here, total.at[(1,) + place], load_sem.at[DOWN1, 0]).start()
            return carry

        lax.fori_loop(low, high, move, 0)

    loads[DOWN1] = [pltpu.make_async_copy(total.at[1], total.at[1], load_sem.at[DOWN1, 0])]
    pairs[DOWN1] = [remote(peer_in.at[pair_slot[DOWN1]], peer_in.at[pair_slot[DOWN1]], pair_s.at[DOWN1, 0], pair_r.at[DOWN1, 0], partner)]
    loads[DOWN2] = [pltpu.make_async_copy(g_down2.at[:, :, :, core], total.at[3], load_sem.at[DOWN2, 0])]

    tiles = SIDE * lanes // TILE

    def span(t):
        return pl.ds(pl.multiple_of(t * TILE, TILE), TILE)

    def fetch_a(t, slot):
        return [
            pltpu.make_async_copy(w_down2.at[span(t)], w_tile.at[slot], tile_sem.at[slot, 0]),
            pltpu.make_async_copy(w_up2.at[:, span(t)], act_tile.at[slot, pl.ds(0, lanes)], tile_sem.at[slot, 1]),
            pltpu.make_async_copy(der2.at[:, span(t)], der_tile.at[slot], tile_sem.at[slot, 2]),
        ]

    def fetch_b(t, slot):
        return [pltpu.make_async_copy(act1.at[:, span(t)], act_tile.at[slot], tile_sem.at[slot, 1])]

    def fetch_c(t, slot):
        return [
            pltpu.make_async_copy(w_down1.at[span(t)], w_tile.at[slot], tile_sem.at[slot, 0]),
            pltpu.make_async_copy(der1.at[:, span(t)], der_tile.at[slot], tile_sem.at[slot, 2]),
        ]

    def begin(copies):
        for copy in copies:
            copy.start()

    def end(copies):
        for copy in copies:
            copy.wait()

    row_loads = [pltpu.make_async_copy(grad_rows, left, row_sem.at[0]), pltpu.make_async_copy(mid_rows, mid_grad, row_sem.at[1])]
    begin(row_loads)
    begin(fetch_a(0, 0))
    begin(loads[DOWN2])
    state_loads = []
    for field in range(COLOURS):
        for mat in range(SIDE):
            dst = (down_state if mat % SIDES else up_state).at[field, mat // SIDES]
            state_loads.append(pltpu.make_async_copy(states[4 * field + mat], dst, state_sem.at[field, mat]))
    begin(state_loads)
    def store_a(t, slot):
        return [pltpu.make_async_copy(out_tile.at[slot], g_up2.at[:, :, :, :, span(t)], store_sem.at[slot])]

    def store_b(t, slot):
        return [pltpu.make_async_copy(mid_acc.at[slot], g_down1.at[span(t)], store_sem.at[slot])]

    def store_c(t, slot):
        return [pltpu.make_async_copy(out_tile.at[slot], g_up1.at[:, :, :, :, span(t)], store_sem.at[slot])]

    def run(first, last, fetch, store, work):
        def tile(t, carry):
            slot = lax.rem(t, SIDES)

            @pl.when(t + 1 < tiles)
            def _():
                begin(fetch(t + 1, 1 - slot))

            end(fetch(t, slot))

            @pl.when(t - first >= 2)
            def _():
                end(store(t - 2, slot))

            work(slot)
            begin(store(t, slot))
            return carry

        lax.fori_loop(first, last, tile, 0)
        for t in range(max(first, last - 2), last):
            end(store(t, t % 2))

    def dot(lhs, rhs, lhs_dim, rhs_dim):
        return lax.dot_general(lhs, rhs, (((lhs_dim,), (rhs_dim,)), ((), ())), preferred_element_type=jnp.float32)

    def work_a(slot):
        grad_act2 = dot(left[...], w_tile[slot], 1, 1).astype(jnp.bfloat16)
        grad_pre2 = (grad_act2.astype(jnp.float32) * der_tile[slot]).astype(jnp.bfloat16)
        out_tile[slot] = dot(flipped[...], grad_pre2, 1, 0).reshape(out_tile.shape[1:])
        mid_acc[...] += dot(grad_pre2, act_tile[slot, pl.ds(0, lanes)], 1, 1).reshape(mid_acc.shape)

    def work_b(slot):
        mid_acc[slot] = dot(act_tile[slot], mid_grad[...], 0, 0)

    def work_c(slot):
        grad_act1 = dot(mid_grad[...], w_tile[slot], 1, 1).astype(jnp.bfloat16)
        grad_pre1 = (grad_act1.astype(jnp.float32) * der_tile[slot]).astype(jnp.bfloat16)
        out_tile[slot] = dot(flipped[...], grad_pre1, 1, 0).reshape(out_tile.shape[1:])

    pl.semaphore_wait(barrier, len(peers))
    pairs[DOWN2] = [remote(g_down2.at[:, :, :, 1 - core], peer_in.at[pair_slot[DOWN2]], pair_s.at[DOWN2, 0], pair_r.at[DOWN2, 0], partner)]
    pairs[DOWN2][0].start()

    def part(mats, coords, colour, side):
        lane = ALL if side is None else pl.ds(half * side, half)
        index = [mats, ALL, ALL, ALL, pl.ds(CHUNK * colour, CHUNK), lane]
        for axis, coord in coords.items():
            index[1 + axis] = coord
        return tuple(index)

    class Phase:
        def __init__(self, level, base, buf, send_sem, recv_sem):
            self.level, self.base, self.buf, self.send_sem, self.recv_sem = level, base, buf, send_sem, recv_sem
            self.mats, self.count = (slice(base, base + 2), 2) if level else (base, 4)
            self.copies = {}

        def where(self, colour, coord):
            order = ORDERS[colour]
            coords = {axis: pos[axis] for axis in order[:self.level]}
            coords[order[self.level]] = coord
            return coords

        def row(self, colour, coord, side, i):
            coords = self.where(colour, coord)
            if self.level:
                return part(self.base + i, coords, colour, side)
            coords[min(axis for axis in range(COLOURS) if axis not in coords)] = i
            return part(self.mats, coords, colour, side)

        def send(self, colour, side, kind, src, target):
            copy = remote(src, self.buf.at[colour, side, kind], self.send_sem.at[colour, side, kind], self.recv_sem.at[colour, side, kind], target)
            copy.start()
            self.copies[colour, side, kind] = copy

        def near(self, colour, side):
            axis = ORDERS[colour][self.level]
            coord = step(axis, 1 if side == 0 else 3)
            return coord, device(axis, coord)

        def start(self):
            for kind in range(SIDES):
                for colour in range(COLOURS):
                    for side in range(SIDES):
                        coord, target = self.near(colour, side)
                        aim = step(ORDERS[colour][self.level], 2) if kind == 0 else coord
                        src = total.at[part(self.mats, self.where(colour, aim), colour, side if kind == 0 else 1 - side)]
                        self.send(colour, side, kind, src, target)

        def forward(self):
            for colour in range(COLOURS):
                for side in range(SIDES):
                    coord, target = self.near(colour, side)
                    self.copies[colour, side, FAR].wait_recv()

                    def add_own(i, carry, colour=colour, side=side, coord=coord):
                        self.buf[colour, side, FAR, i] = self.buf[colour, side, FAR, i] + total[self.row(colour, coord, side, i)]
                        return carry

                    lax.fori_loop(0, self.count, add_own, 0)
                    self.send(colour, side, 2, self.buf.at[colour, side, FAR], target)

        def finish(self):
            for colour in range(COLOURS):
                for side in range(SIDES):
                    self.copies[colour, 1 - side, NEAR].wait_recv()
                    self.copies[colour, side, PASS].wait_recv()

                    def add_both(i, carry, colour=colour, side=side):
                        own = self.row(colour, pos[ORDERS[colour][self.level]], side, i)
                        total[own] = total[own] + (self.buf[colour, 1 - side, NEAR, i] + self.buf[colour, side, PASS, i])
                        return carry

                    lax.fori_loop(0, self.count, add_both, 0)

        def drain(self):
            for copy in self.copies.values():
                copy.wait_send()

    ring_slot = (1, 0, 1, 0)
    class Direct:
        def __init__(self, base, buf, send_sem, recv_sem):
            self.base, self.buf, self.send_sem, self.recv_sem = base, buf, send_sem, recv_sem
            self.copies = {}

        def index(self, colour, coord, mats):
            coords = {axis: pos[axis] for axis in range(COLOURS)}
            coords[ORDERS[colour][2]] = coord
            return part(mats, coords, colour, None)

        def start(self):
            for hops in (2, 1, 3):
                for colour in range(COLOURS):
                    axis = ORDERS[colour][2]
                    coord = step(axis, hops)
                    spots = (colour, hops - 1)
                    src = total.at[self.index(colour, coord, slice(self.base, self.base + 2))]
                    copy = remote(src, self.buf.at[spots], self.send_sem.at[spots], self.recv_sem.at[spots], device(axis, coord))
                    copy.start()
                    self.copies[spots] = copy

        def finish(self):
            for colour in range(COLOURS):
                for hops in range(COLOURS):
                    self.copies[colour, hops].wait_recv()
                for mat in range(SIDES):
                    own = self.index(colour, pos[ORDERS[colour][2]], self.base + mat)
                    total[own] = (total[own] + self.buf[colour, 0, mat]) + (self.buf[colour, 1, mat] + self.buf[colour, 2, mat])

        def drain(self):
            for copy in self.copies.values():
                copy.wait_send()

    first = {mat: Phase(0, mat, rs1.at[ring_slot[mat]], rs1_s.at[mat], rs1_r.at[mat]) for mat in mat_order}

    def add_pair(mat):
        end(loads[mat])
        for copy in pairs[mat]:
            copy.wait_recv()

        def add(i, carry):
            total[mat, i // SIDE, lax.rem(i, SIDE)] = total[mat, i // SIDE, lax.rem(i, SIDE)] + peer_in[pair_slot[mat], i // SIDE, lax.rem(i, SIDE)]
            return carry

        lax.fori_loop(0, 16, add, 0)
        if mat >= 2:
            pl.semaphore_signal(pair_credit, device_id=(partner,), device_id_type=MESH)

    ring = [device(axis, step(axis, hops)) for axis in range(COLOURS) for hops in (1, 3)]

    def close(mat):
        first[mat].finish()
        first[mat].drain()
        for peer in ring:
            pl.semaphore_signal(ring_credit.at[ring_slot[mat]], device_id=(peer,), device_id_type=MESH)

    second = {base: Phase(1, base, rs2.at[base // 2], rs2_s.at[base // 2], rs2_r.at[base // 2]) for base in (2, 0)}
    third = {base: Direct(base, rs3.at[base // 2], rs3_s.at[base // 2], rs3_r.at[base // 2]) for base in (2, 0)}
    end(row_loads)
    flipped[...] = mid_grad[...].T
    mid_acc[...] = jnp.zeros_like(mid_acc)
    run(0, 3, fetch_a, store_a, work_a)
    add_pair(DOWN2)
    first[DOWN2].start()
    issue_up(UP2, 0)
    run(3, tiles, fetch_a, store_a, work_a)
    issue_up(UP2, 1)
    begin(fetch_b(0, 0) + fetch_c(0, 0))
    in_load = pltpu.make_async_copy(in_rows, left, row_sem.at[0])
    in_load.start()
    mid_grad[...] = mid_acc[...].reshape(mid_grad.shape).astype(jnp.bfloat16)
    first[DOWN2].forward()
    run(0, 3, fetch_b, store_b, work_b)
    add_pair(UP2)
    first[UP2].start()
    run(3, tiles, fetch_b, store_b, work_b)
    pl.semaphore_wait(pair_credit)
    issue_rows(0, 64)
    in_load.wait()
    flipped[...] = left[...].T
    close(DOWN2)
    run(0, 2, fetch_c, store_c, work_c)
    first[UP2].forward()
    run(2, 4, fetch_c, store_c, work_c)
    add_pair(DOWN1)
    pl.semaphore_wait(ring_credit.at[0], len(ring))
    first[DOWN1].start()
    pl.semaphore_wait(pair_credit)
    issue_up(UP1, 0)
    run(4, tiles, fetch_c, store_c, work_c)
    issue_up(UP1, 1)
    close(UP2)
    second[UP2].start()
    add_pair(UP1)
    pl.semaphore_wait(ring_credit.at[1], len(ring))
    first[UP1].start()
    first[DOWN1].forward()
    second[UP2].forward()
    second[UP2].finish()
    third[UP2].start()
    first[UP1].forward()
    first[DOWN1].finish()
    third[UP2].finish()
    first[UP1].finish()
    second[UP1].start()
    second[UP1].forward()
    second[UP1].finish()
    third[UP1].start()
    third[UP1].finish()

    group_scale = 1.0 / 128.0
    grad_own = [total[mat, *pos] * group_scale for mat in range(SIDE)]
    partial = None
    for block in grad_own:
        square = block * block
        for row in range(ROWS // 8):
            for col in range(max(1, lanes // 128)):
                tile = square[8 * row:8 * row + 8, 128 * col:128 * col + 128]
                partial = tile if partial is None else partial + tile
    norm_line[line] = partial
    sends = []

    def spread(buf, slot, targets, send_sem, recv_sem):
        copies = []
        for i, target in enumerate(targets):
            copies.append(remote(buf.at[slot], buf.at[slot], send_sem.at[i], recv_sem.at[i], target))
            copies[i].start()
        return copies

    swap = spread(norm_line, line, line_peers, nc_s, nc_r)
    for target in range(SIDE):
        for i, mat in enumerate((0, 2)):
            send_g[target, i] = grad_own[mat][SUB * target:SUB * target + SUB]
    moves = []
    for hops in range(1, SIDE):
        other = lax.rem(member + hops, SIDE)
        copy = remote(send_g.at[other], recv_g.at[member], xg_s.at[hops - 1], xg_r.at[hops - 1], me - member + other)
        copy.start()
        moves.append(copy)
    recv_g[member] = send_g[member]
    for copy in swap:
        copy.wait_recv()
    norm_plane[plane] = jnp.sum(norm_line[...], axis=0)
    cross = spread(norm_plane, plane, plane_peers, na_s, na_r)
    for copy in cross:
        copy.wait_recv()
    running = jnp.sum(norm_plane[...], axis=0)
    sends = swap + cross + moves
    norm = jnp.sqrt(jnp.sum(jnp.sum(running, axis=1, keepdims=True), axis=0, keepdims=True))
    norm_out[...] = jnp.broadcast_to(norm, norm_out.shape)
    clip_scale = jnp.minimum(1.0, clip_ref[0] / (norm + NORM_EPS))
    learn_rate = lr_ref[0]

    end(state_loads)
    for i in range(SIDES):
        fresh = adam_step(grad_own[2 * i + 1] * clip_scale, down_state[0, i], down_state[1, i], down_state[2, i], learn_rate)
        for field in range(COLOURS):
            down_state[field, i] = fresh[field]
        w_own[2 + i] = fresh[0].astype(jnp.bfloat16)

    def spot(group, coords, colour, side):
        lane = ALL if side is None else pl.ds(half * side, half)
        index = [pl.ds(2 * group, 2), ALL, ALL, ALL, core, pl.ds(CHUNK * colour, CHUNK), lane]
        for axis, coord in coords.items():
            index[1 + axis] = coord
        return w_out.at[tuple(index)]

    handed = []

    class Gather:
        def __init__(self, group, level):
            self.group, self.level = group, level
            self.copies = {}

        def spot(self, colour, coord, side):
            order = ORDERS[colour]
            coords = {axis: pos[axis] for axis in order[:self.level]}
            coords[order[self.level]] = coord
            return spot(self.group, coords, colour, side)

        def near(self, colour, side):
            axis = ORDERS[colour][self.level]
            coord = step(axis, 1 if side == 0 else 3)
            return coord, device(axis, coord)

        def send(self, colour, side, kind, src, dst):
            spots = (self.group, self.level, colour, side, kind)
            copy = remote(src, dst, ag_s.at[spots], ag_r.at[spots], self.near(colour, side)[1])
            copy.start()
            self.copies[colour, side, kind] = copy

        def hand(self, ref, slot):
            copy = remote(ref, ref, out_s.at[self.group, slot], out_r.at[self.group, slot], partner)
            copy.start()
            handed.append(copy)

        def start_direct(self):
            for hops in (2, 1, 3):
                for colour in range(COLOURS):
                    axis = ORDERS[colour][self.level]
                    dst = self.spot(colour, pos[axis], None)
                    src = w_own.at[pl.ds(2 * self.group, 2), pl.ds(CHUNK * colour, CHUNK)] if self.level == 2 else dst
                    spots = (self.group, self.level, colour, 0, hops - 1)
                    copy = remote(src, dst, ag_s.at[spots], ag_r.at[spots], device(axis, step(axis, hops)))
                    copy.start()
                    self.copies[colour, hops] = copy

        def finish_direct(self):
            for copy in self.copies.values():
                copy.wait_recv()

        def start(self):
            for kind in range(SIDES):
                for colour in range(COLOURS):
                    for side in range(SIDES):
                        ref = self.spot(colour, pos[ORDERS[colour][0]], side if kind == 0 else 1 - side)
                        self.send(colour, side, kind, ref, ref)
            for colour in range(COLOURS):
                self.hand(self.spot(colour, pos[ORDERS[colour][0]], None), 5 * colour)

        def forward(self):
            for colour in range(COLOURS):
                for side in range(SIDES):
                    self.copies[colour, side, FAR].wait_recv()
                    ref = self.spot(colour, self.near(colour, 1 - side)[0], side)
                    self.send(colour, side, 2, ref, ref)

        def finish(self):
            for colour in range(COLOURS):
                for side in range(SIDES):
                    self.copies[colour, side, NEAR].wait_recv()
                    self.hand(self.spot(colour, self.near(colour, 1 - side)[0], None), 5 * colour + 1 + side)
            for colour in range(COLOURS):
                for side in range(SIDES):
                    self.copies[colour, side, PASS].wait_recv()
                    self.hand(self.spot(colour, step(ORDERS[colour][0], 2), side), 5 * colour + 3 + side)

    keeps = [pltpu.make_async_copy(w_own.at[pl.ds(2 * group, 2)], w_out.at[pl.ds(2 * group, 2), *pos, core], own_sem.at[group]) for group in range(SIDES)]
    gathers = {(group, level): Gather(group, level) for group in range(SIDES) for level in range(COLOURS)}
    gathers[DOWN, EARLY].start_direct()
    keeps[DOWN].start()

    for copy in moves:
        copy.wait_recv()
    for i in range(SIDES):
        for col in range(SIDE):
            cols = slice(col * lanes, (col + 1) * lanes)
            scaled = recv_g[col, i] * clip_scale
            fresh = adam_step(scaled, up_state[0, i, :, cols], up_state[1, i, :, cols], up_state[2, i, :, cols], learn_rate)
            for field in range(COLOURS):
                up_state[field, i, :, cols] = fresh[field]
            send_w[col, i] = fresh[0]
    moves = []
    for hops in range(1, SIDE):
        other = lax.rem(member + hops, SIDE)
        copy = remote(send_w.at[other], recv_w.at[member], xw_s.at[hops - 1], xw_r.at[hops - 1], me - member + other)
        copy.start()
        moves.append(copy)
    recv_w[member] = send_w[member]
    state_stores = [pltpu.make_async_copy(up_state, up_out, state_sem.at[0, 0]), pltpu.make_async_copy(down_state, down_out, state_sem.at[0, 1])]
    begin(state_stores)
    gathers[DOWN, EARLY].finish_direct()
    keeps[DOWN].wait()
    gathers[DOWN, MIDDLE].start_direct()
    for copy in moves:
        copy.wait_recv()
    sends = sends + moves
    for i in range(SIDES):
        for source in range(SIDE):
            block_tmp[SUB * source:SUB * source + SUB] = recv_w[source, i]
        w_own[i] = block_tmp[...].astype(jnp.bfloat16)
    gathers[UP, EARLY].start_direct()
    keeps[UP].start()
    gathers[DOWN, MIDDLE].finish_direct()
    gathers[DOWN, LAST].start()
    gathers[UP, EARLY].finish_direct()
    keeps[UP].wait()
    gathers[UP, MIDDLE].start_direct()
    gathers[UP, MIDDLE].finish_direct()
    gathers[UP, LAST].start()
    gathers[DOWN, LAST].forward()
    gathers[DOWN, LAST].finish()
    gathers[UP, LAST].forward()
    gathers[UP, LAST].finish()
    for gather in gathers.values():
        sends = sends + list(gather.copies.values())
    for phase in [first[DOWN1], first[UP1]] + list(second.values()) + list(third.values()):
        phase.drain()
    for mat in mat_order:
        for copy in pairs[mat]:
            copy.wait_send()
    for copy in sends:
        copy.wait_send()
    for copy in handed + state_stores:
        copy.wait()


def place_kernel(lanes, w_ref, up_ref, down_ref, norm_ref, *refs):
    weights, states, norm_out, (w_tmp, up_tmp, down_tmp, in_sem, state_in, out_sem, state_out) = refs[:4], refs[4:16], refs[16], refs[17:]
    norm_out[0] = jnp.max(norm_ref[...])
    loads = [[pltpu.make_async_copy(w_ref.at[mat % SIDES * 2 + mat // SIDES, z], w_tmp.at[mat, z], in_sem.at[mat, z]) for z in range(SIDE)] for mat in range(SIDE)]
    for row in loads:
        for copy in row:
            copy.start()
    state_loads = [pltpu.make_async_copy(up_ref, up_tmp, state_in.at[0]), pltpu.make_async_copy(down_ref, down_tmp, state_in.at[1])]
    for copy in state_loads:
        copy.start()
    stores = []
    for mat in range(SIDE):
        for z in range(SIDE):
            loads[mat][z].wait()
            if mat % SIDES:
                copies = [pltpu.make_async_copy(w_tmp.at[mat, z], weights[mat].at[z], out_sem.at[mat, z, 0])]
            else:
                copies = []
                for member in range(SIDE):
                    src = w_tmp.at[mat, z, :, :, member // SIDES, member % SIDES]
                    copies.append(pltpu.make_async_copy(src, weights[mat].at[z, :, :, :, pl.ds(member * lanes, lanes)], out_sem.at[mat, z, member]))
            for copy in copies:
                copy.start()
            stores = stores + copies
    for copy in state_loads:
        copy.wait()
    for field in range(COLOURS):
        for mat in range(SIDE):
            src = (down_tmp if mat % SIDES else up_tmp).at[field, mat // SIDES]
            copy = pltpu.make_async_copy(src, states[4 * field + mat], state_out.at[field, mat])
            copy.start()
            stores.append(copy)
    for copy in stores:
        copy.wait()


def comm_call(lanes, grad_down2, rows, weights_in, hidden, masters, moms, vels, learn_rate, clip_norm):
    up = (SIDE, SIDE, SIDES, ROWS, SIDE * lanes)
    down = (SIDE, SIDE, SIDE, SIDES, ROWS, lanes)
    local_rows = rows[0].shape[0]
    half = lanes // 2
    f32 = jnp.float32
    bf16 = jnp.bfloat16
    up_shape = (COLOURS, SIDES, SUB, SIDE * lanes)
    down_shape = (COLOURS, SIDES, ROWS, lanes)
    dma = pltpu.SemaphoreType.DMA
    vmem = pl.BlockSpec(memory_space=pltpu.VMEM)
    smem = pl.BlockSpec(memory_space=pltpu.SMEM)
    hbm = pl.BlockSpec(memory_space=pl.ANY)
    scratch = [
        pltpu.VMEM((SIDE, SIDE, SIDE, SIDE, ROWS, lanes), f32),
        pltpu.VMEM((SIDES, SIDE, SIDE, SIDE, ROWS, lanes), f32),
        pltpu.VMEM((SIDES, COLOURS, SIDES, COLOURS, SIDE, SIDE, CHUNK, half), f32),
        pltpu.VMEM((SIDES, COLOURS, SIDES, COLOURS, SIDES, SIDE, CHUNK, half), f32),
        pltpu.VMEM((SIDES, COLOURS, COLOURS, SIDES, CHUNK, lanes), f32),
        pltpu.VMEM((8, 8, 128), f32),
        pltpu.VMEM((16, 8, 128), f32),
        pltpu.VMEM((SIDE, SIDES, SUB, lanes), f32),
        pltpu.VMEM((SIDE, SIDES, SUB, lanes), f32),
        pltpu.VMEM((SIDE, SIDES, SUB, lanes), f32),
        pltpu.VMEM((SIDE, SIDES, SUB, lanes), f32),
        pltpu.VMEM((ROWS, lanes), f32),
        pltpu.VMEM((SIDE, ROWS, lanes), jnp.bfloat16),
        pltpu.VMEM(up_shape, f32),
        pltpu.VMEM(down_shape, f32),
        pltpu.VMEM((local_rows, lanes), bf16),
        pltpu.VMEM((lanes, local_rows), bf16),
        pltpu.VMEM((SIDES, local_rows // SIDES, lanes), f32),
        pltpu.VMEM((local_rows, lanes), bf16),
        pltpu.VMEM((SIDES, TILE, lanes), bf16),
        pltpu.VMEM((SIDES, local_rows, TILE), bf16),
        pltpu.VMEM((SIDES, local_rows, TILE), f32),
        pltpu.VMEM((SIDES, SIDE, SIDE, SIDES, ROWS, TILE), f32),
        dma((SIDE, SIDE)), dma((COLOURS, SIDE)), dma((SIDE, SIDE)), dma((SIDE, SIDE)),
        dma((SIDE, COLOURS, SIDES, COLOURS)), dma((SIDE, COLOURS, SIDES, COLOURS)), dma((SIDES, COLOURS, SIDES, COLOURS)), dma((SIDES, COLOURS, SIDES, COLOURS)), dma((SIDES, COLOURS, COLOURS)), dma((SIDES, COLOURS, COLOURS)),
        dma((7,)), dma((7,)), dma((15,)), dma((15,)), dma((COLOURS,)), dma((COLOURS,)), dma((COLOURS,)), dma((COLOURS,)),
        dma((SIDES,)), dma((SIDES, COLOURS, COLOURS, SIDES, COLOURS)), dma((SIDES, COLOURS, COLOURS, SIDES, COLOURS)), dma((SIDES, 15)), dma((SIDES, 15)),
        dma((SIDES,)), dma((SIDES, COLOURS)), dma((SIDES,)), pltpu.SemaphoreType.REGULAR, pltpu.SemaphoreType.REGULAR((2,)),
    ]
    outs = pl.pallas_call(
        functools.partial(comm_kernel, lanes),
        name="reduce_update_gather",
        out_shape=[jax.ShapeDtypeStruct((SIDE, SIDE, SIDE, SIDE, SIDES, ROWS, lanes), bf16), jax.ShapeDtypeStruct(up_shape, f32), jax.ShapeDtypeStruct(down_shape, f32), jax.ShapeDtypeStruct((8, 128), f32), jax.ShapeDtypeStruct(up, f32), jax.ShapeDtypeStruct((3072, lanes), f32), jax.ShapeDtypeStruct(up, f32)],
        in_specs=[hbm] * 22 + [smem] * 2,
        out_specs=[hbm] * 3 + [vmem] + [hbm] * 3,
        scratch_shapes=scratch,
        compiler_params=pltpu.CompilerParams(collective_id=0, has_side_effects=True, vmem_limit_bytes=67043328),
    )(grad_down2.reshape(down), *rows, *weights_in, *hidden, *masters, *moms, *vels, learn_rate.reshape(1), clip_norm.reshape(1))
    split = (SIDE, SIDE, SIDES, SIDES, SIDES, ROWS, lanes)
    placed = pl.pallas_call(
        functools.partial(place_kernel, lanes),
        name="place_outputs",
        out_shape=[jax.ShapeDtypeStruct(split if mat % SIDES else up, bf16) for mat in range(SIDE)] + [jax.ShapeDtypeStruct(m.shape, f32) for m in masters] * 3 + [jax.ShapeDtypeStruct((1,), f32)],
        in_specs=[hbm] * 3 + [vmem],
        out_specs=[hbm] * 16 + [smem],
        scratch_shapes=[
            pltpu.VMEM((SIDE,) + split, bf16), pltpu.VMEM(up_shape, f32), pltpu.VMEM(down_shape, f32),
            dma((SIDE, SIDE)), dma((SIDES,)), dma((SIDE, SIDE, SIDE)), dma((COLOURS, SIDE)),
        ],
        compiler_params=pltpu.CompilerParams(vmem_limit_bytes=67043328),
    )(outs[0].reshape((4,) + split), *outs[1:4])
    weights = [placed[mat].reshape(masters[mat].shape[0] * 128, -1) for mat in range(SIDE)]
    return tuple(weights) + tuple(placed[4:16]) + (placed[16][0],)


def mat_tn(left, right):
    return lax.dot_general(left, right, (((0,), (0,)), ((), ())), preferred_element_type=jnp.float32)


def gelu_pair(pre):
    normal_cdf = 0.5 * (1.0 + lax.erf(pre * ROOT_HALF))
    density = jnp.exp(-0.5 * pre * pre) * INV_ROOT_TAU
    return pre * normal_cdf, normal_cdf + pre * density


def solution(mesh):
    rows_spec = P("data", None)
    full_spec = P(None, None)
    scalar_spec = P()

    def shard_body(act_in, grad_out, w_up1, w_down1, w_up2, w_down2, *rest):
        gel_up1, der_up1 = gelu_pair(jnp.dot(act_in, w_up1, preferred_element_type=jnp.float32))
        act_up1 = gel_up1.astype(jnp.bfloat16)
        mid_act = jnp.dot(act_up1, w_down1, preferred_element_type=jnp.float32).astype(jnp.bfloat16)
        gel_up2, der_up2 = gelu_pair(jnp.dot(mid_act, w_up2, preferred_element_type=jnp.float32))
        grad_down2 = mat_tn(gel_up2.astype(jnp.bfloat16), grad_out)
        return comm_call(768, grad_down2, (grad_out, mid_act, act_in), (w_down1, w_up2, w_down2), (der_up1, der_up2, act_up1), rest[0:4], rest[4:8], rest[8:12], rest[12], rest[13])

    in_specs = (rows_spec, rows_spec) + (full_spec,) * 4 + (rows_spec,) * 12 + (scalar_spec, scalar_spec)
    out_specs = (full_spec,) * 4 + (rows_spec,) * 12 + (scalar_spec,)
    return jax.shard_map(shard_body, mesh=mesh, in_specs=in_specs, out_specs=out_specs, check_vma=False)
```

```python
import functools
import math
import jax
import jax.numpy as jnp
from jax import lax
from jax.experimental import pallas as pl
from jax.experimental.pallas import tpu as pltpu
from jax.sharding import PartitionSpec as P

STEP = 20
BETA_ONE = 0.9
BETA_TWO = 0.95
EPSILON = 1e-8
NORM_EPS = 1e-6
CORR_ONE = 1.0 - BETA_ONE ** STEP
CORR_TWO = 1.0 - BETA_TWO ** STEP
ROOT_HALF = math.sqrt(0.5)
INV_ROOT_TAU = 1.0 / math.sqrt(2.0 * math.pi)

MESH = pl.DeviceIdType.MESH
UP1, DOWN1, UP2, DOWN2 = 0, 1, 2, 3
UP, DOWN = 0, 1
LAST, MIDDLE, EARLY = 0, 1, 2
FAR, NEAR, PASS = 0, 1, 2
STRIDES = (32, 8, 2)
ORDERS = ((2, 1, 0), (1, 0, 2), (0, 2, 1))
ROWS = 24
SUB = 6
CHUNK = 8
SIDE = 4
COLOURS = 3
SIDES = 2
ALL = slice(None)
TILE = 512


def adam_step(scaled, master_old, mom_old, vel_old, learn_rate):
    mom_new = BETA_ONE * mom_old + (1.0 - BETA_ONE) * scaled
    vel_new = BETA_TWO * vel_old + (1.0 - BETA_TWO) * scaled * scaled
    master_new = master_old - learn_rate * (mom_new / CORR_ONE) / (jnp.sqrt(vel_new / CORR_TWO) + EPSILON)
    return master_new, mom_new, vel_new


def comm_kernel(lanes, *refs):
    (g_down2, grad_rows, mid_rows, in_rows, w_down1, w_up2, w_down2, der1, der2, act1), refs = refs[:10], refs[10:]
    states, refs = refs[:12], refs[12:]
    (lr_ref, clip_ref), refs = refs[:2], refs[2:]
    (w_out, up_out, down_out, norm_out, g_up1, g_down1, g_up2), refs = refs[:7], refs[7:]
    (total, peer_in, rs1, rs2, rs3, norm_line, norm_plane, send_g, recv_g, send_w, recv_w, block_tmp, w_own, up_state, down_state), refs = refs[:15], refs[15:]
    (left, flipped, mid_acc, mid_grad, w_tile, act_tile, der_tile, out_tile), refs = refs[:8], refs[8:]
    (load_sem, state_sem, pair_s, pair_r, rs1_s, rs1_r, rs2_s, rs2_r, rs3_s, rs3_r, nc_s, nc_r, na_s, na_r, xg_s, xg_r, xw_s, xw_r, own_sem, ag_s, ag_r, out_s, out_r) = refs[:23]
    row_sem, tile_sem, store_sem, pair_credit, ring_credit = refs[23:]
    half = lanes // 2
    me = lax.axis_index("data")
    core = lax.rem(me, SIDES)
    member = lax.rem(me, 4)
    pos = (me // 32, lax.rem(me // 8, 4), lax.rem(me // 2, 4))
    partner = me + 1 - 2 * core

    def device(axis, coord):
        return me + (coord - pos[axis]) * STRIDES[axis]

    def step(axis, hops):
        return lax.rem(pos[axis] + hops, 4)

    def remote(src, dst, send_sem, recv_sem, target):
        return pltpu.make_async_remote_copy(src_ref=src, dst_ref=dst, send_sem=send_sem, recv_sem=recv_sem, device_id=(target,), device_id_type=MESH)

    line, plane = lax.rem(me, 8), me // 8
    line_peers = [me - line + lax.rem(line + hops, 8) for hops in range(1, 8)]
    plane_peers = [8 * lax.rem(plane + hops, 16) + line for hops in range(1, 16)]
    peers = line_peers + plane_peers
    barrier = pltpu.get_barrier_semaphore()
    for peer in peers:
        pl.semaphore_signal(barrier, device_id=(peer,), device_id_type=MESH)

    grads = (g_up1, g_down1, g_up2, g_down2)
    mat_order = (3, 2, 1, 0)
    pair_slot = (1, 0, 1, 0)
    loads, pairs = {0: [], 2: []}, {0: [], 2: []}

    def issue_up(mat, x_low):
        for x in (x_low, x_low + 2):
            for owner in (1 - core, core):
                col = pl.multiple_of((x_low * 2 + owner) * lanes, lanes)
                src = grads[mat].at[:, :, x // SIDES, :, pl.ds(col, lanes)]
                if owner is core:
                    loads[mat].append(pltpu.make_async_copy(src, total.at[mat, :, :, x], load_sem.at[mat, x]))
                    loads[mat][-1].start()
                else:
                    pairs[mat].append(remote(src, peer_in.at[pair_slot[mat], :, :, x], pair_s.at[mat, x], pair_r.at[mat, x], partner))
                    pairs[mat][-1].start()

    def issue_rows(low, high):
        def move(i, carry):
            place = (i // 16, lax.rem(i // SIDE, 4), lax.rem(i, SIDE))
            there = g_down1.at[pl.ds(pl.multiple_of(i * 2 * ROWS + (1 - core) * ROWS, 8), ROWS)]
            here = g_down1.at[pl.ds(pl.multiple_of(i * 2 * ROWS + core * ROWS, 8), ROWS)]
            remote(there, peer_in.at[(pair_slot[DOWN1],) + place], pair_s.at[DOWN1, 0], pair_r.at[DOWN1, 0], partner).start()
            pltpu.make_async_copy(here, total.at[(1,) + place], load_sem.at[DOWN1, 0]).start()
            return carry

        lax.fori_loop(low, high, move, 0)

    loads[DOWN1] = [pltpu.make_async_copy(total.at[1], total.at[1], load_sem.at[DOWN1, 0])]
    pairs[DOWN1] = [remote(peer_in.at[pair_slot[DOWN1]], peer_in.at[pair_slot[DOWN1]], pair_s.at[DOWN1, 0], pair_r.at[DOWN1, 0], partner)]
    loads[DOWN2] = [pltpu.make_async_copy(g_down2.at[:, :, :, core], total.at[3], load_sem.at[DOWN2, 0])]

    tiles = SIDE * lanes // TILE

    def span(t):
        return pl.ds(pl.multiple_of(t * TILE, TILE), TILE)

    def fetch_a(t, slot):
        return [
            pltpu.make_async_copy(w_down2.at[span(t)], w_tile.at[slot], tile_sem.at[slot, 0]),
            pltpu.make_async_copy(w_up2.at[:, span(t)], act_tile.at[slot, pl.ds(0, lanes)], tile_sem.at[slot, 1]),
            pltpu.make_async_copy(der2.at[:, span(t)], der_tile.at[slot], tile_sem.at[slot, 2]),
        ]

    def fetch_b(t, slot):
        return [pltpu.make_async_copy(act1.at[:, span(t)], act_tile.at[slot], tile_sem.at[slot, 1])]

    def fetch_c(t, slot):
        return [
            pltpu.make_async_copy(w_down1.at[span(t)], w_tile.at[slot], tile_sem.at[slot, 0]),
            pltpu.make_async_copy(der1.at[:, span(t)], der_tile.at[slot], tile_sem.at[slot, 2]),
        ]

    def begin(copies):
        for copy in copies:
            copy.start()

    def end(copies):
        for copy in copies:
            copy.wait()

    row_loads = [pltpu.make_async_copy(grad_rows, left, row_sem.at[0]), pltpu.make_async_copy(mid_rows, mid_grad, row_sem.at[1])]
    begin(row_loads)
    begin(fetch_a(0, 0))
    begin(loads[DOWN2])
    state_loads = []
    for field in range(COLOURS):
        for mat in range(SIDE):
            dst = (down_state if mat % SIDES else up_state).at[field, mat // SIDES]
            state_loads.append(pltpu.make_async_copy(states[4 * field + mat], dst, state_sem.at[field, mat]))
    begin(state_loads)
    def store_a(t, slot):
        return [pltpu.make_async_copy(out_tile.at[slot], g_up2.at[:, :, :, :, span(t)], store_sem.at[slot])]

    def store_b(t, slot):
        return [pltpu.make_async_copy(mid_acc.at[slot], g_down1.at[span(t)], store_sem.at[slot])]

    def store_c(t, slot):
        return [pltpu.make_async_copy(out_tile.at[slot], g_up1.at[:, :, :, :, span(t)], store_sem.at[slot])]

    def run(first, last, fetch, store, work):
        def tile(t, carry):
            slot = lax.rem(t, SIDES)

            @pl.when(t + 1 < tiles)
            def _():
                begin(fetch(t + 1, 1 - slot))

            end(fetch(t, slot))

            @pl.when(t - first >= 2)
            def _():
                end(store(t - 2, slot))

            work(slot)
            begin(store(t, slot))
            return carry

        lax.fori_loop(first, last, tile, 0)
        for t in range(max(first, last - 2), last):
            end(store(t, t % 2))

    def dot(lhs, rhs, lhs_dim, rhs_dim):
        return lax.dot_general(lhs, rhs, (((lhs_dim,), (rhs_dim,)), ((), ())), preferred_element_type=jnp.float32)

    def work_a(slot):
        grad_act2 = dot(left[...], w_tile[slot], 1, 1).astype(jnp.bfloat16)
        grad_pre2 = (grad_act2.astype(jnp.float32) * der_tile[slot]).astype(jnp.bfloat16)
        out_tile[slot] = dot(flipped[...], grad_pre2, 1, 0).reshape(out_tile.shape[1:])
        mid_acc[...] += dot(grad_pre2, act_tile[slot, pl.ds(0, lanes)], 1, 1).reshape(mid_acc.shape)

    def work_b(slot):
        mid_acc[slot] = dot(act_tile[slot], mid_grad[...], 0, 0)

    def work_c(slot):
        grad_act1 = dot(mid_grad[...], w_tile[slot], 1, 1).astype(jnp.bfloat16)
        grad_pre1 = (grad_act1.astype(jnp.float32) * der_tile[slot]).astype(jnp.bfloat16)
        out_tile[slot] = dot(flipped[...], grad_pre1, 1, 0).reshape(out_tile.shape[1:])

    def part(mats, coords, colour, side):
        lane = ALL if side is None else pl.ds(half * side, half)
        index = [mats, ALL, ALL, ALL, pl.ds(CHUNK * colour, CHUNK), lane]
        for axis, coord in coords.items():
            index[1 + axis] = coord
        return tuple(index)

    class Phase:
        def __init__(self, level, base, buf, send_sem, recv_sem):
            self.level, self.base, self.buf, self.send_sem, self.recv_sem = level, base, buf, send_sem, recv_sem
            self.mats, self.count = (slice(base, base + 2), 2) if level else (base, 4)
            self.copies = {}

        def where(self, colour, coord):
            order = ORDERS[colour]
            coords = {axis: pos[axis] for axis in order[:self.level]}
            coords[order[self.level]] = coord
            return coords

        def row(self, colour, coord, side, i):
            coords = self.where(colour, coord)
            if self.level:
                return part(self.base + i, coords, colour, side)
            coords[min(axis for axis in range(COLOURS) if axis not in coords)] = i
            return part(self.mats, coords, colour, side)

        def send(self, colour, side, kind, src, target):
            copy = remote(src, self.buf.at[colour, side, kind], self.send_sem.at[colour, side, kind], self.recv_sem.at[colour, side, kind], target)
            copy.start()
            self.copies[colour, side, kind] = copy

        def near(self, colour, side):
            axis = ORDERS[colour][self.level]
            coord = step(axis, 1 if side == 0 else 3)
            return coord, device(axis, coord)

        def start(self):
            for kind in range(SIDES):
                for colour in range(COLOURS):
                    for side in range(SIDES):
                        coord, target = self.near(colour, side)
                        aim = step(ORDERS[colour][self.level], 2) if kind == 0 else coord
                        src = total.at[part(self.mats, self.where(colour, aim), colour, side if kind == 0 else 1 - side)]
                        self.send(colour, side, kind, src, target)

        def forward(self):
            for colour in range(COLOURS):
                for side in range(SIDES):
                    coord, target = self.near(colour, side)
                    self.copies[colour, side, FAR].wait_recv()

                    def add_own(i, carry, colour=colour, side=side, coord=coord):
                        self.buf[colour, side, FAR, i] = self.buf[colour, side, FAR, i] + total[self.row(colour, coord, side, i)]
                        return carry

                    lax.fori_loop(0, self.count, add_own, 0)
                    self.send(colour, side, 2, self.buf.at[colour, side, FAR], target)

        def finish(self):
            for colour in range(COLOURS):
                for side in range(SIDES):
                    self.copies[colour, 1 - side, NEAR].wait_recv()
                    self.copies[colour, side, PASS].wait_recv()

                    def add_both(i, carry, colour=colour, side=side):
                        own = self.row(colour, pos[ORDERS[colour][self.level]], side, i)
                        total[own] = total[own] + (self.buf[colour, 1 - side, NEAR, i] + self.buf[colour, side, PASS, i])
                        return carry

                    lax.fori_loop(0, self.count, add_both, 0)

        def drain(self):
            for copy in self.copies.values():
                copy.wait_send()

    ring_slot = (1, 0, 1, 0)
    class Direct:
        def __init__(self, base, buf, send_sem, recv_sem):
            self.base, self.buf, self.send_sem, self.recv_sem = base, buf, send_sem, recv_sem
            self.copies = {}

        def index(self, colour, coord, mats):
            coords = {axis: pos[axis] for axis in range(COLOURS)}
            coords[ORDERS[colour][2]] = coord
            return part(mats, coords, colour, None)

        def start(self):
            for hops in (2, 1, 3):
                for colour in range(COLOURS):
                    axis = ORDERS[colour][2]
                    coord = step(axis, hops)
                    spots = (colour, hops - 1)
                    src = total.at[self.index(colour, coord, slice(self.base, self.base + 2))]
                    copy = remote(src, self.buf.at[spots], self.send_sem.at[spots], self.recv_sem.at[spots], device(axis, coord))
                    copy.start()
                    self.copies[spots] = copy

        def finish(self):
            for colour in range(COLOURS):
                for hops in range(COLOURS):
                    self.copies[colour, hops].wait_recv()
                for mat in range(SIDES):
                    own = self.index(colour, pos[ORDERS[colour][2]], self.base + mat)
                    total[own] = (total[own] + self.buf[colour, 0, mat]) + (self.buf[colour, 1, mat] + self.buf[colour, 2, mat])

        def drain(self):
            for copy in self.copies.values():
                copy.wait_send()

    first = {mat: Phase(0, mat, rs1.at[ring_slot[mat]], rs1_s.at[mat], rs1_r.at[mat]) for mat in mat_order}

    def add_pair(mat):
        end(loads[mat])
        for copy in pairs[mat]:
            copy.wait_recv()

        def add(i, carry):
            total[mat, i // SIDE, lax.rem(i, SIDE)] = total[mat, i // SIDE, lax.rem(i, SIDE)] + peer_in[pair_slot[mat], i // SIDE, lax.rem(i, SIDE)]
            return carry

        lax.fori_loop(0, 16, add, 0)
        if mat >= 2:
            pl.semaphore_signal(pair_credit, device_id=(partner,), device_id_type=MESH)

    ring = [device(axis, step(axis, hops)) for axis in range(COLOURS) for hops in (1, 3)]

    def close(mat):
        first[mat].finish()
        first[mat].drain()
        for peer in ring:
            pl.semaphore_signal(ring_credit.at[ring_slot[mat]], device_id=(peer,), device_id_type=MESH)

    second = {base: Phase(1, base, rs2.at[base // 2], rs2_s.at[base // 2], rs2_r.at[base // 2]) for base in (2, 0)}
    third = {base: Direct(base, rs3.at[base // 2], rs3_s.at[base // 2], rs3_r.at[base // 2]) for base in (2, 0)}
    end(row_loads)
    flipped[...] = mid_grad[...].T
    mid_acc[...] = jnp.zeros_like(mid_acc)
    run(0, 2, fetch_a, store_a, work_a)
    pl.semaphore_wait(barrier, len(peers))
    pairs[DOWN2] = [remote(g_down2.at[:, :, :, 1 - core], peer_in.at[pair_slot[DOWN2]], pair_s.at[DOWN2, 0], pair_r.at[DOWN2, 0], partner)]
    pairs[DOWN2][0].start()
    run(2, 5, fetch_a, store_a, work_a)
    issue_up(UP2, 0)
    add_pair(DOWN2)
    first[DOWN2].start()
    run(5, tiles, fetch_a, store_a, work_a)
    issue_up(UP2, 1)
    begin(fetch_b(0, 0) + fetch_c(0, 0))
    in_load = pltpu.make_async_copy(in_rows, left, row_sem.at[0])
    in_load.start()
    mid_grad[...] = mid_acc[...].reshape(mid_grad.shape).astype(jnp.bfloat16)
    run(0, 3, fetch_b, store_b, work_b)
    first[DOWN2].forward()
    add_pair(UP2)
    first[UP2].start()
    run(3, tiles, fetch_b, store_b, work_b)
    pl.semaphore_wait(pair_credit)
    issue_rows(0, 64)
    in_load.wait()
    flipped[...] = left[...].T
    run(0, 3, fetch_c, store_c, work_c)
    close(DOWN2)
    first[UP2].forward()
    pl.semaphore_wait(pair_credit)
    issue_up(UP1, 0)
    add_pair(DOWN1)
    pl.semaphore_wait(ring_credit.at[0], len(ring))
    first[DOWN1].start()
    run(3, tiles, fetch_c, store_c, work_c)
    issue_up(UP1, 1)
    close(UP2)
    second[UP2].start()
    add_pair(UP1)
    pl.semaphore_wait(ring_credit.at[1], len(ring))
    first[UP1].start()
    first[DOWN1].forward()
    second[UP2].forward()
    first[UP1].forward()
    second[UP2].finish()
    third[UP2].start()
    first[DOWN1].finish()
    first[UP1].finish()
    second[UP1].start()
    third[UP2].finish()
    second[UP1].forward()
    second[UP1].finish()
    third[UP1].start()
    third[UP1].finish()

    group_scale = 1.0 / 128.0
    grad_own = [total[mat, *pos] * group_scale for mat in range(SIDE)]
    partial = None
    for block in grad_own:
        square = block * block
        for row in range(ROWS // 8):
            for col in range(max(1, lanes // 128)):
                tile = square[8 * row:8 * row + 8, 128 * col:128 * col + 128]
                partial = tile if partial is None else partial + tile
    norm_line[line] = partial
    sends = []

    def spread(buf, slot, targets, send_sem, recv_sem):
        copies = []
        for i, target in enumerate(targets):
            copies.append(remote(buf.at[slot], buf.at[slot], send_sem.at[i], recv_sem.at[i], target))
            copies[i].start()
        return copies

    swap = spread(norm_line, line, line_peers, nc_s, nc_r)
    for target in range(SIDE):
        for i, mat in enumerate((0, 2)):
            send_g[target, i] = grad_own[mat][SUB * target:SUB * target + SUB]
    moves = []
    for hops in range(1, SIDE):
        other = lax.rem(member + hops, SIDE)
        copy = remote(send_g.at[other], recv_g.at[member], xg_s.at[hops - 1], xg_r.at[hops - 1], me - member + other)
        copy.start()
        moves.append(copy)
    recv_g[member] = send_g[member]
    for copy in swap:
        copy.wait_recv()
    norm_plane[plane] = jnp.sum(norm_line[...], axis=0)
    cross = spread(norm_plane, plane, plane_peers, na_s, na_r)
    for copy in cross:
        copy.wait_recv()
    running = jnp.sum(norm_plane[...], axis=0)
    sends = swap + cross + moves
    norm = jnp.sqrt(jnp.sum(jnp.sum(running, axis=1, keepdims=True), axis=0, keepdims=True))
    norm_out[...] = jnp.broadcast_to(norm, norm_out.shape)
    clip_scale = jnp.minimum(1.0, clip_ref[0] / (norm + NORM_EPS))
    learn_rate = lr_ref[0]

    end(state_loads)
    for i in range(SIDES):
        fresh = adam_step(grad_own[2 * i + 1] * clip_scale, down_state[0, i], down_state[1, i], down_state[2, i], learn_rate)
        for field in range(COLOURS):
            down_state[field, i] = fresh[field]
        w_own[2 + i] = fresh[0].astype(jnp.bfloat16)

    def spot(group, coords, colour, side):
        lane = ALL if side is None else pl.ds(half * side, half)
        index = [pl.ds(2 * group, 2), ALL, ALL, ALL, core, pl.ds(CHUNK * colour, CHUNK), lane]
        for axis, coord in coords.items():
            index[1 + axis] = coord
        return w_out.at[tuple(index)]

    handed = []

    class Gather:
        def __init__(self, group, level):
            self.group, self.level = group, level
            self.copies = {}

        def spot(self, colour, coord, side):
            order = ORDERS[colour]
            coords = {axis: pos[axis] for axis in order[:self.level]}
            coords[order[self.level]] = coord
            return spot(self.group, coords, colour, side)

        def near(self, colour, side):
            axis = ORDERS[colour][self.level]
            coord = step(axis, 1 if side == 0 else 3)
            return coord, device(axis, coord)

        def send(self, colour, side, kind, src, dst):
            spots = (self.group, self.level, colour, side, kind)
            copy = remote(src, dst, ag_s.at[spots], ag_r.at[spots], self.near(colour, side)[1])
            copy.start()
            self.copies[colour, side, kind] = copy

        def hand(self, ref, slot):
            copy = remote(ref, ref, out_s.at[self.group, slot], out_r.at[self.group, slot], partner)
            copy.start()
            handed.append(copy)

        def start_direct(self):
            for hops in (2, 1, 3):
                for colour in range(COLOURS):
                    axis = ORDERS[colour][self.level]
                    dst = self.spot(colour, pos[axis], None)
                    src = w_own.at[pl.ds(2 * self.group, 2), pl.ds(CHUNK * colour, CHUNK)] if self.level == 2 else dst
                    spots = (self.group, self.level, colour, 0, hops - 1)
                    copy = remote(src, dst, ag_s.at[spots], ag_r.at[spots], device(axis, step(axis, hops)))
                    copy.start()
                    self.copies[colour, hops] = copy

        def finish_direct(self):
            for copy in self.copies.values():
                copy.wait_recv()

        def start(self):
            for kind in range(SIDES):
                for colour in range(COLOURS):
                    for side in range(SIDES):
                        ref = self.spot(colour, pos[ORDERS[colour][0]], side if kind == 0 else 1 - side)
                        self.send(colour, side, kind, ref, ref)
            for colour in range(COLOURS):
                self.hand(self.spot(colour, pos[ORDERS[colour][0]], None), 5 * colour)

        def forward(self):
            for colour in range(COLOURS):
                for side in range(SIDES):
                    self.copies[colour, side, FAR].wait_recv()
                    ref = self.spot(colour, self.near(colour, 1 - side)[0], side)
                    self.send(colour, side, 2, ref, ref)

        def finish(self):
            for colour in range(COLOURS):
                for side in range(SIDES):
                    self.copies[colour, side, NEAR].wait_recv()
                    self.hand(self.spot(colour, self.near(colour, 1 - side)[0], None), 5 * colour + 1 + side)
            for colour in range(COLOURS):
                for side in range(SIDES):
                    self.copies[colour, side, PASS].wait_recv()
                    self.hand(self.spot(colour, step(ORDERS[colour][0], 2), side), 5 * colour + 3 + side)

    keeps = [pltpu.make_async_copy(w_own.at[pl.ds(2 * group, 2)], w_out.at[pl.ds(2 * group, 2), *pos, core], own_sem.at[group]) for group in range(SIDES)]
    gathers = {(group, level): Gather(group, level) for group in range(SIDES) for level in range(COLOURS)}
    gathers[DOWN, EARLY].start_direct()
    keeps[DOWN].start()

    for copy in moves:
        copy.wait_recv()
    for i in range(SIDES):
        for col in range(SIDE):
            cols = slice(col * lanes, (col + 1) * lanes)
            scaled = recv_g[col, i] * clip_scale
            fresh = adam_step(scaled, up_state[0, i, :, cols], up_state[1, i, :, cols], up_state[2, i, :, cols], learn_rate)
            for field in range(COLOURS):
                up_state[field, i, :, cols] = fresh[field]
            send_w[col, i] = fresh[0]
    moves = []
    for hops in range(1, SIDE):
        other = lax.rem(member + hops, SIDE)
        copy = remote(send_w.at[other], recv_w.at[member], xw_s.at[hops - 1], xw_r.at[hops - 1], me - member + other)
        copy.start()
        moves.append(copy)
    recv_w[member] = send_w[member]
    state_stores = [pltpu.make_async_copy(up_state, up_out, state_sem.at[0, 0]), pltpu.make_async_copy(down_state, down_out, state_sem.at[0, 1])]
    begin(state_stores)
    gathers[DOWN, EARLY].finish_direct()
    keeps[DOWN].wait()
    gathers[DOWN, MIDDLE].start_direct()
    for copy in moves:
        copy.wait_recv()
    sends = sends + moves
    for i in range(SIDES):
        for source in range(SIDE):
            block_tmp[SUB * source:SUB * source + SUB] = recv_w[source, i]
        w_own[i] = block_tmp[...].astype(jnp.bfloat16)
    gathers[UP, EARLY].start_direct()
    keeps[UP].start()
    gathers[DOWN, MIDDLE].finish_direct()
    gathers[DOWN, LAST].start()
    gathers[UP, EARLY].finish_direct()
    keeps[UP].wait()
    gathers[UP, MIDDLE].start_direct()
    gathers[UP, MIDDLE].finish_direct()
    gathers[UP, LAST].start()
    gathers[DOWN, LAST].forward()
    gathers[DOWN, LAST].finish()
    gathers[UP, LAST].forward()
    gathers[UP, LAST].finish()
    for gather in gathers.values():
        sends = sends + list(gather.copies.values())
    for phase in [first[DOWN1], first[UP1]] + list(second.values()) + list(third.values()):
        phase.drain()
    for mat in mat_order:
        for copy in pairs[mat]:
            copy.wait_send()
    for copy in sends:
        copy.wait_send()
    for copy in handed + state_stores:
        copy.wait()


def place_kernel(lanes, w_ref, up_ref, down_ref, norm_ref, *refs):
    weights, states, norm_out, (w_tmp, up_tmp, down_tmp, in_sem, state_in, out_sem, state_out) = refs[:4], refs[4:16], refs[16], refs[17:]
    norm_out[0] = jnp.max(norm_ref[...])
    loads = [[pltpu.make_async_copy(w_ref.at[mat % SIDES * 2 + mat // SIDES, z], w_tmp.at[mat, z], in_sem.at[mat, z]) for z in range(SIDE)] for mat in range(SIDE)]
    for row in loads:
        for copy in row:
            copy.start()
    state_loads = [pltpu.make_async_copy(up_ref, up_tmp, state_in.at[0]), pltpu.make_async_copy(down_ref, down_tmp, state_in.at[1])]
    for copy in state_loads:
        copy.start()
    stores = []
    for mat in range(SIDE):
        for z in range(SIDE):
            loads[mat][z].wait()
            if mat % SIDES:
                copies = [pltpu.make_async_copy(w_tmp.at[mat, z], weights[mat].at[z], out_sem.at[mat, z, 0])]
            else:
                copies = []
                for member in range(SIDE):
                    src = w_tmp.at[mat, z, :, :, member // SIDES, member % SIDES]
                    copies.append(pltpu.make_async_copy(src, weights[mat].at[z, :, :, :, pl.ds(member * lanes, lanes)], out_sem.at[mat, z, member]))
            for copy in copies:
                copy.start()
            stores = stores + copies
    for copy in state_loads:
        copy.wait()
    for field in range(COLOURS):
        for mat in range(SIDE):
            src = (down_tmp if mat % SIDES else up_tmp).at[field, mat // SIDES]
            copy = pltpu.make_async_copy(src, states[4 * field + mat], state_out.at[field, mat])
            copy.start()
            stores.append(copy)
    for copy in stores:
        copy.wait()


def comm_call(lanes, grad_down2, rows, weights_in, hidden, masters, moms, vels, learn_rate, clip_norm):
    up = (SIDE, SIDE, SIDES, ROWS, SIDE * lanes)
    down = (SIDE, SIDE, SIDE, SIDES, ROWS, lanes)
    local_rows = rows[0].shape[0]
    half = lanes // 2
    f32 = jnp.float32
    bf16 = jnp.bfloat16
    up_shape = (COLOURS, SIDES, SUB, SIDE * lanes)
    down_shape = (COLOURS, SIDES, ROWS, lanes)
    dma = pltpu.SemaphoreType.DMA
    vmem = pl.BlockSpec(memory_space=pltpu.VMEM)
    smem = pl.BlockSpec(memory_space=pltpu.SMEM)
    hbm = pl.BlockSpec(memory_space=pl.ANY)
    scratch = [
        pltpu.VMEM((SIDE, SIDE, SIDE, SIDE, ROWS, lanes), f32),
        pltpu.VMEM((SIDES, SIDE, SIDE, SIDE, ROWS, lanes), f32),
        pltpu.VMEM((SIDES, COLOURS, SIDES, COLOURS, SIDE, SIDE, CHUNK, half), f32),
        pltpu.VMEM((SIDES, COLOURS, SIDES, COLOURS, SIDES, SIDE, CHUNK, half), f32),
        pltpu.VMEM((SIDES, COLOURS, COLOURS, SIDES, CHUNK, lanes), f32),
        pltpu.VMEM((8, 8, 128), f32),
        pltpu.VMEM((16, 8, 128), f32),
        pltpu.VMEM((SIDE, SIDES, SUB, lanes), f32),
        pltpu.VMEM((SIDE, SIDES, SUB, lanes), f32),
        pltpu.VMEM((SIDE, SIDES, SUB, lanes), f32),
        pltpu.VMEM((SIDE, SIDES, SUB, lanes), f32),
        pltpu.VMEM((ROWS, lanes), f32),
        pltpu.VMEM((SIDE, ROWS, lanes), jnp.bfloat16),
        pltpu.VMEM(up_shape, f32),
        pltpu.VMEM(down_shape, f32),
        pltpu.VMEM((local_rows, lanes), bf16),
        pltpu.VMEM((lanes, local_rows), bf16),
        pltpu.VMEM((SIDES, local_rows // SIDES, lanes), f32),
        pltpu.VMEM((local_rows, lanes), bf16),
        pltpu.VMEM((SIDES, TILE, lanes), bf16),
        pltpu.VMEM((SIDES, local_rows, TILE), bf16),
        pltpu.VMEM((SIDES, local_rows, TILE), f32),
        pltpu.VMEM((SIDES, SIDE, SIDE, SIDES, ROWS, TILE), f32),
        dma((SIDE, SIDE)), dma((COLOURS, SIDE)), dma((SIDE, SIDE)), dma((SIDE, SIDE)),
        dma((SIDE, COLOURS, SIDES, COLOURS)), dma((SIDE, COLOURS, SIDES, COLOURS)), dma((SIDES, COLOURS, SIDES, COLOURS)), dma((SIDES, COLOURS, SIDES, COLOURS)), dma((SIDES, COLOURS, COLOURS)), dma((SIDES, COLOURS, COLOURS)),
        dma((7,)), dma((7,)), dma((15,)), dma((15,)), dma((COLOURS,)), dma((COLOURS,)), dma((COLOURS,)), dma((COLOURS,)),
        dma((SIDES,)), dma((SIDES, COLOURS, COLOURS, SIDES, COLOURS)), dma((SIDES, COLOURS, COLOURS, SIDES, COLOURS)), dma((SIDES, 15)), dma((SIDES, 15)),
        dma((SIDES,)), dma((SIDES, COLOURS)), dma((SIDES,)), pltpu.SemaphoreType.REGULAR, pltpu.SemaphoreType.REGULAR((2,)),
    ]
    outs = pl.pallas_call(
        functools.partial(comm_kernel, lanes),
        name="reduce_update_gather",
        out_shape=[jax.ShapeDtypeStruct((SIDE, SIDE, SIDE, SIDE, SIDES, ROWS, lanes), bf16), jax.ShapeDtypeStruct(up_shape, f32), jax.ShapeDtypeStruct(down_shape, f32), jax.ShapeDtypeStruct((8, 128), f32), jax.ShapeDtypeStruct(up, f32), jax.ShapeDtypeStruct((3072, lanes), f32), jax.ShapeDtypeStruct(up, f32)],
        in_specs=[hbm] * 22 + [smem] * 2,
        out_specs=[hbm] * 3 + [vmem] + [hbm] * 3,
        scratch_shapes=scratch,
        compiler_params=pltpu.CompilerParams(collective_id=0, has_side_effects=True, vmem_limit_bytes=67043328),
    )(grad_down2.reshape(down), *rows, *weights_in, *hidden, *masters, *moms, *vels, learn_rate.reshape(1), clip_norm.reshape(1))
    split = (SIDE, SIDE, SIDES, SIDES, SIDES, ROWS, lanes)
    placed = pl.pallas_call(
        functools.partial(place_kernel, lanes),
        name="place_outputs",
        out_shape=[jax.ShapeDtypeStruct(split if mat % SIDES else up, bf16) for mat in range(SIDE)] + [jax.ShapeDtypeStruct(m.shape, f32) for m in masters] * 3 + [jax.ShapeDtypeStruct((1,), f32)],
        in_specs=[hbm] * 3 + [vmem],
        out_specs=[hbm] * 16 + [smem],
        scratch_shapes=[
            pltpu.VMEM((SIDE,) + split, bf16), pltpu.VMEM(up_shape, f32), pltpu.VMEM(down_shape, f32),
            dma((SIDE, SIDE)), dma((SIDES,)), dma((SIDE, SIDE, SIDE)), dma((COLOURS, SIDE)),
        ],
        compiler_params=pltpu.CompilerParams(vmem_limit_bytes=67043328),
    )(outs[0].reshape((4,) + split), *outs[1:4])
    weights = [placed[mat].reshape(masters[mat].shape[0] * 128, -1) for mat in range(SIDE)]
    return tuple(weights) + tuple(placed[4:16]) + (placed[16][0],)


def mat_tn(left, right):
    return lax.dot_general(left, right, (((0,), (0,)), ((), ())), preferred_element_type=jnp.float32)


def gelu_pair(pre):
    normal_cdf = 0.5 * (1.0 + lax.erf(pre * ROOT_HALF))
    density = jnp.exp(-0.5 * pre * pre) * INV_ROOT_TAU
    return pre * normal_cdf, normal_cdf + pre * density


def solution(mesh):
    rows_spec = P("data", None)
    full_spec = P(None, None)
    scalar_spec = P()

    def shard_body(act_in, grad_out, w_up1, w_down1, w_up2, w_down2, *rest):
        gel_up1, der_up1 = gelu_pair(jnp.dot(act_in, w_up1, preferred_element_type=jnp.float32))
        act_up1 = gel_up1.astype(jnp.bfloat16)
        mid_act = jnp.dot(act_up1, w_down1, preferred_element_type=jnp.float32).astype(jnp.bfloat16)
        gel_up2, der_up2 = gelu_pair(jnp.dot(mid_act, w_up2, preferred_element_type=jnp.float32))
        grad_down2 = mat_tn(gel_up2.astype(jnp.bfloat16), grad_out)
        return comm_call(768, grad_down2, (grad_out, mid_act, act_in), (w_down1, w_up2, w_down2), (der_up1, der_up2, act_up1), rest[0:4], rest[4:8], rest[8:12], rest[12], rest[13])

    in_specs = (rows_spec, rows_spec) + (full_spec,) * 4 + (rows_spec,) * 12 + (scalar_spec, scalar_spec)
    out_specs = (full_spec,) * 4 + (rows_spec,) * 12 + (scalar_spec,)
    return jax.shard_map(shard_body, mesh=mesh, in_specs=in_specs, out_specs=out_specs, check_vma=False)
```

```python
import functools
import math
import jax
import jax.numpy as jnp
from jax import lax
from jax.experimental import pallas as pl
from jax.experimental.pallas import tpu as pltpu
from jax.sharding import PartitionSpec as P

STEP = 20
BETA_ONE = 0.9
BETA_TWO = 0.95
EPSILON = 1e-8
NORM_EPS = 1e-6
CORR_ONE = 1.0 - BETA_ONE ** STEP
CORR_TWO = 1.0 - BETA_TWO ** STEP
ROOT_HALF = math.sqrt(0.5)
INV_ROOT_TAU = 1.0 / math.sqrt(2.0 * math.pi)

MESH = pl.DeviceIdType.MESH
UP1, DOWN1, UP2, DOWN2 = 0, 1, 2, 3
UP, DOWN = 0, 1
LAST, MIDDLE, EARLY = 0, 1, 2
FAR, NEAR, PASS = 0, 1, 2
STRIDES = (32, 8, 2)
ORDERS = ((2, 1, 0), (1, 0, 2), (0, 2, 1))
ROWS = 24
SUB = 6
CHUNK = 8
SIDE = 4
COLOURS = 3
SIDES = 2
ALL = slice(None)
WINDOW = 5
TILE = 512


def adam_step(scaled, master_old, mom_old, vel_old, learn_rate):
    mom_new = BETA_ONE * mom_old + (1.0 - BETA_ONE) * scaled
    vel_new = BETA_TWO * vel_old + (1.0 - BETA_TWO) * scaled * scaled
    master_new = master_old - learn_rate * (mom_new / CORR_ONE) / (jnp.sqrt(vel_new / CORR_TWO) + EPSILON)
    return master_new, mom_new, vel_new


def comm_kernel(lanes, *refs):
    (g_down2, grad_rows, mid_rows, in_rows, w_down1, w_up2, w_down2, der1, der2, act1), refs = refs[:10], refs[10:]
    states, refs = refs[:12], refs[12:]
    (lr_ref, clip_ref), refs = refs[:2], refs[2:]
    (w_out, up_out, down_out, norm_out, g_up1, g_down1, g_up2), refs = refs[:7], refs[7:]
    (total, peer_in, rs1, rs2, rs3, norm_line, norm_plane, send_g, recv_g, send_w, recv_w, block_tmp, w_own, up_state, down_state), refs = refs[:15], refs[15:]
    (left, flipped, mid_acc, mid_grad, w_tile, act_tile, der_tile, out_tile), refs = refs[:8], refs[8:]
    (load_sem, state_sem, pair_s, pair_r, rs1_s, rs1_r, rs2_s, rs2_r, rs3_s, rs3_r, nc_s, nc_r, na_s, na_r, xg_s, xg_r, xw_s, xw_r, own_sem, ag_s, ag_r, out_s, out_r) = refs[:23]
    row_sem, tile_sem, store_sem, pair_credit, ring_credit = refs[23:]
    half = lanes // 2
    me = lax.axis_index("data")
    core = lax.rem(me, SIDES)
    member = lax.rem(me, 4)
    pos = (me // 32, lax.rem(me // 8, 4), lax.rem(me // 2, 4))
    partner = me + 1 - 2 * core

    def device(axis, coord):
        return me + (coord - pos[axis]) * STRIDES[axis]

    def step(axis, hops):
        return lax.rem(pos[axis] + hops, 4)

    def remote(src, dst, send_sem, recv_sem, target):
        return pltpu.make_async_remote_copy(src_ref=src, dst_ref=dst, send_sem=send_sem, recv_sem=recv_sem, device_id=(target,), device_id_type=MESH)

    line, plane = lax.rem(me, 8), me // 8
    line_peers = [me - line + lax.rem(line + hops, 8) for hops in range(1, 8)]
    plane_peers = [8 * lax.rem(plane + hops, 16) + line for hops in range(1, 16)]
    peers = line_peers + plane_peers
    barrier = pltpu.get_barrier_semaphore()
    for peer in peers:
        pl.semaphore_signal(barrier, device_id=(peer,), device_id_type=MESH)

    grads = (g_up1, g_down1, g_up2, g_down2)
    mat_order = (3, 2, 1, 0)
    pair_slot = (1, 0, 1, 0)
    loads, pairs = {0: [], 2: []}, {0: [], 2: []}

    def issue_up(mat, x_low):
        for x in (x_low, x_low + 2):
            for owner in (1 - core, core):
                col = pl.multiple_of((x_low * 2 + owner) * lanes, lanes)
                src = grads[mat].at[:, :, x // SIDES, :, pl.ds(col, lanes)]
                if owner is core:
                    loads[mat].append(pltpu.make_async_copy(src, total.at[mat, :, :, x], load_sem.at[mat, x]))
                    loads[mat][-1].start()
                else:
                    pairs[mat].append(remote(src, peer_in.at[pair_slot[mat], :, :, x], pair_s.at[mat, x], pair_r.at[mat, x], partner))
                    pairs[mat][-1].start()

    def issue_rows(low, high):
        def move(i, carry):
            place = (i // 16, lax.rem(i // SIDE, 4), lax.rem(i, SIDE))
            there = g_down1.at[pl.ds(pl.multiple_of(i * 2 * ROWS + (1 - core) * ROWS, 8), ROWS)]
            here = g_down1.at[pl.ds(pl.multiple_of(i * 2 * ROWS + core * ROWS, 8), ROWS)]
            remote(there, peer_in.at[(pair_slot[DOWN1],) + place], pair_s.at[DOWN1, 0], pair_r.at[DOWN1, 0], partner).start()
            pltpu.make_async_copy(here, total.at[(1,) + place], load_sem.at[DOWN1, 0]).start()
            return carry

        lax.fori_loop(low, high, move, 0)

    loads[DOWN1] = [pltpu.make_async_copy(total.at[1], total.at[1], load_sem.at[DOWN1, 0])]
    pairs[DOWN1] = [remote(peer_in.at[pair_slot[DOWN1]], peer_in.at[pair_slot[DOWN1]], pair_s.at[DOWN1, 0], pair_r.at[DOWN1, 0], partner)]
    loads[DOWN2] = [pltpu.make_async_copy(g_down2.at[:, :, :, core], total.at[3], load_sem.at[DOWN2, 0])]

    tiles = SIDE * lanes // TILE

    def span(t):
        return pl.ds(pl.multiple_of(t * TILE, TILE), TILE)

    def fetch_a(t, slot):
        return [
            pltpu.make_async_copy(w_down2.at[span(t)], w_tile.at[slot], tile_sem.at[slot, 0]),
            pltpu.make_async_copy(w_up2.at[:, span(t)], act_tile.at[slot, pl.ds(0, lanes)], tile_sem.at[slot, 1]),
            pltpu.make_async_copy(der2.at[:, span(t)], der_tile.at[slot], tile_sem.at[slot, 2]),
        ]

    def fetch_b(t, slot):
        return [pltpu.make_async_copy(act1.at[:, span(t)], act_tile.at[slot], tile_sem.at[slot, 1])]

    def fetch_c(t, slot):
        return [
            pltpu.make_async_copy(w_down1.at[span(t)], w_tile.at[slot], tile_sem.at[slot, 0]),
            pltpu.make_async_copy(der1.at[:, span(t)], der_tile.at[slot], tile_sem.at[slot, 2]),
        ]

    def begin(copies):
        for copy in copies:
            copy.start()

    def end(copies):
        for copy in copies:
            copy.wait()

    row_loads = [pltpu.make_async_copy(grad_rows, left, row_sem.at[0]), pltpu.make_async_copy(mid_rows, mid_grad, row_sem.at[1])]
    begin(row_loads)
    begin(fetch_a(0, 0))
    begin(loads[DOWN2])
    state_loads = []
    for field in range(COLOURS):
        for mat in range(SIDE):
            dst = (down_state if mat % SIDES else up_state).at[field, mat // SIDES]
            state_loads.append(pltpu.make_async_copy(states[4 * field + mat], dst, state_sem.at[field, mat]))
    begin(state_loads)
    def store_a(t, slot):
        return [pltpu.make_async_copy(out_tile.at[slot], g_up2.at[:, :, :, :, span(t)], store_sem.at[slot])]

    def store_b(t, slot):
        return [pltpu.make_async_copy(mid_acc.at[slot], g_down1.at[span(t)], store_sem.at[slot])]

    def store_c(t, slot):
        return [pltpu.make_async_copy(out_tile.at[slot], g_up1.at[:, :, :, :, span(t)], store_sem.at[slot])]

    def run(first, last, fetch, store, work):
        def tile(t, carry):
            slot = lax.rem(t, SIDES)

            @pl.when(t + 1 < tiles)
            def _():
                begin(fetch(t + 1, 1 - slot))

            end(fetch(t, slot))

            @pl.when(t - first >= 2)
            def _():
                end(store(t - 2, slot))

            work(slot)
            begin(store(t, slot))
            return carry

        lax.fori_loop(first, last, tile, 0)
        for t in range(max(first, last - 2), last):
            end(store(t, t % 2))

    def dot(lhs, rhs, lhs_dim, rhs_dim):
        return lax.dot_general(lhs, rhs, (((lhs_dim,), (rhs_dim,)), ((), ())), preferred_element_type=jnp.float32)

    def work_a(slot):
        grad_act2 = dot(left[...], w_tile[slot], 1, 1).astype(jnp.bfloat16)
        grad_pre2 = (grad_act2.astype(jnp.float32) * der_tile[slot]).astype(jnp.bfloat16)
        out_tile[slot] = dot(flipped[...], grad_pre2, 1, 0).reshape(out_tile.shape[1:])
        mid_acc[...] += dot(grad_pre2, act_tile[slot, pl.ds(0, lanes)], 1, 1).reshape(mid_acc.shape)

    def work_b(slot):
        mid_acc[slot] = dot(act_tile[slot], mid_grad[...], 0, 0)

    def work_c(slot):
        grad_act1 = dot(mid_grad[...], w_tile[slot], 1, 1).astype(jnp.bfloat16)
        grad_pre1 = (grad_act1.astype(jnp.float32) * der_tile[slot]).astype(jnp.bfloat16)
        out_tile[slot] = dot(flipped[...], grad_pre1, 1, 0).reshape(out_tile.shape[1:])

    def part(mats, coords, colour, side):
        lane = ALL if side is None else pl.ds(half * side, half)
        index = [mats, ALL, ALL, ALL, pl.ds(CHUNK * colour, CHUNK), lane]
        for axis, coord in coords.items():
            index[1 + axis] = coord
        return tuple(index)

    class Phase:
        def __init__(self, level, base, buf, send_sem, recv_sem):
            self.level, self.base, self.buf, self.send_sem, self.recv_sem = level, base, buf, send_sem, recv_sem
            self.mats, self.count = (slice(base, base + 2), 2) if level else (base, 4)
            self.copies = {}

        def where(self, colour, coord):
            order = ORDERS[colour]
            coords = {axis: pos[axis] for axis in order[:self.level]}
            coords[order[self.level]] = coord
            return coords

        def row(self, colour, coord, side, i):
            coords = self.where(colour, coord)
            if self.level:
                return part(self.base + i, coords, colour, side)
            coords[min(axis for axis in range(COLOURS) if axis not in coords)] = i
            return part(self.mats, coords, colour, side)

        def send(self, colour, side, kind, src, target):
            copy = remote(src, self.buf.at[colour, side, kind], self.send_sem.at[colour, side, kind], self.recv_sem.at[colour, side, kind], target)
            copy.start()
            self.copies[colour, side, kind] = copy

        def near(self, colour, side):
            axis = ORDERS[colour][self.level]
            coord = step(axis, 1 if side == 0 else 3)
            return coord, device(axis, coord)

        def start(self):
            for kind in range(SIDES):
                for colour in range(COLOURS):
                    for side in range(SIDES):
                        coord, target = self.near(colour, side)
                        aim = step(ORDERS[colour][self.level], 2) if kind == 0 else coord
                        src = total.at[part(self.mats, self.where(colour, aim), colour, side if kind == 0 else 1 - side)]
                        self.send(colour, side, kind, src, target)

        def forward(self):
            for colour in range(COLOURS):
                for side in range(SIDES):
                    coord, target = self.near(colour, side)
                    self.copies[colour, side, FAR].wait_recv()

                    def add_own(i, carry, colour=colour, side=side, coord=coord):
                        self.buf[colour, side, FAR, i] = self.buf[colour, side, FAR, i] + total[self.row(colour, coord, side, i)]
                        return carry

                    lax.fori_loop(0, self.count, add_own, 0)
                    self.send(colour, side, 2, self.buf.at[colour, side, FAR], target)

        def finish(self):
            for colour in range(COLOURS):
                for side in range(SIDES):
                    self.copies[colour, 1 - side, NEAR].wait_recv()
                    self.copies[colour, side, PASS].wait_recv()

                    def add_both(i, carry, colour=colour, side=side):
                        own = self.row(colour, pos[ORDERS[colour][self.level]], side, i)
                        total[own] = total[own] + (self.buf[colour, 1 - side, NEAR, i] + self.buf[colour, side, PASS, i])
                        return carry

                    lax.fori_loop(0, self.count, add_both, 0)

        def drain(self):
            for copy in self.copies.values():
                copy.wait_send()

    ring_slot = (1, 0, 1, 0)
    class Direct:
        def __init__(self, base, buf, send_sem, recv_sem):
            self.base, self.buf, self.send_sem, self.recv_sem = base, buf, send_sem, recv_sem
            self.copies = {}

        def index(self, colour, coord, mats):
            coords = {axis: pos[axis] for axis in range(COLOURS)}
            coords[ORDERS[colour][2]] = coord
            return part(mats, coords, colour, None)

        def start(self):
            for hops in (2, 1, 3):
                for colour in range(COLOURS):
                    axis = ORDERS[colour][2]
                    coord = step(axis, hops)
                    spots = (colour, hops - 1)
                    src = total.at[self.index(colour, coord, slice(self.base, self.base + 2))]
                    copy = remote(src, self.buf.at[spots], self.send_sem.at[spots], self.recv_sem.at[spots], device(axis, coord))
                    copy.start()
                    self.copies[spots] = copy

        def finish(self):
            for colour in range(COLOURS):
                for hops in range(COLOURS):
                    self.copies[colour, hops].wait_recv()
                for mat in range(SIDES):
                    own = self.index(colour, pos[ORDERS[colour][2]], self.base + mat)
                    total[own] = (total[own] + self.buf[colour, 0, mat]) + (self.buf[colour, 1, mat] + self.buf[colour, 2, mat])

        def drain(self):
            for copy in self.copies.values():
                copy.wait_send()

    first = {mat: Phase(0, mat, rs1.at[ring_slot[mat]], rs1_s.at[mat], rs1_r.at[mat]) for mat in mat_order}

    def add_pair(mat):
        end(loads[mat])
        for copy in pairs[mat]:
            copy.wait_recv()

        def add(i, carry):
            total[mat, i // SIDE, lax.rem(i, SIDE)] = total[mat, i // SIDE, lax.rem(i, SIDE)] + peer_in[pair_slot[mat], i // SIDE, lax.rem(i, SIDE)]
            return carry

        lax.fori_loop(0, 16, add, 0)
        if mat >= 2:
            pl.semaphore_signal(pair_credit, device_id=(partner,), device_id_type=MESH)

    ring = [device(axis, step(axis, hops)) for axis in range(COLOURS) for hops in (1, 3)]

    def close(mat):
        first[mat].finish()
        first[mat].drain()
        for peer in ring:
            pl.semaphore_signal(ring_credit.at[ring_slot[mat]], device_id=(peer,), device_id_type=MESH)

    second = {base: Phase(1, base, rs2.at[base // 2], rs2_s.at[base // 2], rs2_r.at[base // 2]) for base in (2, 0)}
    third = {base: Direct(base, rs3.at[base // 2], rs3_s.at[base // 2], rs3_r.at[base // 2]) for base in (2, 0)}
    end(row_loads)
    flipped[...] = mid_grad[...].T
    mid_acc[...] = jnp.zeros_like(mid_acc)
    run(0, 1, fetch_a, store_a, work_a)
    pl.semaphore_wait(barrier, len(peers))
    pairs[DOWN2] = [remote(g_down2.at[:, :, :, 1 - core], peer_in.at[pair_slot[DOWN2]], pair_s.at[DOWN2, 0], pair_r.at[DOWN2, 0], partner)]
    pairs[DOWN2][0].start()
    run(1, 4, fetch_a, store_a, work_a)
    issue_up(UP2, 0)
    add_pair(DOWN2)
    first[DOWN2].start()
    run(4, tiles, fetch_a, store_a, work_a)
    issue_up(UP2, 1)
    begin(fetch_b(0, 0) + fetch_c(0, 0))
    in_load = pltpu.make_async_copy(in_rows, left, row_sem.at[0])
    in_load.start()
    mid_grad[...] = mid_acc[...].reshape(mid_grad.shape).astype(jnp.bfloat16)
    run(0, 3, fetch_b, store_b, work_b)
    first[DOWN2].forward()
    add_pair(UP2)
    first[UP2].start()
    run(3, tiles, fetch_b, store_b, work_b)
    pl.semaphore_wait(pair_credit)
    issue_rows(0, 64)
    in_load.wait()
    flipped[...] = left[...].T
    run(0, 3, fetch_c, store_c, work_c)
    close(DOWN2)
    first[UP2].forward()
    pl.semaphore_wait(pair_credit)
    issue_up(UP1, 0)
    add_pair(DOWN1)
    pl.semaphore_wait(ring_credit.at[0], len(ring))
    first[DOWN1].start()
    run(3, tiles, fetch_c, store_c, work_c)
    issue_up(UP1, 1)
    close(UP2)
    second[UP2].start()
    add_pair(UP1)
    pl.semaphore_wait(ring_credit.at[1], len(ring))
    first[UP1].start()
    first[DOWN1].forward()
    second[UP2].forward()
    first[UP1].forward()
    second[UP2].finish()
    third[UP2].start()
    first[DOWN1].finish()
    first[UP1].finish()
    second[UP1].start()
    third[UP2].finish()
    second[UP1].forward()
    second[UP1].finish()
    third[UP1].start()
    third[UP1].finish()

    group_scale = 1.0 / 128.0
    grad_own = [total[mat, *pos] * group_scale for mat in range(SIDE)]
    partial = None
    for block in grad_own:
        square = block * block
        for row in range(ROWS // 8):
            for col in range(max(1, lanes // 128)):
                tile = square[8 * row:8 * row + 8, 128 * col:128 * col + 128]
                partial = tile if partial is None else partial + tile
    norm_line[line] = partial
    sends = []

    def spread(buf, slot, targets, send_sem, recv_sem):
        copies = []
        for i, target in enumerate(targets):
            copies.append(remote(buf.at[slot], buf.at[slot], send_sem.at[i], recv_sem.at[i], target))
            copies[i].start()
        return copies

    swap = spread(norm_line, line, line_peers, nc_s, nc_r)
    for target in range(SIDE):
        for i, mat in enumerate((0, 2)):
            send_g[target, i] = grad_own[mat][SUB * target:SUB * target + SUB]
    moves = []
    for hops in range(1, SIDE):
        other = lax.rem(member + hops, SIDE)
        copy = remote(send_g.at[other], recv_g.at[member], xg_s.at[hops - 1], xg_r.at[hops - 1], me - member + other)
        copy.start()
        moves.append(copy)
    recv_g[member] = send_g[member]
    for copy in swap:
        copy.wait_recv()
    norm_plane[plane] = jnp.sum(norm_line[...], axis=0)
    cross = spread(norm_plane, plane, plane_peers, na_s, na_r)
    for copy in cross:
        copy.wait_recv()
    running = jnp.sum(norm_plane[...], axis=0)
    sends = swap + cross + moves
    norm = jnp.sqrt(jnp.sum(jnp.sum(running, axis=1, keepdims=True), axis=0, keepdims=True))
    norm_out[...] = jnp.broadcast_to(norm, norm_out.shape)
    clip_scale = jnp.minimum(1.0, clip_ref[0] / (norm + NORM_EPS))
    learn_rate = lr_ref[0]

    end(state_loads)
    for i in range(SIDES):
        fresh = adam_step(grad_own[2 * i + 1] * clip_scale, down_state[0, i], down_state[1, i], down_state[2, i], learn_rate)
        for field in range(COLOURS):
            down_state[field, i] = fresh[field]
        w_own[2 + i] = fresh[0].astype(jnp.bfloat16)

    def spot(group, coords, colour, side):
        lane = ALL if side is None else pl.ds(half * side, half)
        index = [pl.ds(2 * group, 2), ALL, ALL, ALL, core, pl.ds(CHUNK * colour, CHUNK), lane]
        for axis, coord in coords.items():
            index[1 + axis] = coord
        return w_out.at[tuple(index)]

    handed = []

    class Gather:
        def __init__(self, group, level):
            self.group, self.level = group, level
            self.copies = {}

        def spot(self, colour, coord, side):
            order = ORDERS[colour]
            coords = {axis: pos[axis] for axis in order[:self.level]}
            coords[order[self.level]] = coord
            return spot(self.group, coords, colour, side)

        def near(self, colour, side):
            axis = ORDERS[colour][self.level]
            coord = step(axis, 1 if side == 0 else 3)
            return coord, device(axis, coord)

        def send(self, colour, side, kind, src, dst):
            spots = (self.group, self.level, colour, side, kind)
            copy = remote(src, dst, ag_s.at[spots], ag_r.at[spots], self.near(colour, side)[1])
            copy.start()
            self.copies[colour, side, kind] = copy

        def hand(self, ref, slot):
            copy = remote(ref, ref, out_s.at[self.group, slot], out_r.at[self.group, slot], partner)
            copy.start()
            handed.append(copy)

        def start_direct(self):
            for hops in (2, 1, 3):
                for colour in range(COLOURS):
                    axis = ORDERS[colour][self.level]
                    dst = self.spot(colour, pos[axis], None)
                    src = w_own.at[pl.ds(2 * self.group, 2), pl.ds(CHUNK * colour, CHUNK)] if self.level == 2 else dst
                    spots = (self.group, self.level, colour, 0, hops - 1)
                    copy = remote(src, dst, ag_s.at[spots], ag_r.at[spots], device(axis, step(axis, hops)))
                    copy.start()
                    self.copies[colour, hops] = copy

        def finish_direct(self):
            for copy in self.copies.values():
                copy.wait_recv()

        def start(self):
            for kind in range(SIDES):
                for colour in range(COLOURS):
                    for side in range(SIDES):
                        ref = self.spot(colour, pos[ORDERS[colour][0]], side if kind == 0 else 1 - side)
                        self.send(colour, side, kind, ref, ref)
            for colour in range(COLOURS):
                self.hand(self.spot(colour, pos[ORDERS[colour][0]], None), 5 * colour)

        def forward(self):
            for colour in range(COLOURS):
                for side in range(SIDES):
                    self.copies[colour, side, FAR].wait_recv()
                    ref = self.spot(colour, self.near(colour, 1 - side)[0], side)
                    self.send(colour, side, 2, ref, ref)

        def finish(self):
            for colour in range(COLOURS):
                for side in range(SIDES):
                    self.copies[colour, side, NEAR].wait_recv()
                    self.hand(self.spot(colour, self.near(colour, 1 - side)[0], None), 5 * colour + 1 + side)
            for colour in range(COLOURS):
                for side in range(SIDES):
                    self.copies[colour, side, PASS].wait_recv()
                    self.hand(self.spot(colour, step(ORDERS[colour][0], 2), side), 5 * colour + 3 + side)

    keeps = [pltpu.make_async_copy(w_own.at[pl.ds(2 * group, 2)], w_out.at[pl.ds(2 * group, 2), *pos, core], own_sem.at[group]) for group in range(SIDES)]
    gathers = {(group, level): Gather(group, level) for group in range(SIDES) for level in range(COLOURS)}
    gathers[DOWN, EARLY].start_direct()
    keeps[DOWN].start()

    for copy in moves:
        copy.wait_recv()
    for i in range(SIDES):
        for col in range(SIDE):
            cols = slice(col * lanes, (col + 1) * lanes)
            scaled = recv_g[col, i] * clip_scale
            fresh = adam_step(scaled, up_state[0, i, :, cols], up_state[1, i, :, cols], up_state[2, i, :, cols], learn_rate)
            for field in range(COLOURS):
                up_state[field, i, :, cols] = fresh[field]
            send_w[col, i] = fresh[0]
    moves = []
    for hops in range(1, SIDE):
        other = lax.rem(member + hops, SIDE)
        copy = remote(send_w.at[other], recv_w.at[member], xw_s.at[hops - 1], xw_r.at[hops - 1], me - member + other)
        copy.start()
        moves.append(copy)
    recv_w[member] = send_w[member]
    state_stores = [pltpu.make_async_copy(up_state, up_out, state_sem.at[0, 0]), pltpu.make_async_copy(down_state, down_out, state_sem.at[0, 1])]
    begin(state_stores)
    gathers[DOWN, EARLY].finish_direct()
    keeps[DOWN].wait()
    gathers[DOWN, MIDDLE].start_direct()
    for copy in moves:
        copy.wait_recv()
    sends = sends + moves
    for i in range(SIDES):
        for source in range(SIDE):
            block_tmp[SUB * source:SUB * source + SUB] = recv_w[source, i]
        w_own[i] = block_tmp[...].astype(jnp.bfloat16)
    gathers[UP, EARLY].start_direct()
    keeps[UP].start()
    gathers[DOWN, MIDDLE].finish_direct()
    gathers[DOWN, LAST].start()
    gathers[UP, EARLY].finish_direct()
    keeps[UP].wait()
    gathers[UP, MIDDLE].start_direct()
    gathers[DOWN, LAST].forward()
    gathers[UP, MIDDLE].finish_direct()
    gathers[UP, LAST].start()
    gathers[DOWN, LAST].finish()
    gathers[UP, LAST].forward()
    gathers[UP, LAST].finish()
    for gather in gathers.values():
        sends = sends + list(gather.copies.values())
    for phase in [first[DOWN1], first[UP1]] + list(second.values()) + list(third.values()):
        phase.drain()
    for mat in mat_order:
        for copy in pairs[mat]:
            copy.wait_send()
    for copy in sends:
        copy.wait_send()
    for copy in handed + state_stores:
        copy.wait()


def place_kernel(lanes, w_ref, up_ref, down_ref, norm_ref, *refs):
    weights, states, norm_out, (w_tmp, up_tmp, down_tmp, in_sem, state_in, out_sem, state_out) = refs[:4], refs[4:16], refs[16], refs[17:]
    norm_out[0] = jnp.max(norm_ref[...])
    loads = [[pltpu.make_async_copy(w_ref.at[mat % SIDES * 2 + mat // SIDES, z], w_tmp.at[mat, z], in_sem.at[mat, z]) for z in range(SIDE)] for mat in range(SIDE)]
    queue = [copy for row in loads for copy in row]
    for copy in queue[:WINDOW]:
        copy.start()
    state_loads = [pltpu.make_async_copy(up_ref, up_tmp, state_in.at[0]), pltpu.make_async_copy(down_ref, down_tmp, state_in.at[1])]
    for copy in state_loads:
        copy.start()
    stores = []
    for mat in range(SIDE):
        for z in range(SIDE):
            loads[mat][z].wait()
            ahead = 4 * mat + z + WINDOW
            if ahead < len(queue):
                queue[ahead].start()
            if mat % SIDES:
                copies = [pltpu.make_async_copy(w_tmp.at[mat, z], weights[mat].at[z], out_sem.at[mat, z, 0])]
            else:
                copies = []
                for member in range(SIDE):
                    src = w_tmp.at[mat, z, :, :, member // SIDES, member % SIDES]
                    copies.append(pltpu.make_async_copy(src, weights[mat].at[z, :, :, :, pl.ds(member * lanes, lanes)], out_sem.at[mat, z, member]))
            for copy in copies:
                copy.start()
            stores = stores + copies
    for copy in state_loads:
        copy.wait()
    for field in range(COLOURS):
        for mat in range(SIDE):
            src = (down_tmp if mat % SIDES else up_tmp).at[field, mat // SIDES]
            copy = pltpu.make_async_copy(src, states[4 * field + mat], state_out.at[field, mat])
            copy.start()
            stores.append(copy)
    for copy in stores:
        copy.wait()


def comm_call(lanes, grad_down2, rows, weights_in, hidden, masters, moms, vels, learn_rate, clip_norm):
    up = (SIDE, SIDE, SIDES, ROWS, SIDE * lanes)
    down = (SIDE, SIDE, SIDE, SIDES, ROWS, lanes)
    local_rows = rows[0].shape[0]
    half = lanes // 2
    f32 = jnp.float32
    bf16 = jnp.bfloat16
    up_shape = (COLOURS, SIDES, SUB, SIDE * lanes)
    down_shape = (COLOURS, SIDES, ROWS, lanes)
    dma = pltpu.SemaphoreType.DMA
    vmem = pl.BlockSpec(memory_space=pltpu.VMEM)
    smem = pl.BlockSpec(memory_space=pltpu.SMEM)
    hbm = pl.BlockSpec(memory_space=pl.ANY)
    scratch = [
        pltpu.VMEM((SIDE, SIDE, SIDE, SIDE, ROWS, lanes), f32),
        pltpu.VMEM((SIDES, SIDE, SIDE, SIDE, ROWS, lanes), f32),
        pltpu.VMEM((SIDES, COLOURS, SIDES, COLOURS, SIDE, SIDE, CHUNK, half), f32),
        pltpu.VMEM((SIDES, COLOURS, SIDES, COLOURS, SIDES, SIDE, CHUNK, half), f32),
        pltpu.VMEM((SIDES, COLOURS, COLOURS, SIDES, CHUNK, lanes), f32),
        pltpu.VMEM((8, 8, 128), f32),
        pltpu.VMEM((16, 8, 128), f32),
        pltpu.VMEM((SIDE, SIDES, SUB, lanes), f32),
        pltpu.VMEM((SIDE, SIDES, SUB, lanes), f32),
        pltpu.VMEM((SIDE, SIDES, SUB, lanes), f32),
        pltpu.VMEM((SIDE, SIDES, SUB, lanes), f32),
        pltpu.VMEM((ROWS, lanes), f32),
        pltpu.VMEM((SIDE, ROWS, lanes), jnp.bfloat16),
        pltpu.VMEM(up_shape, f32),
        pltpu.VMEM(down_shape, f32),
        pltpu.VMEM((local_rows, lanes), bf16),
        pltpu.VMEM((lanes, local_rows), bf16),
        pltpu.VMEM((SIDES, local_rows // SIDES, lanes), f32),
        pltpu.VMEM((local_rows, lanes), bf16),
        pltpu.VMEM((SIDES, TILE, lanes), bf16),
        pltpu.VMEM((SIDES, local_rows, TILE), bf16),
        pltpu.VMEM((SIDES, local_rows, TILE), f32),
        pltpu.VMEM((SIDES, SIDE, SIDE, SIDES, ROWS, TILE), f32),
        dma((SIDE, SIDE)), dma((COLOURS, SIDE)), dma((SIDE, SIDE)), dma((SIDE, SIDE)),
        dma((SIDE, COLOURS, SIDES, COLOURS)), dma((SIDE, COLOURS, SIDES, COLOURS)), dma((SIDES, COLOURS, SIDES, COLOURS)), dma((SIDES, COLOURS, SIDES, COLOURS)), dma((SIDES, COLOURS, COLOURS)), dma((SIDES, COLOURS, COLOURS)),
        dma((7,)), dma((7,)), dma((15,)), dma((15,)), dma((COLOURS,)), dma((COLOURS,)), dma((COLOURS,)), dma((COLOURS,)),
        dma((SIDES,)), dma((SIDES, COLOURS, COLOURS, SIDES, COLOURS)), dma((SIDES, COLOURS, COLOURS, SIDES, COLOURS)), dma((SIDES, 15)), dma((SIDES, 15)),
        dma((SIDES,)), dma((SIDES, COLOURS)), dma((SIDES,)), pltpu.SemaphoreType.REGULAR, pltpu.SemaphoreType.REGULAR((2,)),
    ]
    outs = pl.pallas_call(
        functools.partial(comm_kernel, lanes),
        name="reduce_update_gather",
        out_shape=[jax.ShapeDtypeStruct((SIDE, SIDE, SIDE, SIDE, SIDES, ROWS, lanes), bf16), jax.ShapeDtypeStruct(up_shape, f32), jax.ShapeDtypeStruct(down_shape, f32), jax.ShapeDtypeStruct((8, 128), f32), jax.ShapeDtypeStruct(up, f32), jax.ShapeDtypeStruct((3072, lanes), f32), jax.ShapeDtypeStruct(up, f32)],
        in_specs=[hbm] * 22 + [smem] * 2,
        out_specs=[hbm] * 3 + [vmem] + [hbm] * 3,
        scratch_shapes=scratch,
        compiler_params=pltpu.CompilerParams(collective_id=0, has_side_effects=True, vmem_limit_bytes=67043328),
    )(grad_down2.reshape(down), *rows, *weights_in, *hidden, *masters, *moms, *vels, learn_rate.reshape(1), clip_norm.reshape(1))
    split = (SIDE, SIDE, SIDES, SIDES, SIDES, ROWS, lanes)
    placed = pl.pallas_call(
        functools.partial(place_kernel, lanes),
        name="place_outputs",
        out_shape=[jax.ShapeDtypeStruct(split if mat % SIDES else up, bf16) for mat in range(SIDE)] + [jax.ShapeDtypeStruct(m.shape, f32) for m in masters] * 3 + [jax.ShapeDtypeStruct((1,), f32)],
        in_specs=[hbm] * 3 + [vmem],
        out_specs=[hbm] * 16 + [smem],
        scratch_shapes=[
            pltpu.VMEM((SIDE,) + split, bf16), pltpu.VMEM(up_shape, f32), pltpu.VMEM(down_shape, f32),
            dma((SIDE, SIDE)), dma((SIDES,)), dma((SIDE, SIDE, SIDE)), dma((COLOURS, SIDE)),
        ],
        compiler_params=pltpu.CompilerParams(vmem_limit_bytes=67043328),
    )(outs[0].reshape((4,) + split), *outs[1:4])
    weights = [placed[mat].reshape(masters[mat].shape[0] * 128, -1) for mat in range(SIDE)]
    return tuple(weights) + tuple(placed[4:16]) + (placed[16][0],)


def mat_tn(left, right):
    return lax.dot_general(left, right, (((0,), (0,)), ((), ())), preferred_element_type=jnp.float32)


def gelu_pair(pre):
    normal_cdf = 0.5 * (1.0 + lax.erf(pre * ROOT_HALF))
    density = jnp.exp(-0.5 * pre * pre) * INV_ROOT_TAU
    return pre * normal_cdf, normal_cdf + pre * density


def solution(mesh):
    rows_spec = P("data", None)
    full_spec = P(None, None)
    scalar_spec = P()

    def shard_body(act_in, grad_out, w_up1, w_down1, w_up2, w_down2, *rest):
        gel_up1, der_up1 = gelu_pair(jnp.dot(act_in, w_up1, preferred_element_type=jnp.float32))
        act_up1 = gel_up1.astype(jnp.bfloat16)
        mid_act = jnp.dot(act_up1, w_down1, preferred_element_type=jnp.float32).astype(jnp.bfloat16)
        gel_up2, der_up2 = gelu_pair(jnp.dot(mid_act, w_up2, preferred_element_type=jnp.float32))
        grad_down2 = mat_tn(gel_up2.astype(jnp.bfloat16), grad_out)
        return comm_call(768, grad_down2, (grad_out, mid_act, act_in), (w_down1, w_up2, w_down2), (der_up1, der_up2, act_up1), rest[0:4], rest[4:8], rest[8:12], rest[12], rest[13])

    in_specs = (rows_spec, rows_spec) + (full_spec,) * 4 + (rows_spec,) * 12 + (scalar_spec, scalar_spec)
    out_specs = (full_spec,) * 4 + (rows_spec,) * 12 + (scalar_spec,)
    return jax.shard_map(shard_body, mesh=mesh, in_specs=in_specs, out_specs=out_specs, check_vma=False)
```

```python
import functools
import math
import jax
import jax.numpy as jnp
from jax import lax
from jax.experimental import pallas as pl
from jax.experimental.pallas import tpu as pltpu
from jax.sharding import PartitionSpec as P

STEP = 20
BETA_ONE = 0.9
BETA_TWO = 0.95
EPSILON = 1e-8
NORM_EPS = 1e-6
CORR_ONE = 1.0 - BETA_ONE ** STEP
CORR_TWO = 1.0 - BETA_TWO ** STEP
ROOT_HALF = math.sqrt(0.5)
INV_ROOT_TAU = 1.0 / math.sqrt(2.0 * math.pi)

MESH = pl.DeviceIdType.MESH
UP1, DOWN1, UP2, DOWN2 = 0, 1, 2, 3
UP, DOWN = 0, 1
LAST, MIDDLE, EARLY = 0, 1, 2
FAR, NEAR, PASS = 0, 1, 2
STRIDES = (32, 8, 2)
ORDERS = ((2, 1, 0), (1, 0, 2), (0, 2, 1))
ROWS = 24
SUB = 6
CHUNK = 8
SIDE = 4
COLOURS = 3
SIDES = 2
ALL = slice(None)
WINDOW = 16
TILE = 512


def adam_step(scaled, master_old, mom_old, vel_old, learn_rate):
    mom_new = BETA_ONE * mom_old + (1.0 - BETA_ONE) * scaled
    vel_new = BETA_TWO * vel_old + (1.0 - BETA_TWO) * scaled * scaled
    master_new = master_old - learn_rate * (mom_new / CORR_ONE) / (jnp.sqrt(vel_new / CORR_TWO) + EPSILON)
    return master_new, mom_new, vel_new


def comm_kernel(lanes, *refs):
    (g_down2, grad_rows, mid_rows, in_rows, w_down1, w_up2, w_down2, der1, der2, act1), refs = refs[:10], refs[10:]
    states, refs = refs[:12], refs[12:]
    (lr_ref, clip_ref), refs = refs[:2], refs[2:]
    (w_out, up_out, down_out, norm_out, g_up1, g_down1, g_up2), refs = refs[:7], refs[7:]
    (total, peer_in, rs1, rs2, rs3, norm_line, norm_plane, send_g, recv_g, send_w, recv_w, block_tmp, w_own, up_state, down_state), refs = refs[:15], refs[15:]
    (left, flipped, mid_acc, mid_grad, w_tile, act_tile, der_tile, out_tile), refs = refs[:8], refs[8:]
    (load_sem, state_sem, pair_s, pair_r, rs1_s, rs1_r, rs2_s, rs2_r, rs3_s, rs3_r, nc_s, nc_r, na_s, na_r, xg_s, xg_r, xw_s, xw_r, own_sem, ag_s, ag_r, out_s, out_r) = refs[:23]
    row_sem, tile_sem, store_sem, pair_credit, ring_credit, early_l, early_s, early_r = refs[23:]
    half = lanes // 2
    me = lax.axis_index("data")
    core = lax.rem(me, SIDES)
    member = lax.rem(me, 4)
    pos = (me // 32, lax.rem(me // 8, 4), lax.rem(me // 2, 4))
    partner = me + 1 - 2 * core

    def device(axis, coord):
        return me + (coord - pos[axis]) * STRIDES[axis]

    def step(axis, hops):
        return lax.rem(pos[axis] + hops, 4)

    def remote(src, dst, send_sem, recv_sem, target):
        return pltpu.make_async_remote_copy(src_ref=src, dst_ref=dst, send_sem=send_sem, recv_sem=recv_sem, device_id=(target,), device_id_type=MESH)

    line, plane = lax.rem(me, 8), me // 8
    line_peers = [me - line + lax.rem(line + hops, 8) for hops in range(1, 8)]
    plane_peers = [8 * lax.rem(plane + hops, 16) + line for hops in range(1, 16)]
    peers = line_peers + plane_peers
    barrier = pltpu.get_barrier_semaphore()
    for peer in peers:
        pl.semaphore_signal(barrier, device_id=(peer,), device_id_type=MESH)

    grads = (g_up1, g_down1, g_up2, g_down2)
    mat_order = (3, 2, 1, 0)
    pair_slot = (1, 0, 1, 0)
    loads, pairs = {0: [], 2: []}, {0: [], 2: []}

    def issue_up(mat, x_low):
        for x in (x_low, x_low + 2):
            for owner in (1 - core, core):
                col = pl.multiple_of((x_low * 2 + owner) * lanes, lanes)
                src = grads[mat].at[:, :, x // SIDES, :, pl.ds(col, lanes)]
                if owner is core:
                    loads[mat].append(pltpu.make_async_copy(src, total.at[mat, :, :, x], load_sem.at[mat, x]))
                    loads[mat][-1].start()
                else:
                    pairs[mat].append(remote(src, peer_in.at[pair_slot[mat], :, :, x], pair_s.at[mat, x], pair_r.at[mat, x], partner))
                    pairs[mat][-1].start()

    def issue_rows(low, high):
        def move(i, carry):
            place = (i // 16, lax.rem(i // SIDE, 4), lax.rem(i, SIDE))
            there = g_down1.at[pl.ds(pl.multiple_of(i * 2 * ROWS + (1 - core) * ROWS, 8), ROWS)]
            here = g_down1.at[pl.ds(pl.multiple_of(i * 2 * ROWS + core * ROWS, 8), ROWS)]
            remote(there, peer_in.at[(pair_slot[DOWN1],) + place], pair_s.at[DOWN1, 0], pair_r.at[DOWN1, 0], partner).start()
            pltpu.make_async_copy(here, total.at[(1,) + place], load_sem.at[DOWN1, 0]).start()
            return carry

        lax.fori_loop(low, high, move, 0)

    loads[DOWN1] = [pltpu.make_async_copy(total.at[1], total.at[1], load_sem.at[DOWN1, 0])]
    pairs[DOWN1] = [remote(peer_in.at[pair_slot[DOWN1]], peer_in.at[pair_slot[DOWN1]], pair_s.at[DOWN1, 0], pair_r.at[DOWN1, 0], partner)]
    early = {}
    for hops in (2, 1, 3, 0):
        for colour in range(COLOURS):
            axis = ORDERS[colour][0]
            where = [ALL] * 3
            where[axis] = step(axis, hops)
            rows = pl.ds(CHUNK * colour, CHUNK)
            spots = (colour, hops)
            early[spots] = (
                pltpu.make_async_copy(g_down2.at[(*where, core, rows)], total.at[(DOWN2, *where, rows)], early_l.at[spots]),
                remote(g_down2.at[(*where, 1 - core, rows)], peer_in.at[(pair_slot[DOWN2], *where, rows)], early_s.at[spots], early_r.at[spots], partner),
            )

    tiles = SIDE * lanes // TILE

    def span(t):
        return pl.ds(pl.multiple_of(t * TILE, TILE), TILE)

    def fetch_a(t, slot):
        return [
            pltpu.make_async_copy(w_down2.at[span(t)], w_tile.at[slot], tile_sem.at[slot, 0]),
            pltpu.make_async_copy(w_up2.at[:, span(t)], act_tile.at[slot, pl.ds(0, lanes)], tile_sem.at[slot, 1]),
            pltpu.make_async_copy(der2.at[:, span(t)], der_tile.at[slot], tile_sem.at[slot, 2]),
        ]

    def fetch_b(t, slot):
        return [pltpu.make_async_copy(act1.at[:, span(t)], act_tile.at[slot], tile_sem.at[slot, 1])]

    def fetch_c(t, slot):
        return [
            pltpu.make_async_copy(w_down1.at[span(t)], w_tile.at[slot], tile_sem.at[slot, 0]),
            pltpu.make_async_copy(der1.at[:, span(t)], der_tile.at[slot], tile_sem.at[slot, 2]),
        ]

    def begin(copies):
        for copy in copies:
            copy.start()

    def end(copies):
        for copy in copies:
            copy.wait()

    row_loads = [pltpu.make_async_copy(grad_rows, left, row_sem.at[0]), pltpu.make_async_copy(mid_rows, mid_grad, row_sem.at[1])]
    begin(row_loads)
    begin(fetch_a(0, 0))
    begin([copies[0] for copies in early.values()])
    state_loads = []
    for field in range(COLOURS):
        for mat in range(SIDE):
            dst = (down_state if mat % SIDES else up_state).at[field, mat // SIDES]
            state_loads.append(pltpu.make_async_copy(states[4 * field + mat], dst, state_sem.at[field, mat]))
    begin(state_loads)
    def store_a(t, slot):
        return [pltpu.make_async_copy(out_tile.at[slot], g_up2.at[:, :, :, :, span(t)], store_sem.at[slot])]

    def store_b(t, slot):
        return [pltpu.make_async_copy(mid_acc.at[slot], g_down1.at[span(t)], store_sem.at[slot])]

    def store_c(t, slot):
        return [pltpu.make_async_copy(out_tile.at[slot], g_up1.at[:, :, :, :, span(t)], store_sem.at[slot])]

    def run(first, last, fetch, store, work):
        def tile(t, carry):
            slot = lax.rem(t, SIDES)

            @pl.when(t + 1 < tiles)
            def _():
                begin(fetch(t + 1, 1 - slot))

            end(fetch(t, slot))

            @pl.when(t - first >= 2)
            def _():
                end(store(t - 2, slot))

            work(slot)
            begin(store(t, slot))
            return carry

        lax.fori_loop(first, last, tile, 0)
        for t in range(max(first, last - 2), last):
            end(store(t, t % 2))

    def dot(lhs, rhs, lhs_dim, rhs_dim):
        return lax.dot_general(lhs, rhs, (((lhs_dim,), (rhs_dim,)), ((), ())), preferred_element_type=jnp.float32)

    def work_a(slot):
        grad_act2 = dot(left[...], w_tile[slot], 1, 1).astype(jnp.bfloat16)
        grad_pre2 = (grad_act2.astype(jnp.float32) * der_tile[slot]).astype(jnp.bfloat16)
        out_tile[slot] = dot(flipped[...], grad_pre2, 1, 0).reshape(out_tile.shape[1:])
        mid_acc[...] += dot(grad_pre2, act_tile[slot, pl.ds(0, lanes)], 1, 1).reshape(mid_acc.shape)

    def work_b(slot):
        mid_acc[slot] = dot(act_tile[slot], mid_grad[...], 0, 0)

    def work_c(slot):
        grad_act1 = dot(mid_grad[...], w_tile[slot], 1, 1).astype(jnp.bfloat16)
        grad_pre1 = (grad_act1.astype(jnp.float32) * der_tile[slot]).astype(jnp.bfloat16)
        out_tile[slot] = dot(flipped[...], grad_pre1, 1, 0).reshape(out_tile.shape[1:])

    def part(mats, coords, colour, side):
        lane = ALL if side is None else pl.ds(half * side, half)
        index = [mats, ALL, ALL, ALL, pl.ds(CHUNK * colour, CHUNK), lane]
        for axis, coord in coords.items():
            index[1 + axis] = coord
        return tuple(index)

    class Phase:
        def __init__(self, level, base, buf, send_sem, recv_sem):
            self.level, self.base, self.buf, self.send_sem, self.recv_sem = level, base, buf, send_sem, recv_sem
            self.mats, self.count = (slice(base, base + 2), 2) if level else (base, 4)
            self.copies = {}

        def where(self, colour, coord):
            order = ORDERS[colour]
            coords = {axis: pos[axis] for axis in order[:self.level]}
            coords[order[self.level]] = coord
            return coords

        def row(self, colour, coord, side, i):
            coords = self.where(colour, coord)
            if self.level:
                return part(self.base + i, coords, colour, side)
            coords[min(axis for axis in range(COLOURS) if axis not in coords)] = i
            return part(self.mats, coords, colour, side)

        def send(self, colour, side, kind, src, target):
            copy = remote(src, self.buf.at[colour, side, kind], self.send_sem.at[colour, side, kind], self.recv_sem.at[colour, side, kind], target)
            copy.start()
            self.copies[colour, side, kind] = copy

        def near(self, colour, side):
            axis = ORDERS[colour][self.level]
            coord = step(axis, 1 if side == 0 else 3)
            return coord, device(axis, coord)

        def start(self, kinds=(0, 1)):
            for kind in kinds:
                for colour in range(COLOURS):
                    for side in range(SIDES):
                        coord, target = self.near(colour, side)
                        aim = step(ORDERS[colour][self.level], 2) if kind == 0 else coord
                        src = total.at[part(self.mats, self.where(colour, aim), colour, side if kind == 0 else 1 - side)]
                        self.send(colour, side, kind, src, target)

        def forward(self):
            for colour in range(COLOURS):
                for side in range(SIDES):
                    coord, target = self.near(colour, side)
                    self.copies[colour, side, FAR].wait_recv()

                    def add_own(i, carry, colour=colour, side=side, coord=coord):
                        self.buf[colour, side, FAR, i] = self.buf[colour, side, FAR, i] + total[self.row(colour, coord, side, i)]
                        return carry

                    lax.fori_loop(0, self.count, add_own, 0)
                    self.send(colour, side, 2, self.buf.at[colour, side, FAR], target)

        def finish(self):
            for colour in range(COLOURS):
                for side in range(SIDES):
                    self.copies[colour, 1 - side, NEAR].wait_recv()
                    self.copies[colour, side, PASS].wait_recv()

                    def add_both(i, carry, colour=colour, side=side):
                        own = self.row(colour, pos[ORDERS[colour][self.level]], side, i)
                        total[own] = total[own] + (self.buf[colour, 1 - side, NEAR, i] + self.buf[colour, side, PASS, i])
                        return carry

                    lax.fori_loop(0, self.count, add_both, 0)

        def drain(self):
            for copy in self.copies.values():
                copy.wait_send()

    ring_slot = (1, 0, 1, 0)
    class Direct:
        def __init__(self, base, buf, send_sem, recv_sem):
            self.base, self.buf, self.send_sem, self.recv_sem = base, buf, send_sem, recv_sem
            self.copies = {}

        def index(self, colour, coord, mats):
            coords = {axis: pos[axis] for axis in range(COLOURS)}
            coords[ORDERS[colour][2]] = coord
            return part(mats, coords, colour, None)

        def start(self):
            for hops in (2, 1, 3):
                for colour in range(COLOURS):
                    axis = ORDERS[colour][2]
                    coord = step(axis, hops)
                    spots = (colour, hops - 1)
                    src = total.at[self.index(colour, coord, slice(self.base, self.base + 2))]
                    copy = remote(src, self.buf.at[spots], self.send_sem.at[spots], self.recv_sem.at[spots], device(axis, coord))
                    copy.start()
                    self.copies[spots] = copy

        def finish(self):
            for colour in range(COLOURS):
                for hops in range(COLOURS):
                    self.copies[colour, hops].wait_recv()
                for mat in range(SIDES):
                    own = self.index(colour, pos[ORDERS[colour][2]], self.base + mat)
                    total[own] = (total[own] + self.buf[colour, 0, mat]) + (self.buf[colour, 1, mat] + self.buf[colour, 2, mat])

        def drain(self):
            for copy in self.copies.values():
                copy.wait_send()

    first = {mat: Phase(0, mat, rs1.at[ring_slot[mat]], rs1_s.at[mat], rs1_r.at[mat]) for mat in mat_order}

    def add_pair(mat):
        end(loads[mat])
        for copy in pairs[mat]:
            copy.wait_recv()

        def add(i, carry):
            total[mat, i // SIDE, lax.rem(i, SIDE)] = total[mat, i // SIDE, lax.rem(i, SIDE)] + peer_in[pair_slot[mat], i // SIDE, lax.rem(i, SIDE)]
            return carry

        lax.fori_loop(0, 16, add, 0)
        if mat == UP2:
            pl.semaphore_signal(pair_credit, device_id=(partner,), device_id_type=MESH)

    def add_early(hops):
        for colour in range(COLOURS):
            early[colour, hops][0].wait()
            early[colour, hops][1].wait_recv()
            axis = ORDERS[colour][0]

            def add(i, carry, colour=colour, axis=axis):
                coords = {axis: step(axis, hops), (1 if axis == 0 else 0): i}
                own = part(DOWN2, coords, colour, None)
                total[own] = total[own] + peer_in[part(pair_slot[DOWN2], coords, colour, None)]
                return carry

            lax.fori_loop(0, 4, add, 0)

    ring = [device(axis, step(axis, hops)) for axis in range(COLOURS) for hops in (1, 3)]

    def close(mat):
        first[mat].finish()
        first[mat].drain()
        for peer in ring:
            pl.semaphore_signal(ring_credit.at[ring_slot[mat]], device_id=(peer,), device_id_type=MESH)

    second = {base: Phase(1, base, rs2.at[base // 2], rs2_s.at[base // 2], rs2_r.at[base // 2]) for base in (2, 0)}
    third = {base: Direct(base, rs3.at[base // 2], rs3_s.at[base // 2], rs3_r.at[base // 2]) for base in (2, 0)}
    end(row_loads)
    flipped[...] = mid_grad[...].T
    mid_acc[...] = jnp.zeros_like(mid_acc)
    run(0, 1, fetch_a, store_a, work_a)
    pl.semaphore_wait(barrier, len(peers))
    pairs[DOWN2] = [copies[1] for copies in early.values()]
    begin(pairs[DOWN2])
    run(1, 2, fetch_a, store_a, work_a)
    add_early(2)
    first[DOWN2].start((FAR,))
    run(2, 4, fetch_a, store_a, work_a)
    issue_up(UP2, 0)
    add_early(1)
    add_early(3)
    first[DOWN2].start((NEAR,))
    add_early(0)
    pl.semaphore_signal(pair_credit, device_id=(partner,), device_id_type=MESH)
    first[DOWN2].forward()
    run(4, tiles, fetch_a, store_a, work_a)
    issue_up(UP2, 1)
    begin(fetch_b(0, 0) + fetch_c(0, 0))
    in_load = pltpu.make_async_copy(in_rows, left, row_sem.at[0])
    in_load.start()
    mid_grad[...] = mid_acc[...].reshape(mid_grad.shape).astype(jnp.bfloat16)
    run(0, 3, fetch_b, store_b, work_b)
    add_pair(UP2)
    first[UP2].start()
    run(3, tiles, fetch_b, store_b, work_b)
    pl.semaphore_wait(pair_credit)
    issue_rows(0, 64)
    in_load.wait()
    flipped[...] = left[...].T
    run(0, 3, fetch_c, store_c, work_c)
    close(DOWN2)
    first[UP2].forward()
    pl.semaphore_wait(pair_credit)
    issue_up(UP1, 0)
    add_pair(DOWN1)
    pl.semaphore_wait(ring_credit.at[0], len(ring))
    first[DOWN1].start()
    run(3, tiles, fetch_c, store_c, work_c)
    issue_up(UP1, 1)
    close(UP2)
    second[UP2].start()
    add_pair(UP1)
    pl.semaphore_wait(ring_credit.at[1], len(ring))
    first[UP1].start()
    first[DOWN1].forward()
    second[UP2].forward()
    first[UP1].forward()
    second[UP2].finish()
    third[UP2].start()
    first[DOWN1].finish()
    first[UP1].finish()
    second[UP1].start()
    third[UP2].finish()
    second[UP1].forward()
    second[UP1].finish()
    third[UP1].start()
    third[UP1].finish()

    group_scale = 1.0 / 128.0
    grad_own = [total[mat, *pos] * group_scale for mat in range(SIDE)]
    partial = None
    for block in grad_own:
        square = block * block
        for row in range(ROWS // 8):
            for col in range(max(1, lanes // 128)):
                tile = square[8 * row:8 * row + 8, 128 * col:128 * col + 128]
                partial = tile if partial is None else partial + tile
    norm_line[line] = partial
    sends = []

    def spread(buf, slot, targets, send_sem, recv_sem):
        copies = []
        for i, target in enumerate(targets):
            copies.append(remote(buf.at[slot], buf.at[slot], send_sem.at[i], recv_sem.at[i], target))
            copies[i].start()
        return copies

    swap = spread(norm_line, line, line_peers, nc_s, nc_r)
    for target in range(SIDE):
        for i, mat in enumerate((0, 2)):
            send_g[target, i] = grad_own[mat][SUB * target:SUB * target + SUB]
    moves = []
    for hops in range(1, SIDE):
        other = lax.rem(member + hops, SIDE)
        copy = remote(send_g.at[other], recv_g.at[member], xg_s.at[hops - 1], xg_r.at[hops - 1], me - member + other)
        copy.start()
        moves.append(copy)
    recv_g[member] = send_g[member]
    for copy in swap:
        copy.wait_recv()
    norm_plane[plane] = jnp.sum(norm_line[...], axis=0)
    cross = spread(norm_plane, plane, plane_peers, na_s, na_r)
    for copy in cross:
        copy.wait_recv()
    running = jnp.sum(norm_plane[...], axis=0)
    sends = swap + cross + moves
    norm = jnp.sqrt(jnp.sum(jnp.sum(running, axis=1, keepdims=True), axis=0, keepdims=True))
    norm_out[...] = jnp.broadcast_to(norm, norm_out.shape)
    clip_scale = jnp.minimum(1.0, clip_ref[0] / (norm + NORM_EPS))
    learn_rate = lr_ref[0]

    end(state_loads)
    for i in range(SIDES):
        fresh = adam_step(grad_own[2 * i + 1] * clip_scale, down_state[0, i], down_state[1, i], down_state[2, i], learn_rate)
        for field in range(COLOURS):
            down_state[field, i] = fresh[field]
        w_own[2 + i] = fresh[0].astype(jnp.bfloat16)

    def spot(group, coords, colour, side):
        lane = ALL if side is None else pl.ds(half * side, half)
        index = [pl.ds(2 * group, 2), ALL, ALL, ALL, core, pl.ds(CHUNK * colour, CHUNK), lane]
        for axis, coord in coords.items():
            index[1 + axis] = coord
        return w_out.at[tuple(index)]

    handed = []

    class Gather:
        def __init__(self, group, level):
            self.group, self.level = group, level
            self.copies = {}

        def spot(self, colour, coord, side):
            order = ORDERS[colour]
            coords = {axis: pos[axis] for axis in order[:self.level]}
            coords[order[self.level]] = coord
            return spot(self.group, coords, colour, side)

        def near(self, colour, side):
            axis = ORDERS[colour][self.level]
            coord = step(axis, 1 if side == 0 else 3)
            return coord, device(axis, coord)

        def send(self, colour, side, kind, src, dst):
            spots = (self.group, self.level, colour, side, kind)
            copy = remote(src, dst, ag_s.at[spots], ag_r.at[spots], self.near(colour, side)[1])
            copy.start()
            self.copies[colour, side, kind] = copy

        def hand(self, ref, slot):
            copy = remote(ref, ref, out_s.at[self.group, slot], out_r.at[self.group, slot], partner)
            copy.start()
            handed.append(copy)

        def start_direct(self):
            for hops in (2, 1, 3):
                for colour in range(COLOURS):
                    axis = ORDERS[colour][self.level]
                    dst = self.spot(colour, pos[axis], None)
                    src = w_own.at[pl.ds(2 * self.group, 2), pl.ds(CHUNK * colour, CHUNK)] if self.level == 2 else dst
                    spots = (self.group, self.level, colour, 0, hops - 1)
                    copy = remote(src, dst, ag_s.at[spots], ag_r.at[spots], device(axis, step(axis, hops)))
                    copy.start()
                    self.copies[colour, hops] = copy

        def finish_direct(self):
            for copy in self.copies.values():
                copy.wait_recv()

        def start(self):
            for kind in range(SIDES):
                for colour in range(COLOURS):
                    for side in range(SIDES):
                        ref = self.spot(colour, pos[ORDERS[colour][0]], side if kind == 0 else 1 - side)
                        self.send(colour, side, kind, ref, ref)
            for colour in range(COLOURS):
                self.hand(self.spot(colour, pos[ORDERS[colour][0]], None), 5 * colour)

        def forward(self):
            for colour in range(COLOURS):
                for side in range(SIDES):
                    self.copies[colour, side, FAR].wait_recv()
                    ref = self.spot(colour, self.near(colour, 1 - side)[0], side)
                    self.send(colour, side, 2, ref, ref)

        def finish(self):
            for colour in range(COLOURS):
                for side in range(SIDES):
                    self.copies[colour, side, NEAR].wait_recv()
                    self.hand(self.spot(colour, self.near(colour, 1 - side)[0], None), 5 * colour + 1 + side)
            for colour in range(COLOURS):
                for side in range(SIDES):
                    self.copies[colour, side, PASS].wait_recv()
                    self.hand(self.spot(colour, step(ORDERS[colour][0], 2), side), 5 * colour + 3 + side)

    keeps = [pltpu.make_async_copy(w_own.at[pl.ds(2 * group, 2)], w_out.at[pl.ds(2 * group, 2), *pos, core], own_sem.at[group]) for group in range(SIDES)]
    gathers = {(group, level): Gather(group, level) for group in range(SIDES) for level in range(COLOURS)}
    gathers[DOWN, EARLY].start_direct()
    keeps[DOWN].start()

    for copy in moves:
        copy.wait_recv()
    for i in range(SIDES):
        for col in range(SIDE):
            cols = slice(col * lanes, (col + 1) * lanes)
            scaled = recv_g[col, i] * clip_scale
            fresh = adam_step(scaled, up_state[0, i, :, cols], up_state[1, i, :, cols], up_state[2, i, :, cols], learn_rate)
            for field in range(COLOURS):
                up_state[field, i, :, cols] = fresh[field]
            send_w[col, i] = fresh[0]
    moves = []
    for hops in range(1, SIDE):
        other = lax.rem(member + hops, SIDE)
        copy = remote(send_w.at[other], recv_w.at[member], xw_s.at[hops - 1], xw_r.at[hops - 1], me - member + other)
        copy.start()
        moves.append(copy)
    recv_w[member] = send_w[member]
    state_stores = [pltpu.make_async_copy(up_state, up_out, state_sem.at[0, 0]), pltpu.make_async_copy(down_state, down_out, state_sem.at[0, 1])]
    begin(state_stores)
    gathers[DOWN, EARLY].finish_direct()
    keeps[DOWN].wait()
    gathers[DOWN, MIDDLE].start_direct()
    for copy in moves:
        copy.wait_recv()
    sends = sends + moves
    for i in range(SIDES):
        for source in range(SIDE):
            block_tmp[SUB * source:SUB * source + SUB] = recv_w[source, i]
        w_own[i] = block_tmp[...].astype(jnp.bfloat16)
    gathers[UP, EARLY].start_direct()
    keeps[UP].start()
    gathers[DOWN, MIDDLE].finish_direct()
    gathers[DOWN, LAST].start()
    gathers[UP, EARLY].finish_direct()
    keeps[UP].wait()
    gathers[UP, MIDDLE].start_direct()
    gathers[DOWN, LAST].forward()
    gathers[UP, MIDDLE].finish_direct()
    gathers[UP, LAST].start()
    gathers[DOWN, LAST].finish()
    gathers[UP, LAST].forward()
    gathers[UP, LAST].finish()
    for gather in gathers.values():
        sends = sends + list(gather.copies.values())
    for phase in [first[DOWN1], first[UP1]] + list(second.values()) + list(third.values()):
        phase.drain()
    for mat in mat_order:
        for copy in pairs[mat]:
            copy.wait_send()
    for copy in sends:
        copy.wait_send()
    for copy in handed + state_stores:
        copy.wait()


def place_kernel(lanes, w_ref, up_ref, down_ref, norm_ref, *refs):
    weights, states, norm_out, (w_tmp, up_tmp, down_tmp, in_sem, state_in, out_sem, state_out) = refs[:4], refs[4:16], refs[16], refs[17:]
    norm_out[0] = jnp.max(norm_ref[...])
    loads = [[pltpu.make_async_copy(w_ref.at[mat % SIDES * 2 + mat // SIDES, z], w_tmp.at[mat, z], in_sem.at[mat, z]) for z in range(SIDE)] for mat in range(SIDE)]
    queue = [copy for row in loads for copy in row]
    for copy in queue[:WINDOW]:
        copy.start()
    state_loads = [pltpu.make_async_copy(up_ref, up_tmp, state_in.at[0]), pltpu.make_async_copy(down_ref, down_tmp, state_in.at[1])]
    for copy in state_loads:
        copy.start()
    stores = []
    for mat in range(SIDE):
        for z in range(SIDE):
            loads[mat][z].wait()
            ahead = 4 * mat + z + WINDOW
            if ahead < len(queue):
                queue[ahead].start()
            if mat % SIDES:
                copies = [pltpu.make_async_copy(w_tmp.at[mat, z], weights[mat].at[z], out_sem.at[mat, z, 0])]
            else:
                copies = []
                for member in range(SIDE):
                    src = w_tmp.at[mat, z, :, :, member // SIDES, member % SIDES]
                    copies.append(pltpu.make_async_copy(src, weights[mat].at[z, :, :, :, pl.ds(member * lanes, lanes)], out_sem.at[mat, z, member]))
            for copy in copies:
                copy.start()
            stores = stores + copies
    for copy in state_loads:
        copy.wait()
    for field in range(COLOURS):
        for mat in range(SIDE):
            src = (down_tmp if mat % SIDES else up_tmp).at[field, mat // SIDES]
            copy = pltpu.make_async_copy(src, states[4 * field + mat], state_out.at[field, mat])
            copy.start()
            stores.append(copy)
    for copy in stores:
        copy.wait()


def comm_call(lanes, grad_down2, rows, weights_in, hidden, masters, moms, vels, learn_rate, clip_norm):
    up = (SIDE, SIDE, SIDES, ROWS, SIDE * lanes)
    down = (SIDE, SIDE, SIDE, SIDES, ROWS, lanes)
    local_rows = rows[0].shape[0]
    half = lanes // 2
    f32 = jnp.float32
    bf16 = jnp.bfloat16
    up_shape = (COLOURS, SIDES, SUB, SIDE * lanes)
    down_shape = (COLOURS, SIDES, ROWS, lanes)
    dma = pltpu.SemaphoreType.DMA
    vmem = pl.BlockSpec(memory_space=pltpu.VMEM)
    smem = pl.BlockSpec(memory_space=pltpu.SMEM)
    hbm = pl.BlockSpec(memory_space=pl.ANY)
    scratch = [
        pltpu.VMEM((SIDE, SIDE, SIDE, SIDE, ROWS, lanes), f32),
        pltpu.VMEM((SIDES, SIDE, SIDE, SIDE, ROWS, lanes), f32),
        pltpu.VMEM((SIDES, COLOURS, SIDES, COLOURS, SIDE, SIDE, CHUNK, half), f32),
        pltpu.VMEM((SIDES, COLOURS, SIDES, COLOURS, SIDES, SIDE, CHUNK, half), f32),
        pltpu.VMEM((SIDES, COLOURS, COLOURS, SIDES, CHUNK, lanes), f32),
        pltpu.VMEM((8, 8, 128), f32),
        pltpu.VMEM((16, 8, 128), f32),
        pltpu.VMEM((SIDE, SIDES, SUB, lanes), f32),
        pltpu.VMEM((SIDE, SIDES, SUB, lanes), f32),
        pltpu.VMEM((SIDE, SIDES, SUB, lanes), f32),
        pltpu.VMEM((SIDE, SIDES, SUB, lanes), f32),
        pltpu.VMEM((ROWS, lanes), f32),
        pltpu.VMEM((SIDE, ROWS, lanes), jnp.bfloat16),
        pltpu.VMEM(up_shape, f32),
        pltpu.VMEM(down_shape, f32),
        pltpu.VMEM((local_rows, lanes), bf16),
        pltpu.VMEM((lanes, local_rows), bf16),
        pltpu.VMEM((SIDES, local_rows // SIDES, lanes), f32),
        pltpu.VMEM((local_rows, lanes), bf16),
        pltpu.VMEM((SIDES, TILE, lanes), bf16),
        pltpu.VMEM((SIDES, local_rows, TILE), bf16),
        pltpu.VMEM((SIDES, local_rows, TILE), f32),
        pltpu.VMEM((SIDES, SIDE, SIDE, SIDES, ROWS, TILE), f32),
        dma((SIDE, SIDE)), dma((COLOURS, SIDE)), dma((SIDE, SIDE)), dma((SIDE, SIDE)),
        dma((SIDE, COLOURS, SIDES, COLOURS)), dma((SIDE, COLOURS, SIDES, COLOURS)), dma((SIDES, COLOURS, SIDES, COLOURS)), dma((SIDES, COLOURS, SIDES, COLOURS)), dma((SIDES, COLOURS, COLOURS)), dma((SIDES, COLOURS, COLOURS)),
        dma((7,)), dma((7,)), dma((15,)), dma((15,)), dma((COLOURS,)), dma((COLOURS,)), dma((COLOURS,)), dma((COLOURS,)),
        dma((SIDES,)), dma((SIDES, COLOURS, COLOURS, SIDES, COLOURS)), dma((SIDES, COLOURS, COLOURS, SIDES, COLOURS)), dma((SIDES, 15)), dma((SIDES, 15)),
        dma((SIDES,)), dma((SIDES, COLOURS)), dma((SIDES,)), pltpu.SemaphoreType.REGULAR, pltpu.SemaphoreType.REGULAR((2,)), dma((COLOURS, SIDE)), dma((COLOURS, SIDE)), dma((COLOURS, SIDE)),
    ]
    outs = pl.pallas_call(
        functools.partial(comm_kernel, lanes),
        name="reduce_update_gather",
        out_shape=[jax.ShapeDtypeStruct((SIDE, SIDE, SIDE, SIDE, SIDES, ROWS, lanes), bf16), jax.ShapeDtypeStruct(up_shape, f32), jax.ShapeDtypeStruct(down_shape, f32), jax.ShapeDtypeStruct((8, 128), f32), jax.ShapeDtypeStruct(up, f32), jax.ShapeDtypeStruct((3072, lanes), f32), jax.ShapeDtypeStruct(up, f32)],
        in_specs=[hbm] * 22 + [smem] * 2,
        out_specs=[hbm] * 3 + [vmem] + [hbm] * 3,
        scratch_shapes=scratch,
        compiler_params=pltpu.CompilerParams(collective_id=0, has_side_effects=True, vmem_limit_bytes=67043328),
    )(grad_down2.reshape(down), *rows, *weights_in, *hidden, *masters, *moms, *vels, learn_rate.reshape(1), clip_norm.reshape(1))
    split = (SIDE, SIDE, SIDES, SIDES, SIDES, ROWS, lanes)
    placed = pl.pallas_call(
        functools.partial(place_kernel, lanes),
        name="place_outputs",
        out_shape=[jax.ShapeDtypeStruct(split if mat % SIDES else up, bf16) for mat in range(SIDE)] + [jax.ShapeDtypeStruct(m.shape, f32) for m in masters] * 3 + [jax.ShapeDtypeStruct((1,), f32)],
        in_specs=[hbm] * 3 + [vmem],
        out_specs=[hbm] * 16 + [smem],
        scratch_shapes=[
            pltpu.VMEM((SIDE,) + split, bf16), pltpu.VMEM(up_shape, f32), pltpu.VMEM(down_shape, f32),
            dma((SIDE, SIDE)), dma((SIDES,)), dma((SIDE, SIDE, SIDE)), dma((COLOURS, SIDE)),
        ],
        compiler_params=pltpu.CompilerParams(vmem_limit_bytes=67043328),
    )(outs[0].reshape((4,) + split), *outs[1:4])
    weights = [placed[mat].reshape(masters[mat].shape[0] * 128, -1) for mat in range(SIDE)]
    return tuple(weights) + tuple(placed[4:16]) + (placed[16][0],)


def mat_tn(left, right):
    return lax.dot_general(left, right, (((0,), (0,)), ((), ())), preferred_element_type=jnp.float32)


def gelu_pair(pre):
    normal_cdf = 0.5 * (1.0 + lax.erf(pre * ROOT_HALF))
    density = jnp.exp(-0.5 * pre * pre) * INV_ROOT_TAU
    return pre * normal_cdf, normal_cdf + pre * density


def solution(mesh):
    rows_spec = P("data", None)
    full_spec = P(None, None)
    scalar_spec = P()

    def shard_body(act_in, grad_out, w_up1, w_down1, w_up2, w_down2, *rest):
        gel_up1, der_up1 = gelu_pair(jnp.dot(act_in, w_up1, preferred_element_type=jnp.float32))
        act_up1 = gel_up1.astype(jnp.bfloat16)
        mid_act = jnp.dot(act_up1, w_down1, preferred_element_type=jnp.float32).astype(jnp.bfloat16)
        gel_up2, der_up2 = gelu_pair(jnp.dot(mid_act, w_up2, preferred_element_type=jnp.float32))
        grad_down2 = mat_tn(gel_up2.astype(jnp.bfloat16), grad_out)
        return comm_call(768, grad_down2, (grad_out, mid_act, act_in), (w_down1, w_up2, w_down2), (der_up1, der_up2, act_up1), rest[0:4], rest[4:8], rest[8:12], rest[12], rest[13])

    in_specs = (rows_spec, rows_spec) + (full_spec,) * 4 + (rows_spec,) * 12 + (scalar_spec, scalar_spec)
    out_specs = (full_spec,) * 4 + (rows_spec,) * 12 + (scalar_spec,)
    return jax.shard_map(shard_body, mesh=mesh, in_specs=in_specs, out_specs=out_specs, check_vma=False)
```

```python
import functools
import math
import jax
import jax.numpy as jnp
from jax import lax
from jax.experimental import pallas as pl
from jax.experimental.pallas import tpu as pltpu
from jax.sharding import PartitionSpec as P

STEP = 20
BETA_ONE = 0.9
BETA_TWO = 0.95
EPSILON = 1e-8
NORM_EPS = 1e-6
CORR_ONE = 1.0 - BETA_ONE ** STEP
CORR_TWO = 1.0 - BETA_TWO ** STEP
ROOT_HALF = math.sqrt(0.5)
INV_ROOT_TAU = 1.0 / math.sqrt(2.0 * math.pi)

MESH = pl.DeviceIdType.MESH
UP1, DOWN1, UP2, DOWN2 = 0, 1, 2, 3
UP, DOWN = 0, 1
LAST, MIDDLE, EARLY = 0, 1, 2
FAR, NEAR, PASS = 0, 1, 2
STRIDES = (32, 8, 2)
ORDERS = ((2, 1, 0), (1, 0, 2), (0, 2, 1))
ROWS = 24
SUB = 6
CHUNK = 8
SIDE = 4
COLOURS = 3
SIDES = 2
ALL = slice(None)
WINDOW = 16
TILE = 512


def adam_step(scaled, master_old, mom_old, vel_old, learn_rate):
    mom_new = BETA_ONE * mom_old + (1.0 - BETA_ONE) * scaled
    vel_new = BETA_TWO * vel_old + (1.0 - BETA_TWO) * scaled * scaled
    master_new = master_old - learn_rate * (mom_new / CORR_ONE) / (jnp.sqrt(vel_new / CORR_TWO) + EPSILON)
    return master_new, mom_new, vel_new


def comm_kernel(lanes, *refs):
    (g_down2, grad_rows, mid_rows, in_rows, w_down1, w_up2, w_down2, der1, der2, act1), refs = refs[:10], refs[10:]
    states, refs = refs[:12], refs[12:]
    (lr_ref, clip_ref), refs = refs[:2], refs[2:]
    (w_out, up_out, down_out, norm_out, g_up1, g_down1, g_up2), refs = refs[:7], refs[7:]
    (total, peer_in, rs1, rs2, rs3, norm_line, norm_plane, send_g, recv_g, send_w, recv_w, block_tmp, w_own, up_state, down_state), refs = refs[:15], refs[15:]
    (left, flipped, mid_acc, mid_grad, w_tile, act_tile, der_tile, out_tile), refs = refs[:8], refs[8:]
    (load_sem, state_sem, pair_s, pair_r, rs1_s, rs1_r, rs2_s, rs2_r, rs3_s, rs3_r, nc_s, nc_r, na_s, na_r, xg_s, xg_r, xw_s, xw_r, own_sem, ag_s, ag_r, out_s, out_r) = refs[:23]
    row_sem, tile_sem, store_sem, pair_credit, ring_credit, early_l, early_s, early_r = refs[23:]
    half = lanes // 2
    me = lax.axis_index("data")
    core = lax.rem(me, SIDES)
    member = lax.rem(me, 4)
    pos = (me // 32, lax.rem(me // 8, 4), lax.rem(me // 2, 4))
    partner = me + 1 - 2 * core

    def device(axis, coord):
        return me + (coord - pos[axis]) * STRIDES[axis]

    def step(axis, hops):
        return lax.rem(pos[axis] + hops, 4)

    def remote(src, dst, send_sem, recv_sem, target):
        return pltpu.make_async_remote_copy(src_ref=src, dst_ref=dst, send_sem=send_sem, recv_sem=recv_sem, device_id=(target,), device_id_type=MESH)

    line, plane = lax.rem(me, 8), me // 8
    line_peers = [me - line + lax.rem(line + hops, 8) for hops in range(1, 8)]
    plane_peers = [8 * lax.rem(plane + hops, 16) + line for hops in range(1, 16)]
    peers = line_peers + plane_peers
    barrier = pltpu.get_barrier_semaphore()
    for peer in peers:
        pl.semaphore_signal(barrier, device_id=(peer,), device_id_type=MESH)

    grads = (g_up1, g_down1, g_up2, g_down2)
    mat_order = (3, 2, 1, 0)
    pair_slot = (1, 0, 1, 0)
    loads, pairs = {0: [], 2: []}, {0: [], 2: []}

    def issue_up(mat, x_low):
        for x in (x_low, x_low + 2):
            for owner in (1 - core, core):
                col = pl.multiple_of((x_low * 2 + owner) * lanes, lanes)
                src = grads[mat].at[:, :, x // SIDES, :, pl.ds(col, lanes)]
                if owner is core:
                    loads[mat].append(pltpu.make_async_copy(src, total.at[mat, :, :, x], load_sem.at[mat, x]))
                    loads[mat][-1].start()
                else:
                    pairs[mat].append(remote(src, peer_in.at[pair_slot[mat], :, :, x], pair_s.at[mat, x], pair_r.at[mat, x], partner))
                    pairs[mat][-1].start()

    def issue_rows(low, high):
        def move(i, carry):
            place = (i // 16, lax.rem(i // SIDE, 4), lax.rem(i, SIDE))
            there = g_down1.at[pl.ds(pl.multiple_of(i * 2 * ROWS + (1 - core) * ROWS, 8), ROWS)]
            here = g_down1.at[pl.ds(pl.multiple_of(i * 2 * ROWS + core * ROWS, 8), ROWS)]
            remote(there, peer_in.at[(pair_slot[DOWN1],) + place], pair_s.at[DOWN1, 0], pair_r.at[DOWN1, 0], partner).start()
            pltpu.make_async_copy(here, total.at[(1,) + place], load_sem.at[DOWN1, 0]).start()
            return carry

        lax.fori_loop(low, high, move, 0)

    loads[DOWN1] = [pltpu.make_async_copy(total.at[1], total.at[1], load_sem.at[DOWN1, 0])]
    pairs[DOWN1] = [remote(peer_in.at[pair_slot[DOWN1]], peer_in.at[pair_slot[DOWN1]], pair_s.at[DOWN1, 0], pair_r.at[DOWN1, 0], partner)]
    early = {}
    for hops in (2, 1, 3, 0):
        for colour in range(COLOURS):
            axis = ORDERS[colour][0]
            where = [ALL] * 3
            where[axis] = step(axis, hops)
            rows = pl.ds(CHUNK * colour, CHUNK)
            spots = (colour, hops)
            early[spots] = (
                pltpu.make_async_copy(g_down2.at[(*where, core, rows)], total.at[(DOWN2, *where, rows)], early_l.at[spots]),
                remote(g_down2.at[(*where, 1 - core, rows)], peer_in.at[(pair_slot[DOWN2], *where, rows)], early_s.at[spots], early_r.at[spots], partner),
            )

    tiles = SIDE * lanes // TILE

    def span(t):
        return pl.ds(pl.multiple_of(t * TILE, TILE), TILE)

    def fetch_a(t, slot):
        return [
            pltpu.make_async_copy(w_down2.at[span(t)], w_tile.at[slot], tile_sem.at[slot, 0]),
            pltpu.make_async_copy(w_up2.at[:, span(t)], act_tile.at[slot, pl.ds(0, lanes)], tile_sem.at[slot, 1]),
            pltpu.make_async_copy(der2.at[:, span(t)], der_tile.at[slot], tile_sem.at[slot, 2]),
        ]

    def fetch_b(t, slot):
        return [pltpu.make_async_copy(act1.at[:, span(t)], act_tile.at[slot], tile_sem.at[slot, 1])]

    def fetch_c(t, slot):
        return [
            pltpu.make_async_copy(w_down1.at[span(t)], w_tile.at[slot], tile_sem.at[slot, 0]),
            pltpu.make_async_copy(der1.at[:, span(t)], der_tile.at[slot], tile_sem.at[slot, 2]),
        ]

    def begin(copies):
        for copy in copies:
            copy.start()

    def end(copies):
        for copy in copies:
            copy.wait()

    row_loads = [pltpu.make_async_copy(grad_rows, left, row_sem.at[0]), pltpu.make_async_copy(mid_rows, mid_grad, row_sem.at[1])]
    begin(row_loads)
    begin(fetch_a(0, 0))
    begin([copies[0] for copies in early.values()])
    state_loads = []
    for field in range(COLOURS):
        for mat in range(SIDE):
            dst = (down_state if mat % SIDES else up_state).at[field, mat // SIDES]
            state_loads.append(pltpu.make_async_copy(states[4 * field + mat], dst, state_sem.at[field, mat]))
    begin(state_loads)
    def store_a(t, slot):
        return [pltpu.make_async_copy(out_tile.at[slot], g_up2.at[:, :, :, :, span(t)], store_sem.at[slot])]

    def store_b(t, slot):
        return [pltpu.make_async_copy(mid_acc.at[slot], g_down1.at[span(t)], store_sem.at[slot])]

    def store_c(t, slot):
        return [pltpu.make_async_copy(out_tile.at[slot], g_up1.at[:, :, :, :, span(t)], store_sem.at[slot])]

    def run(first, last, fetch, store, work):
        def tile(t, carry):
            slot = lax.rem(t, SIDES)

            @pl.when(t + 1 < tiles)
            def _():
                begin(fetch(t + 1, 1 - slot))

            end(fetch(t, slot))

            @pl.when(t - first >= 2)
            def _():
                end(store(t - 2, slot))

            work(slot)
            begin(store(t, slot))
            return carry

        lax.fori_loop(first, last, tile, 0)
        for t in range(max(first, last - 2), last):
            end(store(t, t % 2))

    def dot(lhs, rhs, lhs_dim, rhs_dim):
        return lax.dot_general(lhs, rhs, (((lhs_dim,), (rhs_dim,)), ((), ())), preferred_element_type=jnp.float32)

    def work_a(slot):
        grad_act2 = dot(left[...], w_tile[slot], 1, 1).astype(jnp.bfloat16)
        grad_pre2 = (grad_act2.astype(jnp.float32) * der_tile[slot]).astype(jnp.bfloat16)
        out_tile[slot] = dot(flipped[...], grad_pre2, 1, 0).reshape(out_tile.shape[1:])
        mid_acc[...] += dot(grad_pre2, act_tile[slot, pl.ds(0, lanes)], 1, 1).reshape(mid_acc.shape)

    def work_b(slot):
        mid_acc[slot] = dot(act_tile[slot], mid_grad[...], 0, 0)

    def work_c(slot):
        grad_act1 = dot(mid_grad[...], w_tile[slot], 1, 1).astype(jnp.bfloat16)
        grad_pre1 = (grad_act1.astype(jnp.float32) * der_tile[slot]).astype(jnp.bfloat16)
        out_tile[slot] = dot(flipped[...], grad_pre1, 1, 0).reshape(out_tile.shape[1:])

    def part(mats, coords, colour, side):
        lane = ALL if side is None else pl.ds(half * side, half)
        index = [mats, ALL, ALL, ALL, pl.ds(CHUNK * colour, CHUNK), lane]
        for axis, coord in coords.items():
            index[1 + axis] = coord
        return tuple(index)

    class Phase:
        def __init__(self, level, base, buf, send_sem, recv_sem):
            self.level, self.base, self.buf, self.send_sem, self.recv_sem = level, base, buf, send_sem, recv_sem
            self.mats, self.count = (slice(base, base + 2), 2) if level else (base, 4)
            self.copies = {}

        def where(self, colour, coord):
            order = ORDERS[colour]
            coords = {axis: pos[axis] for axis in order[:self.level]}
            coords[order[self.level]] = coord
            return coords

        def row(self, colour, coord, side, i):
            coords = self.where(colour, coord)
            if self.level:
                return part(self.base + i, coords, colour, side)
            coords[min(axis for axis in range(COLOURS) if axis not in coords)] = i
            return part(self.mats, coords, colour, side)

        def send(self, colour, side, kind, src, target):
            copy = remote(src, self.buf.at[colour, side, kind], self.send_sem.at[colour, side, kind], self.recv_sem.at[colour, side, kind], target)
            copy.start()
            self.copies[colour, side, kind] = copy

        def near(self, colour, side):
            axis = ORDERS[colour][self.level]
            coord = step(axis, 1 if side == 0 else 3)
            return coord, device(axis, coord)

        def start(self, kinds=(0, 1)):
            for kind in kinds:
                for colour in range(COLOURS):
                    for side in range(SIDES):
                        coord, target = self.near(colour, side)
                        aim = step(ORDERS[colour][self.level], 2) if kind == 0 else coord
                        src = total.at[part(self.mats, self.where(colour, aim), colour, side if kind == 0 else 1 - side)]
                        self.send(colour, side, kind, src, target)

        def forward(self):
            for colour in range(COLOURS):
                for side in range(SIDES):
                    coord, target = self.near(colour, side)
                    self.copies[colour, side, FAR].wait_recv()

                    def add_own(i, carry, colour=colour, side=side, coord=coord):
                        self.buf[colour, side, FAR, i] = self.buf[colour, side, FAR, i] + total[self.row(colour, coord, side, i)]
                        return carry

                    lax.fori_loop(0, self.count, add_own, 0)
                    self.send(colour, side, 2, self.buf.at[colour, side, FAR], target)

        def finish(self):
            for colour in range(COLOURS):
                for side in range(SIDES):
                    self.copies[colour, 1 - side, NEAR].wait_recv()
                    self.copies[colour, side, PASS].wait_recv()

                    def add_both(i, carry, colour=colour, side=side):
                        own = self.row(colour, pos[ORDERS[colour][self.level]], side, i)
                        total[own] = total[own] + (self.buf[colour, 1 - side, NEAR, i] + self.buf[colour, side, PASS, i])
                        return carry

                    lax.fori_loop(0, self.count, add_both, 0)

        def drain(self):
            for copy in self.copies.values():
                copy.wait_send()

    ring_slot = (1, 0, 1, 0)
    class Direct:
        def __init__(self, base, buf, send_sem, recv_sem):
            self.base, self.buf, self.send_sem, self.recv_sem = base, buf, send_sem, recv_sem
            self.copies = {}

        def index(self, colour, coord, mats):
            coords = {axis: pos[axis] for axis in range(COLOURS)}
            coords[ORDERS[colour][2]] = coord
            return part(mats, coords, colour, None)

        def start(self):
            for hops in (2, 1, 3):
                for colour in range(COLOURS):
                    axis = ORDERS[colour][2]
                    coord = step(axis, hops)
                    spots = (colour, hops - 1)
                    src = total.at[self.index(colour, coord, slice(self.base, self.base + 2))]
                    copy = remote(src, self.buf.at[spots], self.send_sem.at[spots], self.recv_sem.at[spots], device(axis, coord))
                    copy.start()
                    self.copies[spots] = copy

        def finish(self):
            for colour in range(COLOURS):
                for hops in range(COLOURS):
                    self.copies[colour, hops].wait_recv()
                for mat in range(SIDES):
                    own = self.index(colour, pos[ORDERS[colour][2]], self.base + mat)
                    total[own] = (total[own] + self.buf[colour, 0, mat]) + (self.buf[colour, 1, mat] + self.buf[colour, 2, mat])

        def drain(self):
            for copy in self.copies.values():
                copy.wait_send()

    first = {mat: Phase(0, mat, rs1.at[ring_slot[mat]], rs1_s.at[mat], rs1_r.at[mat]) for mat in mat_order}

    def add_pair(mat):
        end(loads[mat])
        for copy in pairs[mat]:
            copy.wait_recv()

        def add(i, carry):
            total[mat, i // SIDE, lax.rem(i, SIDE)] = total[mat, i // SIDE, lax.rem(i, SIDE)] + peer_in[pair_slot[mat], i // SIDE, lax.rem(i, SIDE)]
            return carry

        lax.fori_loop(0, 16, add, 0)
        if mat == UP2:
            pl.semaphore_signal(pair_credit, device_id=(partner,), device_id_type=MESH)

    def add_early(hops):
        for colour in range(COLOURS):
            early[colour, hops][0].wait()
            early[colour, hops][1].wait_recv()
            axis = ORDERS[colour][0]

            def add(i, carry, colour=colour, axis=axis):
                coords = {axis: step(axis, hops), (1 if axis == 0 else 0): i}
                own = part(DOWN2, coords, colour, None)
                total[own] = total[own] + peer_in[part(pair_slot[DOWN2], coords, colour, None)]
                return carry

            lax.fori_loop(0, 4, add, 0)

    ring = [device(axis, step(axis, hops)) for axis in range(COLOURS) for hops in (1, 3)]

    def close(mat):
        first[mat].finish()
        first[mat].drain()
        for peer in ring:
            pl.semaphore_signal(ring_credit.at[ring_slot[mat]], device_id=(peer,), device_id_type=MESH)

    second = {base: Phase(1, base, rs2.at[base // 2], rs2_s.at[base // 2], rs2_r.at[base // 2]) for base in (2, 0)}
    third = {base: Direct(base, rs3.at[base // 2], rs3_s.at[base // 2], rs3_r.at[base // 2]) for base in (2, 0)}
    end(row_loads)
    flipped[...] = mid_grad[...].T
    mid_acc[...] = jnp.zeros_like(mid_acc)
    run(0, 1, fetch_a, store_a, work_a)
    pl.semaphore_wait(barrier, len(peers))
    pairs[DOWN2] = [copies[1] for copies in early.values()]
    begin(pairs[DOWN2])
    run(1, 2, fetch_a, store_a, work_a)
    add_early(2)
    first[DOWN2].start((FAR,))
    run(2, 4, fetch_a, store_a, work_a)
    issue_up(UP2, 0)
    add_early(1)
    add_early(3)
    first[DOWN2].start((NEAR,))
    add_early(0)
    pl.semaphore_signal(pair_credit, device_id=(partner,), device_id_type=MESH)
    first[DOWN2].forward()
    run(4, tiles, fetch_a, store_a, work_a)
    issue_up(UP2, 1)
    begin(fetch_b(0, 0) + fetch_c(0, 0))
    in_load = pltpu.make_async_copy(in_rows, left, row_sem.at[0])
    in_load.start()
    mid_grad[...] = mid_acc[...].reshape(mid_grad.shape).astype(jnp.bfloat16)
    run(0, 2, fetch_b, store_b, work_b)
    add_pair(UP2)
    first[UP2].start()
    close(DOWN2)
    run(2, tiles, fetch_b, store_b, work_b)
    pl.semaphore_wait(pair_credit)
    issue_rows(0, 64)
    in_load.wait()
    flipped[...] = left[...].T
    run(0, 1, fetch_c, store_c, work_c)
    first[UP2].forward()
    run(1, 3, fetch_c, store_c, work_c)
    pl.semaphore_wait(pair_credit)
    issue_up(UP1, 0)
    add_pair(DOWN1)
    pl.semaphore_wait(ring_credit.at[0], len(ring))
    first[DOWN1].start()
    run(3, tiles, fetch_c, store_c, work_c)
    issue_up(UP1, 1)
    close(UP2)
    second[UP2].start()
    add_pair(UP1)
    pl.semaphore_wait(ring_credit.at[1], len(ring))
    first[UP1].start()
    first[DOWN1].forward()
    second[UP2].forward()
    first[UP1].forward()
    second[UP2].finish()
    third[UP2].start()
    first[DOWN1].finish()
    first[UP1].finish()
    second[UP1].start()
    third[UP2].finish()
    second[UP1].forward()
    second[UP1].finish()
    third[UP1].start()
    third[UP1].finish()

    group_scale = 1.0 / 128.0
    grad_own = [total[mat, *pos] * group_scale for mat in range(SIDE)]
    partial = None
    for block in grad_own:
        square = block * block
        for row in range(ROWS // 8):
            for col in range(max(1, lanes // 128)):
                tile = square[8 * row:8 * row + 8, 128 * col:128 * col + 128]
                partial = tile if partial is None else partial + tile
    norm_line[line] = partial
    sends = []

    def spread(buf, slot, targets, send_sem, recv_sem):
        copies = []
        for i, target in enumerate(targets):
            copies.append(remote(buf.at[slot], buf.at[slot], send_sem.at[i], recv_sem.at[i], target))
            copies[i].start()
        return copies

    swap = spread(norm_line, line, line_peers, nc_s, nc_r)
    for target in range(SIDE):
        for i, mat in enumerate((0, 2)):
            send_g[target, i] = grad_own[mat][SUB * target:SUB * target + SUB]
    moves = []
    for hops in range(1, SIDE):
        other = lax.rem(member + hops, SIDE)
        copy = remote(send_g.at[other], recv_g.at[member], xg_s.at[hops - 1], xg_r.at[hops - 1], me - member + other)
        copy.start()
        moves.append(copy)
    recv_g[member] = send_g[member]
    for copy in swap:
        copy.wait_recv()
    norm_plane[plane] = jnp.sum(norm_line[...], axis=0)
    cross = spread(norm_plane, plane, plane_peers, na_s, na_r)
    for copy in cross:
        copy.wait_recv()
    running = jnp.sum(norm_plane[...], axis=0)
    sends = swap + cross + moves
    norm = jnp.sqrt(jnp.sum(jnp.sum(running, axis=1, keepdims=True), axis=0, keepdims=True))
    norm_out[...] = jnp.broadcast_to(norm, norm_out.shape)
    clip_scale = jnp.minimum(1.0, clip_ref[0] / (norm + NORM_EPS))
    learn_rate = lr_ref[0]

    end(state_loads)
    for i in range(SIDES):
        fresh = adam_step(grad_own[2 * i + 1] * clip_scale, down_state[0, i], down_state[1, i], down_state[2, i], learn_rate)
        for field in range(COLOURS):
            down_state[field, i] = fresh[field]
        w_own[2 + i] = fresh[0].astype(jnp.bfloat16)

    def spot(group, coords, colour, side):
        lane = ALL if side is None else pl.ds(half * side, half)
        index = [pl.ds(2 * group, 2), ALL, ALL, ALL, core, pl.ds(CHUNK * colour, CHUNK), lane]
        for axis, coord in coords.items():
            index[1 + axis] = coord
        return w_out.at[tuple(index)]

    handed = []

    class Gather:
        def __init__(self, group, level):
            self.group, self.level = group, level
            self.copies = {}

        def spot(self, colour, coord, side):
            order = ORDERS[colour]
            coords = {axis: pos[axis] for axis in order[:self.level]}
            coords[order[self.level]] = coord
            return spot(self.group, coords, colour, side)

        def near(self, colour, side):
            axis = ORDERS[colour][self.level]
            coord = step(axis, 1 if side == 0 else 3)
            return coord, device(axis, coord)

        def send(self, colour, side, kind, src, dst):
            spots = (self.group, self.level, colour, side, kind)
            copy = remote(src, dst, ag_s.at[spots], ag_r.at[spots], self.near(colour, side)[1])
            copy.start()
            self.copies[colour, side, kind] = copy

        def hand(self, ref, slot):
            copy = remote(ref, ref, out_s.at[self.group, slot], out_r.at[self.group, slot], partner)
            copy.start()
            handed.append(copy)

        def start_direct(self):
            for hops in (2, 1, 3):
                for colour in range(COLOURS):
                    axis = ORDERS[colour][self.level]
                    dst = self.spot(colour, pos[axis], None)
                    src = w_own.at[pl.ds(2 * self.group, 2), pl.ds(CHUNK * colour, CHUNK)] if self.level == 2 else dst
                    spots = (self.group, self.level, colour, 0, hops - 1)
                    copy = remote(src, dst, ag_s.at[spots], ag_r.at[spots], device(axis, step(axis, hops)))
                    copy.start()
                    self.copies[colour, hops] = copy

        def finish_direct(self):
            for copy in self.copies.values():
                copy.wait_recv()

        def start(self):
            for kind in range(SIDES):
                for colour in range(COLOURS):
                    for side in range(SIDES):
                        ref = self.spot(colour, pos[ORDERS[colour][0]], side if kind == 0 else 1 - side)
                        self.send(colour, side, kind, ref, ref)
            for colour in range(COLOURS):
                self.hand(self.spot(colour, pos[ORDERS[colour][0]], None), 5 * colour)

        def forward(self):
            for colour in range(COLOURS):
                for side in range(SIDES):
                    self.copies[colour, side, FAR].wait_recv()
                    ref = self.spot(colour, self.near(colour, 1 - side)[0], side)
                    self.send(colour, side, 2, ref, ref)

        def finish(self):
            for colour in range(COLOURS):
                for side in range(SIDES):
                    self.copies[colour, side, NEAR].wait_recv()
                    self.hand(self.spot(colour, self.near(colour, 1 - side)[0], None), 5 * colour + 1 + side)
            for colour in range(COLOURS):
                for side in range(SIDES):
                    self.copies[colour, side, PASS].wait_recv()
                    self.hand(self.spot(colour, step(ORDERS[colour][0], 2), side), 5 * colour + 3 + side)

    keeps = [pltpu.make_async_copy(w_own.at[pl.ds(2 * group, 2)], w_out.at[pl.ds(2 * group, 2), *pos, core], own_sem.at[group]) for group in range(SIDES)]
    gathers = {(group, level): Gather(group, level) for group in range(SIDES) for level in range(COLOURS)}
    gathers[DOWN, EARLY].start_direct()
    keeps[DOWN].start()

    for copy in moves:
        copy.wait_recv()
    for i in range(SIDES):
        for col in range(SIDE):
            cols = slice(col * lanes, (col + 1) * lanes)
            scaled = recv_g[col, i] * clip_scale
            fresh = adam_step(scaled, up_state[0, i, :, cols], up_state[1, i, :, cols], up_state[2, i, :, cols], learn_rate)
            for field in range(COLOURS):
                up_state[field, i, :, cols] = fresh[field]
            send_w[col, i] = fresh[0]
    moves = []
    for hops in range(1, SIDE):
        other = lax.rem(member + hops, SIDE)
        copy = remote(send_w.at[other], recv_w.at[member], xw_s.at[hops - 1], xw_r.at[hops - 1], me - member + other)
        copy.start()
        moves.append(copy)
    recv_w[member] = send_w[member]
    state_stores = [pltpu.make_async_copy(up_state, up_out, state_sem.at[0, 0]), pltpu.make_async_copy(down_state, down_out, state_sem.at[0, 1])]
    begin(state_stores)
    gathers[DOWN, EARLY].finish_direct()
    keeps[DOWN].wait()
    gathers[DOWN, MIDDLE].start_direct()
    for copy in moves:
        copy.wait_recv()
    sends = sends + moves
    for i in range(SIDES):
        for source in range(SIDE):
            block_tmp[SUB * source:SUB * source + SUB] = recv_w[source, i]
        w_own[i] = block_tmp[...].astype(jnp.bfloat16)
    gathers[UP, EARLY].start_direct()
    keeps[UP].start()
    gathers[DOWN, MIDDLE].finish_direct()
    gathers[DOWN, LAST].start()
    gathers[UP, EARLY].finish_direct()
    keeps[UP].wait()
    gathers[UP, MIDDLE].start_direct()
    gathers[DOWN, LAST].forward()
    gathers[UP, MIDDLE].finish_direct()
    gathers[UP, LAST].start()
    gathers[DOWN, LAST].finish()
    gathers[UP, LAST].forward()
    gathers[UP, LAST].finish()
    for gather in gathers.values():
        sends = sends + list(gather.copies.values())
    for phase in [first[DOWN1], first[UP1]] + list(second.values()) + list(third.values()):
        phase.drain()
    for mat in mat_order:
        for copy in pairs[mat]:
            copy.wait_send()
    for copy in sends:
        copy.wait_send()
    for copy in handed + state_stores:
        copy.wait()


def place_kernel(lanes, w_ref, up_ref, down_ref, norm_ref, *refs):
    weights, states, norm_out, (w_tmp, up_tmp, down_tmp, in_sem, state_in, out_sem, state_out) = refs[:4], refs[4:16], refs[16], refs[17:]
    norm_out[0] = jnp.max(norm_ref[...])
    loads = [[pltpu.make_async_copy(w_ref.at[mat % SIDES * 2 + mat // SIDES, z], w_tmp.at[mat, z], in_sem.at[mat, z]) for z in range(SIDE)] for mat in range(SIDE)]
    queue = [copy for row in loads for copy in row]
    for copy in queue[:WINDOW]:
        copy.start()
    state_loads = [pltpu.make_async_copy(up_ref, up_tmp, state_in.at[0]), pltpu.make_async_copy(down_ref, down_tmp, state_in.at[1])]
    for copy in state_loads:
        copy.start()
    stores = []
    for mat in range(SIDE):
        for z in range(SIDE):
            loads[mat][z].wait()
            ahead = 4 * mat + z + WINDOW
            if ahead < len(queue):
                queue[ahead].start()
            if mat % SIDES:
                copies = [pltpu.make_async_copy(w_tmp.at[mat, z], weights[mat].at[z], out_sem.at[mat, z, 0])]
            else:
                copies = []
                for member in range(SIDE):
                    src = w_tmp.at[mat, z, :, :, member // SIDES, member % SIDES]
                    copies.append(pltpu.make_async_copy(src, weights[mat].at[z, :, :, :, pl.ds(member * lanes, lanes)], out_sem.at[mat, z, member]))
            for copy in copies:
                copy.start()
            stores = stores + copies
    for copy in state_loads:
        copy.wait()
    for field in range(COLOURS):
        for mat in range(SIDE):
            src = (down_tmp if mat % SIDES else up_tmp).at[field, mat // SIDES]
            copy = pltpu.make_async_copy(src, states[4 * field + mat], state_out.at[field, mat])
            copy.start()
            stores.append(copy)
    for copy in stores:
        copy.wait()


def comm_call(lanes, grad_down2, rows, weights_in, hidden, masters, moms, vels, learn_rate, clip_norm):
    up = (SIDE, SIDE, SIDES, ROWS, SIDE * lanes)
    down = (SIDE, SIDE, SIDE, SIDES, ROWS, lanes)
    local_rows = rows[0].shape[0]
    half = lanes // 2
    f32 = jnp.float32
    bf16 = jnp.bfloat16
    up_shape = (COLOURS, SIDES, SUB, SIDE * lanes)
    down_shape = (COLOURS, SIDES, ROWS, lanes)
    dma = pltpu.SemaphoreType.DMA
    vmem = pl.BlockSpec(memory_space=pltpu.VMEM)
    smem = pl.BlockSpec(memory_space=pltpu.SMEM)
    hbm = pl.BlockSpec(memory_space=pl.ANY)
    scratch = [
        pltpu.VMEM((SIDE, SIDE, SIDE, SIDE, ROWS, lanes), f32),
        pltpu.VMEM((SIDES, SIDE, SIDE, SIDE, ROWS, lanes), f32),
        pltpu.VMEM((SIDES, COLOURS, SIDES, COLOURS, SIDE, SIDE, CHUNK, half), f32),
        pltpu.VMEM((SIDES, COLOURS, SIDES, COLOURS, SIDES, SIDE, CHUNK, half), f32),
        pltpu.VMEM((SIDES, COLOURS, COLOURS, SIDES, CHUNK, lanes), f32),
        pltpu.VMEM((8, 8, 128), f32),
        pltpu.VMEM((16, 8, 128), f32),
        pltpu.VMEM((SIDE, SIDES, SUB, lanes), f32),
        pltpu.VMEM((SIDE, SIDES, SUB, lanes), f32),
        pltpu.VMEM((SIDE, SIDES, SUB, lanes), f32),
        pltpu.VMEM((SIDE, SIDES, SUB, lanes), f32),
        pltpu.VMEM((ROWS, lanes), f32),
        pltpu.VMEM((SIDE, ROWS, lanes), jnp.bfloat16),
        pltpu.VMEM(up_shape, f32),
        pltpu.VMEM(down_shape, f32),
        pltpu.VMEM((local_rows, lanes), bf16),
        pltpu.VMEM((lanes, local_rows), bf16),
        pltpu.VMEM((SIDES, local_rows // SIDES, lanes), f32),
        pltpu.VMEM((local_rows, lanes), bf16),
        pltpu.VMEM((SIDES, TILE, lanes), bf16),
        pltpu.VMEM((SIDES, local_rows, TILE), bf16),
        pltpu.VMEM((SIDES, local_rows, TILE), f32),
        pltpu.VMEM((SIDES, SIDE, SIDE, SIDES, ROWS, TILE), f32),
        dma((SIDE, SIDE)), dma((COLOURS, SIDE)), dma((SIDE, SIDE)), dma((SIDE, SIDE)),
        dma((SIDE, COLOURS, SIDES, COLOURS)), dma((SIDE, COLOURS, SIDES, COLOURS)), dma((SIDES, COLOURS, SIDES, COLOURS)), dma((SIDES, COLOURS, SIDES, COLOURS)), dma((SIDES, COLOURS, COLOURS)), dma((SIDES, COLOURS, COLOURS)),
        dma((7,)), dma((7,)), dma((15,)), dma((15,)), dma((COLOURS,)), dma((COLOURS,)), dma((COLOURS,)), dma((COLOURS,)),
        dma((SIDES,)), dma((SIDES, COLOURS, COLOURS, SIDES, COLOURS)), dma((SIDES, COLOURS, COLOURS, SIDES, COLOURS)), dma((SIDES, 15)), dma((SIDES, 15)),
        dma((SIDES,)), dma((SIDES, COLOURS)), dma((SIDES,)), pltpu.SemaphoreType.REGULAR, pltpu.SemaphoreType.REGULAR((2,)), dma((COLOURS, SIDE)), dma((COLOURS, SIDE)), dma((COLOURS, SIDE)),
    ]
    outs = pl.pallas_call(
        functools.partial(comm_kernel, lanes),
        name="reduce_update_gather",
        out_shape=[jax.ShapeDtypeStruct((SIDE, SIDE, SIDE, SIDE, SIDES, ROWS, lanes), bf16), jax.ShapeDtypeStruct(up_shape, f32), jax.ShapeDtypeStruct(down_shape, f32), jax.ShapeDtypeStruct((8, 128), f32), jax.ShapeDtypeStruct(up, f32), jax.ShapeDtypeStruct((3072, lanes), f32), jax.ShapeDtypeStruct(up, f32)],
        in_specs=[hbm] * 22 + [smem] * 2,
        out_specs=[hbm] * 3 + [vmem] + [hbm] * 3,
        scratch_shapes=scratch,
        compiler_params=pltpu.CompilerParams(collective_id=0, has_side_effects=True, vmem_limit_bytes=67043328),
    )(grad_down2.reshape(down), *rows, *weights_in, *hidden, *masters, *moms, *vels, learn_rate.reshape(1), clip_norm.reshape(1))
    split = (SIDE, SIDE, SIDES, SIDES, SIDES, ROWS, lanes)
    placed = pl.pallas_call(
        functools.partial(place_kernel, lanes),
        name="place_outputs",
        out_shape=[jax.ShapeDtypeStruct(split if mat % SIDES else up, bf16) for mat in range(SIDE)] + [jax.ShapeDtypeStruct(m.shape, f32) for m in masters] * 3 + [jax.ShapeDtypeStruct((1,), f32)],
        in_specs=[hbm] * 3 + [vmem],
        out_specs=[hbm] * 16 + [smem],
        scratch_shapes=[
            pltpu.VMEM((SIDE,) + split, bf16), pltpu.VMEM(up_shape, f32), pltpu.VMEM(down_shape, f32),
            dma((SIDE, SIDE)), dma((SIDES,)), dma((SIDE, SIDE, SIDE)), dma((COLOURS, SIDE)),
        ],
        compiler_params=pltpu.CompilerParams(vmem_limit_bytes=67043328),
    )(outs[0].reshape((4,) + split), *outs[1:4])
    weights = [placed[mat].reshape(masters[mat].shape[0] * 128, -1) for mat in range(SIDE)]
    return tuple(weights) + tuple(placed[4:16]) + (placed[16][0],)


def mat_tn(left, right):
    return lax.dot_general(left, right, (((0,), (0,)), ((), ())), preferred_element_type=jnp.float32)


def gelu_pair(pre):
    normal_cdf = 0.5 * (1.0 + lax.erf(pre * ROOT_HALF))
    density = jnp.exp(-0.5 * pre * pre) * INV_ROOT_TAU
    return pre * normal_cdf, normal_cdf + pre * density


def solution(mesh):
    rows_spec = P("data", None)
    full_spec = P(None, None)
    scalar_spec = P()

    def shard_body(act_in, grad_out, w_up1, w_down1, w_up2, w_down2, *rest):
        gel_up1, der_up1 = gelu_pair(jnp.dot(act_in, w_up1, preferred_element_type=jnp.float32))
        act_up1 = gel_up1.astype(jnp.bfloat16)
        mid_act = jnp.dot(act_up1, w_down1, preferred_element_type=jnp.float32).astype(jnp.bfloat16)
        gel_up2, der_up2 = gelu_pair(jnp.dot(mid_act, w_up2, preferred_element_type=jnp.float32))
        grad_down2 = mat_tn(gel_up2.astype(jnp.bfloat16), grad_out)
        return comm_call(768, grad_down2, (grad_out, mid_act, act_in), (w_down1, w_up2, w_down2), (der_up1, der_up2, act_up1), rest[0:4], rest[4:8], rest[8:12], rest[12], rest[13])

    in_specs = (rows_spec, rows_spec) + (full_spec,) * 4 + (rows_spec,) * 12 + (scalar_spec, scalar_spec)
    out_specs = (full_spec,) * 4 + (rows_spec,) * 12 + (scalar_spec,)
    return jax.shard_map(shard_body, mesh=mesh, in_specs=in_specs, out_specs=out_specs, check_vma=False)
```
